8 devices in a mesh: dp: 2 (over z, y), sp: 4 (over x, core).
Axes of the slice: x: 2, y: 2, z: 1, core: 2. Of those that a mesh axis runs over, the one named last changes fastest.
Arguments:
- dec_hidden: bfloat16 [2048, 1280], P(('dp', 'sp')), parts along dimension 0
- enc_memory: bfloat16 [8192, 1280], P(('dp', 'sp')), parts along dimension 0
- mem_len: int32 [2], P('dp'), parts along dimension 0
- norm_self: bfloat16 [2, 1280], replicated
- norm_cross: bfloat16 [2, 1280], replicated
- norm_mlp: bfloat16 [2, 1280], replicated
- self_q: bfloat16 [2, 1280, 1280], replicated
- self_k: bfloat16 [2, 1280, 1280], replicated
- self_v: bfloat16 [2, 1280, 1280], replicated
- self_o: bfloat16 [2, 20, 64, 1280], replicated
- cross_q: bfloat16 [2, 1280, 1280], replicated
- cross_k: bfloat16 [2, 1280, 1280], replicated
- cross_v: bfloat16 [2, 1280, 1280], replicated
- cross_o: bfloat16 [2, 20, 64, 1280], replicated
- mlp_gate: bfloat16 [2, 1280, 5120], replicated
- mlp_up: bfloat16 [2, 1280, 5120], replicated
- mlp_down: bfloat16 [2, 5120, 1280], replicated
Outputs:
- output: bfloat16 [2048, 1280], P(('dp', 'sp')), parts along dimension 0
There are 2 independent parts. The reference program is written for one: setup_inputs(seed, part) draws one part's arguments, and reference() takes and returns one part's arrays. A program takes and returns all parts, laid end to end along the dimension named above; an argument that names none is the same for every part.
All inputs are finite; a program needn't handle non-finite values.
Results may differ from the reference program's by a relative error of at most 0.015751.
Values are sent between devices in bfloat16 or wider.
A program may use at most 1 GiB of HBM per device.

```python
import jax
import jax.numpy as jnp
from jax import lax

D = 1280
HEADS = 20
KV_HEADS = 20
HEAD = 64
FF = 5120
LAYERS = 2
TQ = 1024
TM = 4096
WAVES = 4
EPS = 1e-6
NEG_BIG = -1e30
SOFT_SCALE = HEAD ** -0.5
DKV = KV_HEADS * HEAD


def smooth_field(wave_key, n_rows, n_cols):
    directions = jax.random.normal(wave_key, (WAVES, n_cols), jnp.float32)
    positions = jnp.arange(n_rows, dtype=jnp.float32) / n_rows
    freq_list = jnp.arange(1, WAVES + 1, dtype=jnp.float32)
    wave_rows = jnp.cos(jnp.pi * positions[:, None] * freq_list[None, :])
    return jnp.dot(wave_rows, directions)


def setup_inputs(seed: int = 0, part: int = 0) -> dict:
    part_key = jax.random.fold_in(jax.random.key(seed), part)
    part_keys = jax.random.split(part_key, 5)
    shared = jax.random.split(jax.random.key(seed + 1), 16)

    def weight(key_index, shape_tail, fan_in):
        raw_draw = jax.random.normal(shared[key_index], (LAYERS,) + shape_tail, jnp.float32)
        return (raw_draw * fan_in ** -0.5).astype(jnp.bfloat16)

    def gain(key_index):
        return jax.random.uniform(shared[key_index], (LAYERS, D), jnp.float32, 0.5, 1.5).astype(jnp.bfloat16)

    dec_hidden = jax.random.normal(part_keys[0], (TQ, D), jnp.float32) + smooth_field(part_keys[1], TQ, D)
    enc_memory = jax.random.normal(part_keys[2], (TM, D), jnp.float32) + smooth_field(part_keys[3], TM, D)
    mem_len = jax.random.randint(part_keys[4], (1,), TM // 4, 3 * TM // 4 + 1, dtype=jnp.int32)
    return {
        'dec_hidden': dec_hidden.astype(jnp.bfloat16),
        'enc_memory': enc_memory.astype(jnp.bfloat16),
        'mem_len': mem_len,
        'norm_self': gain(0),
        'norm_cross': gain(1),
        'norm_mlp': gain(2),
        'self_q': weight(3, (D, D), D),
        'self_k': weight(4, (D, D), D),
        'self_v': weight(5, (D, D), D),
        'self_o': weight(6, (HEADS, HEAD, D), D),
        'cross_q': weight(7, (D, D), D),
        'cross_k': weight(8, (D, DKV), D),
        'cross_v': weight(9, (D, DKV), D),
        'cross_o': weight(10, (HEADS, HEAD, D), D),
        'mlp_gate': weight(11, (D, FF), D),
        'mlp_up': weight(12, (D, FF), D),
        'mlp_down': weight(13, (FF, D), FF),
    }


def rms_norm(hidden, gain_vec):
    hidden32 = hidden.astype(jnp.float32)
    inv_rms = lax.rsqrt(jnp.mean(hidden32 * hidden32, axis=-1, keepdims=True) + EPS)
    return (hidden32 * inv_rms * gain_vec.astype(jnp.float32)).astype(jnp.bfloat16)


def project(acts, weight_mat):
    return jnp.dot(acts, weight_mat, preferred_element_type=jnp.float32).astype(jnp.bfloat16)


def add_residual(hidden, update):
    return (hidden.astype(jnp.float32) + update).astype(jnp.bfloat16)


def head_attend(query_h, key_h, value_h, allowed):
    scores = jnp.dot(query_h, key_h.T, preferred_element_type=jnp.float32) * SOFT_SCALE
    scores = jnp.where(allowed, scores, NEG_BIG)
    weights = jnp.exp(scores - jnp.max(scores, axis=-1, keepdims=True))
    numerator = jnp.dot(weights.astype(jnp.bfloat16), value_h, preferred_element_type=jnp.float32)
    return numerator / jnp.sum(weights, axis=-1, keepdims=True)


def multi_head(queries, keys_all, values_all, allowed):
    q_rows = queries.shape[0]
    k_rows = keys_all.shape[0]
    kv_count = keys_all.shape[1] // HEAD
    q_heads = queries.reshape(q_rows, HEADS, HEAD).transpose(1, 0, 2)
    k_heads = jnp.repeat(keys_all.reshape(k_rows, kv_count, HEAD).transpose(1, 0, 2), HEADS // kv_count, axis=0)
    v_heads = jnp.repeat(values_all.reshape(k_rows, kv_count, HEAD).transpose(1, 0, 2), HEADS // kv_count, axis=0)
    per_head = lax.map(lambda head_trio: head_attend(head_trio[0], head_trio[1], head_trio[2], allowed), (q_heads, k_heads, v_heads))
    return per_head.transpose(1, 0, 2).astype(jnp.bfloat16)


def reference(dec_hidden, enc_memory, mem_len, norm_self, norm_cross, norm_mlp, self_q, self_k, self_v, self_o, cross_q, cross_k, cross_v, cross_o, mlp_gate, mlp_up, mlp_down):
    causal = jnp.arange(TQ)[:, None] >= jnp.arange(TQ)[None, :]
    mem_valid = (jnp.arange(TM) < mem_len[0])[None, :]
    stacked = {
        'norm_self': norm_self, 'norm_cross': norm_cross, 'norm_mlp': norm_mlp,
        'self_q': self_q, 'self_k': self_k, 'self_v': self_v, 'self_o': self_o,
        'cross_q': cross_q, 'cross_k': cross_k, 'cross_v': cross_v, 'cross_o': cross_o,
        'mlp_gate': mlp_gate, 'mlp_up': mlp_up, 'mlp_down': mlp_down,
    }

    def layer_step(hidden, params):
        normed = rms_norm(hidden, params['norm_self'])
        attended = multi_head(project(normed, params['self_q']), project(normed, params['self_k']), project(normed, params['self_v']), causal)
        update = jnp.einsum('thd,hdo->to', attended.astype(jnp.float32), params['self_o'].astype(jnp.float32))
        hidden = add_residual(hidden, update)
        normed = rms_norm(hidden, params['norm_cross'])
        attended = multi_head(project(normed, params['cross_q']), project(enc_memory, params['cross_k']), project(enc_memory, params['cross_v']), mem_valid)
        update = jnp.einsum('thd,hdo->to', attended.astype(jnp.float32), params['cross_o'].astype(jnp.float32))
        hidden = add_residual(hidden, update)
        normed = rms_norm(hidden, params['norm_mlp'])
        gate_pre = jnp.dot(normed, params['mlp_gate'], preferred_element_type=jnp.float32)
        up_proj = jnp.dot(normed, params['mlp_up'], preferred_element_type=jnp.float32)
        hidden_act = (jax.nn.silu(gate_pre) * up_proj).astype(jnp.bfloat16)
        update = jnp.dot(hidden_act, params['mlp_down'], preferred_element_type=jnp.float32)
        return add_residual(hidden, update), None

    final_hidden, _ = lax.scan(layer_step, dec_hidden, stacked)
    return final_hidden
```

```python
import functools

import jax
import jax.numpy as jnp
from jax import lax
from jax.experimental import pallas as pl
from jax.experimental.pallas import tpu as pltpu
from jax.sharding import PartitionSpec as P

EPS = 1e-6
NEG_BIG = -1e30
F32 = jnp.float32
BF16 = jnp.bfloat16
CH = 512
VMEM_LIMIT = 62 * 1024 * 1024
ANY = pl.BlockSpec(memory_space=pl.ANY)
SMEM = pl.BlockSpec(memory_space=pltpu.SMEM)
VMEM = pl.BlockSpec(memory_space=pltpu.VMEM)


def rms(h, gain):
    h32 = h.astype(F32)
    inv = lax.rsqrt(jnp.mean(h32 * h32, axis=-1, keepdims=True) + EPS)
    return (h32 * inv * gain.astype(F32)).astype(BF16)


def dot(a, b):
    return jnp.dot(a, b, preferred_element_type=F32)


def dot_nt(a, b):
    return lax.dot_general(a, b, (((1,), (1,)), ((), ())), preferred_element_type=F32)


def kv_kernel(n_src, lim_ref, pick_ref, *refs):
    srcs, (wk_ref, wv_ref, k_ref, vt_ref, mem, sem) = refs[:n_src], refs[n_src:]
    rows = mem.shape[0]

    @pl.when((pl.program_id(0) == 0) & (pl.program_id(1) == 0))
    def _():
        if n_src == 1:
            cp = pltpu.make_async_copy(srcs[0], mem, sem)
            cp.start()
            cp.wait()
        else:
            @pl.when(pick_ref[0] == 0)
            def _():
                cp = pltpu.make_async_copy(srcs[0], mem, sem)
                cp.start()
                cp.wait()

            @pl.when(pick_ref[0] != 0)
            def _():
                cp = pltpu.make_async_copy(srcs[1], mem.at[pl.ds(0, CH)], sem)
                cp.start()
                cp.wait()

    for r in range(rows // 256):
        @pl.when(lim_ref[r * 256 // CH] > 0)
        def _(r=r):
            m = mem[pl.ds(r * 256, 256), :]
            k_ref[0, pl.ds(r * 256, 256), :] = dot(m, wk_ref[0]).astype(BF16)
            vt_ref[0, :, pl.ds(r * 256, 256)] = dot(m, wv_ref[0]).astype(BF16).T


def kv_project(lims, pick, srcs, wk, wv, rows, layers):
    width, cols = wk.shape[1], wk.shape[2]
    lo, n = layers
    flops = n * 4 * rows * width * cols
    return pl.pallas_call(
        functools.partial(kv_kernel, len(srcs)),
        grid=(n, cols // 256),
        in_specs=[SMEM, SMEM] + [ANY] * len(srcs) + [pl.BlockSpec((1, width, 256), lambda l, t: (l + lo, 0, t))] * 2,
        out_specs=[pl.BlockSpec((1, rows, 256), lambda l, t: (l, 0, t)), pl.BlockSpec((1, 256, rows), lambda l, t: (l, t, 0))],
        out_shape=[jax.ShapeDtypeStruct((n, rows, cols), BF16), jax.ShapeDtypeStruct((n, cols, rows), BF16)],
        scratch_shapes=[pltpu.VMEM((rows, width), BF16), pltpu.SemaphoreType.DMA],
        cost_estimate=pl.CostEstimate(flops=flops, bytes_accessed=n * 4 * width * cols, transcendentals=0),
        compiler_params=pltpu.CompilerParams(vmem_limit_bytes=40 * 1024 * 1024),
        name="kv_project",
    )(lims, pick, *srcs, wk, wv)


def pair_queries(q):
    lane = lax.broadcasted_iota(jnp.int32, q.shape, 1)
    zero = jnp.zeros_like(q)
    return jnp.where(lane < 64, q, zero), jnp.where(lane < 64, zero, q)


def attend_chunk(k, vt, q_pair, m_ref, l_ref, acc_ref, fix):
    for h in range(2):
        s = fix(dot_nt(k, q_pair[h]))
        m_old = m_ref[h:h + 1, :]
        m_new = jnp.maximum(m_old, jnp.max(s, axis=0, keepdims=True))
        p = jnp.exp(s - m_new)
        alpha = jnp.exp(m_old - m_new)
        m_ref[h:h + 1, :] = m_new
        l_ref[h:h + 1, :] = l_ref[h:h + 1, :] * alpha + jnp.sum(p, axis=0, keepdims=True)
        acc_ref[h] = acc_ref[h] * alpha + dot(vt[h * 64:(h + 1) * 64, :], p.astype(BF16))


def attend_init(m_ref, l_ref, acc_ref):
    m_ref[...] = jnp.full_like(m_ref, -jnp.inf)
    l_ref[...] = jnp.zeros_like(l_ref)
    acc_ref[...] = jnp.zeros_like(acc_ref)


def attend_finish(at_ref, pair, l_ref, acc_ref):
    for h in range(2):
        rows = pl.ds(pl.multiple_of(pair * 128 + h * 64, 64), 64)
        at_ref[rows, :] = (acc_ref[h] / l_ref[h:h + 1, :]).astype(BF16)


def self_kernel(layer, dev_ref, own_ref, s1_ref, s2_ref, s3_ref, gs_ref, gc_ref, wq, wk, wv, wo, wcq, hid_ref, q_ref,
                w_s, x_s, k_s, vt_s, qs, bias, at_s, a_s, m_s, l_s, acc_s, sems):
    rows, width = own_ref.shape
    tiles = width // 256
    dev = dev_ref[0]
    chip1 = dev >= 2

    def copy(n, src, t):
        cols = pl.ds(pl.multiple_of(t * 256, 256), 256)
        return pltpu.make_async_copy(src.at[layer, :, cols], w_s.at[n, t], sems.at[n, t])

    for n, src in enumerate((wk, wv, wq, wo, wcq)):
        for t in range(tiles):
            copy(n, src, t).start()

    gain = gs_ref[layer:layer + 1, :]
    x_s[pl.ds(0, rows), :] = rms(own_ref[...], gain)
    x_s[pl.ds(rows, rows), :] = rms(s1_ref[...], gain)

    @pl.when(chip1)
    def _():
        x_s[pl.ds(2 * rows, rows), :] = rms(s2_ref[...], gain)
        x_s[pl.ds(3 * rows, rows), :] = rms(s3_ref[...], gain)

    key = lax.broadcasted_iota(jnp.int32, (rows, rows), 0)
    query = lax.broadcasted_iota(jnp.int32, (rows, rows), 1)
    bias[pl.ds(0, rows), :] = jnp.where(key <= query, 0.0, NEG_BIG)
    bias[pl.ds(rows, rows), :] = jnp.full((rows, rows), jnp.where(dev % 2 == 1, 0.0, NEG_BIG), F32)

    def project_kv(t, _):
        cols = pl.ds(pl.multiple_of(t * 256, 256), 256)
        copy(0, wk, t).wait()
        copy(1, wv, t).wait()

        def part(at):
            part_rows = pl.ds(at, 2 * rows)
            x = x_s[part_rows, :]
            k_s[part_rows, cols] = dot(x, w_s[0, t]).astype(BF16)
            vt_s[cols, part_rows] = dot(x, w_s[1, t]).astype(BF16).T

        part(0)

        @pl.when(chip1)
        def _():
            part(2 * rows)
        return 0

    lax.fori_loop(0, tiles, project_kv, 0)

    def project_q(t, _):
        cols = pl.ds(pl.multiple_of(t * 256, 256), 256)
        copy(2, wq, t).wait()
        qs[:, cols] = dot(x_s[pl.ds(0, rows), :], w_s[2, t]).astype(BF16) * BF16(0.125)
        return 0

    lax.fori_loop(0, tiles, project_q, 0)

    def pair_step(i, _):
        cols = pl.ds(pl.multiple_of(i * 128, 128), 128)
        q_pair = pair_queries(qs[:, cols])
        attend_init(m_s, l_s, acc_s)
        attend_chunk(k_s[pl.ds(0, 2 * rows), cols], vt_s[cols, pl.ds(0, 2 * rows)], q_pair, m_s, l_s, acc_s,
                     lambda s: s + bias[...])

        @pl.when(chip1)
        def _():
            attend_chunk(k_s[pl.ds(2 * rows, 2 * rows), cols], vt_s[cols, pl.ds(2 * rows, 2 * rows)], q_pair, m_s, l_s, acc_s,
                         lambda s: s)
        attend_finish(at_s, i, l_s, acc_s)
        return 0

    lax.fori_loop(0, width // 128, pair_step, 0)

    a_s[...] = at_s[...].T

    def project_o(t, _):
        cols = pl.ds(pl.multiple_of(t * 256, 256), 256)
        copy(3, wo, t).wait()
        hid_ref[:, cols] = (own_ref[:, cols].astype(F32) + dot(a_s[...], w_s[3, t])).astype(BF16)
        return 0

    lax.fori_loop(0, tiles, project_o, 0)
    a_s[...] = rms(hid_ref[...], gc_ref[layer:layer + 1, :])

    def project_cq(t, _):
        cols = pl.ds(pl.multiple_of(t * 256, 256), 256)
        copy(4, wcq, t).wait()
        q_ref[:, cols] = dot(a_s[...], w_s[4, t]).astype(BF16) * BF16(0.125)
        return 0

    lax.fori_loop(0, tiles, project_cq, 0)


def self_attention(layer, dev, own, s1, s2, s3, gs, gc, wq, wk, wv, wo, wcq):
    rows, width = own.shape
    tiles = width // 256
    shape = jax.ShapeDtypeStruct((rows, width), BF16)
    flops = 2 * rows * width * width * 11 + 4 * rows * 4 * rows * width
    return pl.pallas_call(
        functools.partial(self_kernel, layer),
        in_specs=[SMEM] + [VMEM] * 6 + [ANY] * 5,
        out_specs=[VMEM, VMEM],
        out_shape=[shape, shape],
        scratch_shapes=[
            pltpu.VMEM((5, tiles, width, 256), BF16),
            pltpu.VMEM((4 * rows, width), BF16),
            pltpu.VMEM((4 * rows, width), BF16),
            pltpu.VMEM((width, 4 * rows), BF16),
            pltpu.VMEM((rows, width), BF16),
            pltpu.VMEM((2 * rows, rows), F32),
            pltpu.VMEM((width, rows), BF16),
            pltpu.VMEM((rows, width), BF16),
            pltpu.VMEM((2, rows), F32),
            pltpu.VMEM((2, rows), F32),
            pltpu.VMEM((2, 64, rows), F32),
            pltpu.SemaphoreType.DMA((5, tiles)),
        ],
        cost_estimate=pl.CostEstimate(flops=flops, bytes_accessed=10 * width * width, transcendentals=0),
        compiler_params=pltpu.CompilerParams(vmem_limit_bytes=VMEM_LIMIT),
        name="self_attention",
    )(dev, own, s1, s2, s3, gs, gc, wq, wk, wv, wo, wcq)


def cross_kernel(layer, planes, n_kv, lim_ref, q_ref, hid_ref, gm_ref, *refs):
    ks, vts = refs[:n_kv], refs[n_kv:2 * n_kv]
    (wco, wg, wu, wd, out_ref, kbuf, vbuf, at_s, a_s, x_s, acc_o, m_s, l_s, acc_s, wo_s, wg_s, wu_s, wd_s,
     kv_sems, o_sem, w_sems) = refs[2 * n_kv:]
    rows, width = q_ref.shape
    pairs = width // 128
    steps = wg_s.shape[0]
    ff = wg_s.shape[2]

    def kv_copies(i, slot):
        cols = pl.ds(pl.multiple_of(i * 128, 128), 128)
        out, at = [], 0
        for n in range(n_kv):
            n_rows = ks[n].shape[1]
            out.append(pltpu.make_async_copy(ks[n].at[planes[n], :, cols], kbuf.at[slot, pl.ds(at, n_rows), :], kv_sems.at[slot, 0, n]))
            out.append(pltpu.make_async_copy(vts[n].at[planes[n], cols, :], vbuf.at[slot, :, pl.ds(at, n_rows)], kv_sems.at[slot, 1, n]))
            at += n_rows
        return out

    def w_copies(j):
        cols = pl.ds(pl.multiple_of(j * ff, ff), ff)
        return (pltpu.make_async_copy(wg.at[layer, :, cols], wg_s.at[j], w_sems.at[0, j]),
                pltpu.make_async_copy(wu.at[layer, :, cols], wu_s.at[j], w_sems.at[1, j]),
                pltpu.make_async_copy(wd.at[layer, cols, :], wd_s.at[j], w_sems.at[2, j]))

    for cp in kv_copies(0, 0):
        cp.start()
    o_copy = pltpu.make_async_copy(wco.at[layer], wo_s, o_sem)

    def pair_step(i, _):
        slot = lax.rem(i, 2)

        @pl.when(i + 1 < pairs)
        def _():
            for cp in kv_copies(i + 1, 1 - slot):
                cp.start()

        @pl.when(i == 0)
        def _():
            o_copy.start()

        @pl.when(i < steps)
        def _():
            for cp in w_copies(i):
                cp.start()

        for cp in kv_copies(i, slot):
            cp.wait()
        cols = pl.ds(pl.multiple_of(i * 128, 128), 128)
        q_pair = pair_queries(q_ref[:, cols])
        attend_init(m_s, l_s, acc_s)

        def chunk_step(c, _):
            at = pl.ds(pl.multiple_of(c * CH, CH), CH)
            lim = lim_ref[c]

            @pl.when(lim >= CH)
            def _():
                attend_chunk(kbuf[slot, at, :], vbuf[slot, :, at], q_pair, m_s, l_s, acc_s, lambda s: s)

            @pl.when((lim > 0) & (lim < CH))
            def _():
                def fix(s):
                    row = lax.broadcasted_iota(jnp.int32, s.shape, 0)
                    return jnp.where(row < lim, s, NEG_BIG)
                attend_chunk(kbuf[slot, at, :], vbuf[slot, :, at], q_pair, m_s, l_s, acc_s, fix)
            return 0

        lax.fori_loop(0, lim_ref.shape[0], chunk_step, 0)
        attend_finish(at_s, i, l_s, acc_s)
        return 0

    lax.fori_loop(0, pairs, pair_step, 0)

    a_s[...] = at_s[...].T
    o_copy.wait()

    def project_o(t, _):
        cols = pl.ds(pl.multiple_of(t * 256, 256), 256)
        out_ref[:, cols] = (hid_ref[:, cols].astype(F32) + dot(a_s[...], wo_s[:, cols])).astype(BF16)
        return 0

    lax.fori_loop(0, width // 256, project_o, 0)
    x_s[...] = rms(out_ref[...], gm_ref[layer:layer + 1, :])
    acc_o[...] = jnp.zeros_like(acc_o)

    def mlp_step(j, _):
        for cp in w_copies(j):
            cp.wait()
        x = x_s[...]
        gate = dot(x, wg_s[j])
        up = dot(x, wu_s[j])
        act = (gate / (1.0 + jnp.exp(-gate)) * up).astype(BF16)
        acc_o[...] += dot(act, wd_s[j])
        return 0

    lax.fori_loop(0, steps, mlp_step, 0)
    out_ref[...] = (out_ref[...].astype(F32) + acc_o[...]).astype(BF16)


def cross_mlp(layer, lims, q, hid, gm, kvs, wco, wg, wu, wd):
    rows, width = q.shape
    steps = 10
    ff = wg.shape[2] // steps
    planes = tuple(plane for _, _, plane in kvs)
    ks, vts = [k for k, _, _ in kvs], [v for _, v, _ in kvs]
    total = sum(k.shape[1] for k in ks)
    n = len(kvs)
    flops = 2 * rows * width * (width + 3 * wg.shape[2]) + 4 * rows * 3072 * width
    return pl.pallas_call(
        functools.partial(cross_kernel, layer, planes, n),
        in_specs=[SMEM, VMEM, VMEM, VMEM] + [ANY] * (2 * n + 4),
        out_specs=VMEM,
        out_shape=jax.ShapeDtypeStruct((rows, width), BF16),
        scratch_shapes=[
            pltpu.VMEM((2, total, 128), BF16),
            pltpu.VMEM((2, 128, total), BF16),
            pltpu.VMEM((width, rows), BF16),
            pltpu.VMEM((rows, width), BF16),
            pltpu.VMEM((rows, width), BF16),
            pltpu.VMEM((rows, width), F32),
            pltpu.VMEM((2, rows), F32),
            pltpu.VMEM((2, rows), F32),
            pltpu.VMEM((2, 64, rows), F32),
            pltpu.VMEM((width, width), BF16),
            pltpu.VMEM((steps, width, ff), BF16),
            pltpu.VMEM((steps, width, ff), BF16),
            pltpu.VMEM((steps, ff, width), BF16),
            pltpu.SemaphoreType.DMA((2, 2, n)),
            pltpu.SemaphoreType.DMA,
            pltpu.SemaphoreType.DMA((3, steps)),
        ],
        cost_estimate=pl.CostEstimate(flops=flops, bytes_accessed=2 * width * (width + 3 * wg.shape[2]), transcendentals=0),
        compiler_params=pltpu.CompilerParams(vmem_limit_bytes=VMEM_LIMIT),
        name="cross_mlp",
    )(lims, q, hid, gm, *ks, *vts, wco, wg, wu, wd)


NONE = 1 << 20
BASES = (
    (0, 512, 1024, 1536, 2048, NONE, NONE, 2560),
    (1024, 1536, 0, 512, NONE, 2048, 2560, NONE),
    (2048, NONE, 2560, NONE, 0, 1024, 512, 1536),
    (2560, NONE, 2048, NONE, 1024, 0, 1536, 512),
)


def solution(mesh):
    row_spec = P(('dp', 'sp'), None)

    def local_step(hidden, memory, mem_len, norm_self, norm_cross, norm_mlp, self_q, self_k, self_v, self_o, cross_q, cross_k, cross_v, cross_o, mlp_gate, mlp_up, mlp_down):
        layers, width = norm_self.shape
        w_so = self_o.reshape(layers, width, width)
        w_co = cross_o.reshape(layers, width, width)
        dev = lax.axis_index('sp')
        dev_arr = dev.astype(jnp.int32).reshape(1)
        bases = jnp.array(BASES, jnp.int32)[dev]
        lims = jnp.clip(mem_len[0] - bases, 0, CH)
        is3 = (dev_arr == 3).astype(jnp.int32)

        def swap(x):
            return lax.ppermute(x, 'sp', [(0, 1), (1, 0), (2, 3), (3, 2)])

        def earlier_rows(h):
            s1 = lax.ppermute(h, 'sp', [(0, 1), (2, 3)])
            s2 = lax.ppermute(h, 'sp', [(0, 2), (1, 3)])
            s3 = lax.ppermute(s2, 'sp', [(2, 3), (3, 2)])
            return s1, s2, s3

        blocks = earlier_rows(hidden)
        mem_a, mem_b = memory[:CH], memory[CH:]
        c2b = lax.ppermute(mem_b, 'sp', [(2, 3)])
        rem_a = lax.ppermute(mem_a, 'sp', [(0, 2), (1, 3), (2, 0)])
        rem_b = lax.ppermute(mem_b, 'sp', [(0, 2), (1, 3), (2, 1)])

        both = (0, layers)
        ka, va = kv_project(lims[0:2], is3, [memory, c2b], cross_k, cross_v, 2 * CH, both)
        kas, vas = swap(ka), swap(va)
        kvs = []
        for layer in range(layers):
            kvs.append([(ka, va, layer), (kas, vas, layer)])
        for layer in range(layers):
            for rem, at in ((rem_a, 4), (rem_b, 6)):
                k, v = kv_project(lims[at:at + 1], is3, [rem], cross_k, cross_v, CH, (layer, 1))
                kvs[layer] += [(k, v, 0), (swap(k), swap(v), 0)]

        for layer in range(layers):
            hidden, q = self_attention(layer, dev_arr, hidden, *blocks, norm_self, norm_cross, self_q, self_k, self_v, w_so, cross_q)
            hidden = cross_mlp(layer, lims, q, hidden, norm_mlp, kvs[layer], w_co, mlp_gate, mlp_up, mlp_down)
            if layer + 1 < layers:
                blocks = earlier_rows(hidden)
        return hidden

    return jax.shard_map(local_step, mesh=mesh, in_specs=(row_spec, row_spec, P('dp')) + (P(),) * 14, out_specs=row_spec, check_vma=False)
```

```python
import functools

import jax
import jax.numpy as jnp
from jax import lax
from jax.experimental import pallas as pl
from jax.experimental.pallas import tpu as pltpu
from jax.sharding import PartitionSpec as P


EPS = 1e-6
NEG_BIG = -1e30
F32 = jnp.float32
BF16 = jnp.bfloat16
CH = 512
VMEM_LIMIT = 62 * 1024 * 1024
ANY = pl.BlockSpec(memory_space=pl.ANY)
SMEM = pl.BlockSpec(memory_space=pltpu.SMEM)
VMEM = pl.BlockSpec(memory_space=pltpu.VMEM)


def rms(h, gain):
    h32 = h.astype(F32)
    inv = lax.rsqrt(jnp.mean(h32 * h32, axis=-1, keepdims=True) + EPS)
    return (h32 * inv * gain.astype(F32)).astype(BF16)


def dot(a, b):
    return jnp.dot(a, b, preferred_element_type=F32)


def dot_nt(a, b):
    return lax.dot_general(a, b, (((1,), (1,)), ((), ())), preferred_element_type=F32)


def kv_kernel(layers, n_src, lim_ref, pick_ref, *refs):
    srcs, (wk, wv, k_out, vt_out, mem, w_s, k_s, vt_s, sem, w_sems, o_sems) = refs[:n_src], refs[n_src:]
    rows = mem.shape[0]
    lo, n = layers

    def from_src(go):
        if n_src == 1:
            go(pltpu.make_async_copy(srcs[0], mem, sem))
        else:
            @pl.when(pick_ref[0] == 0)
            def _():
                go(pltpu.make_async_copy(srcs[0], mem, sem))

            @pl.when(pick_ref[0] != 0)
            def _():
                go(pltpu.make_async_copy(srcs[1], mem.at[pl.ds(0, CH)], sem))

    w_copies = []
    for i in range(n):
        for v, src in enumerate((wk, wv)):
            w_copies.append(pltpu.make_async_copy(src.at[lo + i], w_s.at[2 * i + v], w_sems.at[2 * i + v]))
    w_copies[0].start()
    from_src(lambda cp: cp.start())
    for cp in w_copies[1:]:
        cp.start()
    from_src(lambda cp: cp.wait())

    def out_copy(i, v, c):
        at = pl.ds(c * CH, CH)
        if v == 0:
            return pltpu.make_async_copy(k_s.at[i, at, :], k_out.at[i, at, :], o_sems.at[i, v, c])
        return pltpu.make_async_copy(vt_s.at[i, :, at], vt_out.at[i, :, at], o_sems.at[i, v, c])

    for i in range(n):
        for v in range(2):
            w_copies[2 * i + v].wait()
            for c in range(rows // CH):
                @pl.when(lim_ref[c] > 0)
                def _(i=i, v=v, c=c):
                    def step(r, _):
                        at = pl.ds(pl.multiple_of(c * CH + r * 256, 256), 256)
                        out = dot(mem[at, :], w_s[2 * i + v]).astype(BF16)
                        if v == 0:
                            k_s[i, at, :] = out
                        else:
                            vt_s[i, :, at] = out.T
                        return 0

                    lax.fori_loop(0, CH // 256, step, 0)
                    out_copy(i, v, c).start()
    for i in range(n):
        for v in range(2):
            for c in range(rows // CH):
                @pl.when(lim_ref[c] > 0)
                def _(i=i, v=v, c=c):
                    out_copy(i, v, c).wait()


def kv_project(lims, pick, srcs, wk, wv, rows, layers):
    width, cols = wk.shape[1], wk.shape[2]
    n = layers[1]
    flops = n * 4 * rows * width * cols
    return pl.pallas_call(
        functools.partial(kv_kernel, layers, len(srcs)),
        in_specs=[SMEM, SMEM] + [ANY] * (len(srcs) + 2),
        out_specs=[ANY, ANY],
        out_shape=[jax.ShapeDtypeStruct((n, rows, cols), BF16), jax.ShapeDtypeStruct((n, cols, rows), BF16)],
        scratch_shapes=[
            pltpu.VMEM((rows, width), BF16),
            pltpu.VMEM((2 * n, width, cols), BF16),
            pltpu.VMEM((n, rows, cols), BF16),
            pltpu.VMEM((n, cols, rows), BF16),
            pltpu.SemaphoreType.DMA,
            pltpu.SemaphoreType.DMA((2 * n,)),
            pltpu.SemaphoreType.DMA((n, 2, rows // CH)),
        ],
        cost_estimate=pl.CostEstimate(flops=flops, bytes_accessed=n * 4 * width * cols, transcendentals=0),
        compiler_params=pltpu.CompilerParams(vmem_limit_bytes=48 * 1024 * 1024),
        name="kv_project",
    )(lims, pick, *srcs, wk, wv)


def pair_queries(q):
    lane = lax.broadcasted_iota(jnp.int32, q.shape, 1)
    zero = jnp.zeros_like(q)
    return jnp.where(lane < 64, q, zero), jnp.where(lane < 64, zero, q)


def attend_all(pairs, n_chunks, scores, values, enter, at_ref, s_refs, mx_refs, m_ref, l_ref, acc_ref):
    def stage1(pair, j, buf):
        for h, s in enumerate(scores(pair, j)):
            s_refs[buf][h] = s
            mx_refs[buf][h:h + 1, :] = jnp.max(s, axis=0, keepdims=True)

    def stage2(pair, j, buf):
        vt = values(pair, j)
        for h in range(2):
            m_old = m_ref[h:h + 1, :]
            m_new = jnp.maximum(m_old, mx_refs[buf][h:h + 1, :])
            p = jnp.exp(s_refs[buf][h] - m_new)
            alpha = jnp.exp(m_old - m_new)
            m_ref[h:h + 1, :] = m_new
            l_ref[h:h + 1, :] = l_ref[h:h + 1, :] * alpha + jnp.sum(p, axis=0, keepdims=True)
            acc_ref[h] = acc_ref[h] * alpha + dot(vt[h * 64:(h + 1) * 64, :], p.astype(BF16))

    def advance(pair, j):
        wrap = j + 1 == n_chunks
        return jnp.where(wrap, pair + 1, pair), jnp.where(wrap, 0, j + 1)

    enter(0)
    stage1(0, 0, 0)

    def step(_, now):
        pair, j = now
        for buf in range(2):
            pair_next, j_next = advance(pair, j)

            @pl.when(j == 0)
            def _():
                m_ref[...] = jnp.full_like(m_ref, -jnp.inf)
                l_ref[...] = jnp.zeros_like(l_ref)
                acc_ref[...] = jnp.zeros_like(acc_ref)

            @pl.when((j_next == 0) & (pair_next < pairs))
            def _(pair_next=pair_next):
                enter(pair_next)

            stage1(jnp.minimum(pair_next, pairs - 1), j_next, 1 - buf)
            stage2(pair, j, buf)

            @pl.when(j_next == 0)
            def _(pair=pair):
                for h in range(2):
                    rows = pl.ds(pl.multiple_of(pair * 128 + h * 64, 64), 64)
                    at_ref[rows, :] = (acc_ref[h] / l_ref[h:h + 1, :]).astype(BF16)

            pair, j = pair_next, j_next
        return pair, j

    lax.fori_loop(0, pairs * n_chunks // 2, step, (jnp.int32(0), jnp.int32(0)))


def attend_scratch(rows):
    return [pltpu.VMEM((2, CH, rows), F32)] * 2 + [pltpu.VMEM((2, rows), F32)] * 4 + [pltpu.VMEM((2, 64, rows), F32)]


def self_kernel(layer, dev_ref, own_ref, s1_ref, s2_ref, s3_ref, gs_ref, gc_ref, wq, wk, wv, wo, wcq, hid_ref, q_ref,
                w_s, x_s, k_s, vt_s, qs, bias, at_s, a_s, s0, s1, mx0, mx1, m_s, l_s, acc_s, sems):
    rows, width = own_ref.shape
    tiles = width // 256
    dev = dev_ref[0]
    chip1 = dev >= 2

    w_copies = [pltpu.make_async_copy(src.at[layer], w_s.at[n], sems.at[n]) for n, src in enumerate((wk, wv, wq, wo, wcq))]
    w_copies[0].start()
    w_copies[1].start()

    gain = gs_ref[layer:layer + 1, :]
    x_s[pl.ds(0, rows), :] = rms(own_ref[...], gain)
    x_s[pl.ds(rows, rows), :] = rms(s1_ref[...], gain)

    @pl.when(chip1)
    def _():
        x_s[pl.ds(2 * rows, rows), :] = rms(s2_ref[...], gain)
        x_s[pl.ds(3 * rows, rows), :] = rms(s3_ref[...], gain)

    key = lax.broadcasted_iota(jnp.int32, (rows, rows), 0)
    query = lax.broadcasted_iota(jnp.int32, (rows, rows), 1)
    bias[pl.ds(0, rows), :] = jnp.where(key <= query, 0.0, NEG_BIG)
    bias[pl.ds(rows, rows), :] = jnp.full((rows, rows), jnp.where(dev % 2 == 1, 0.0, NEG_BIG), F32)
    bias[pl.ds(2 * rows, 2 * rows), :] = jnp.zeros((2 * rows, rows), F32)

    def tile(t):
        return pl.ds(pl.multiple_of(t * 256, 256), 256)

    def project(n, store):
        w_copies[n].wait()
        if n + 2 < len(w_copies):
            w_copies[n + 2].start()

        def step(r, _):
            at = tile(r)
            store(at, dot(x_s[at, :], w_s[n]).astype(BF16))
            return 0

        lax.fori_loop(0, jnp.where(chip1, 4, 2), step, 0)

    def store_k(at, out):
        k_s[at, :] = out

    def store_v(at, out):
        vt_s[:, at] = out.T

    project(0, store_k)
    project(1, store_v)
    w_copies[2].wait()
    w_copies[4].start()
    qs[...] = dot(x_s[pl.ds(0, rows), :], w_s[2]).astype(BF16) * BF16(0.125)

    def chunk(j):
        return pl.ds(pl.multiple_of(j * CH, CH), CH)

    def head_cols(i):
        return pl.ds(pl.multiple_of(i * 128, 128), 128)

    def scores(i, j):
        k = k_s[chunk(j), head_cols(i)]
        return [dot_nt(k, q) + bias[chunk(j), :] for q in pair_queries(qs[:, head_cols(i)])]

    def values(i, j):
        return vt_s[head_cols(i), chunk(j)]

    attend_all(width // 128, jnp.where(chip1, 2, 1), scores, values, lambda i: None, at_s, (s0, s1), (mx0, mx1), m_s, l_s, acc_s)

    a_s[...] = at_s[...].T
    w_copies[3].wait()

    def project_o(t, _):
        cols = tile(t)
        hid_ref[:, cols] = (own_ref[:, cols].astype(F32) + dot(a_s[...], w_s[3, :, cols])).astype(BF16)
        return 0

    lax.fori_loop(0, tiles, project_o, 0)
    a_s[...] = rms(hid_ref[...], gc_ref[layer:layer + 1, :])
    w_copies[4].wait()

    def project_cq(t, _):
        cols = tile(t)
        q_ref[:, cols] = dot(a_s[...], w_s[4, :, cols]).astype(BF16) * BF16(0.125)
        return 0

    lax.fori_loop(0, tiles, project_cq, 0)


def self_attention(layer, dev, own, s1, s2, s3, gs, gc, wq, wk, wv, wo, wcq):
    rows, width = own.shape
    shape = jax.ShapeDtypeStruct((rows, width), BF16)
    flops = 2 * rows * width * width * 11 + 4 * rows * 4 * rows * width
    return pl.pallas_call(
        functools.partial(self_kernel, layer),
        in_specs=[SMEM] + [VMEM] * 6 + [ANY] * 5,
        out_specs=[VMEM, VMEM],
        out_shape=[shape, shape],
        scratch_shapes=[
            pltpu.VMEM((5, width, width), BF16),
            pltpu.VMEM((4 * rows, width), BF16),
            pltpu.VMEM((4 * rows, width), BF16),
            pltpu.VMEM((width, 4 * rows), BF16),
            pltpu.VMEM((rows, width), BF16),
            pltpu.VMEM((4 * rows, rows), F32),
            pltpu.VMEM((width, rows), BF16),
            pltpu.VMEM((rows, width), BF16),
            *attend_scratch(rows),
            pltpu.SemaphoreType.DMA((5,)),
        ],
        cost_estimate=pl.CostEstimate(flops=flops, bytes_accessed=10 * width * width, transcendentals=0),
        compiler_params=pltpu.CompilerParams(vmem_limit_bytes=VMEM_LIMIT),
        name="self_attention",
    )(dev, own, s1, s2, s3, gs, gc, wq, wk, wv, wo, wcq)


def cross_kernel(layer, planes, n_kv, lim_ref, q_ref, hid_ref, gm_ref, *refs):
    ks, vts = refs[:n_kv], refs[n_kv:2 * n_kv]
    (wco, wg, wu, wd, out_ref, kbuf, vbuf, at_s, a_s, x_s, acc_o, s0, s1, mx0, mx1, m_s, l_s, acc_s, mask, list_s,
     wo_s, wg_s, wu_s, wd_s, kv_sems, o_sem, w_sems) = refs[2 * n_kv:]
    rows, width = q_ref.shape
    pairs = width // 128
    steps = wg_s.shape[0]
    ff = wg_s.shape[2]

    def kv_copies(i, slot):
        cols = pl.ds(pl.multiple_of(i * 128, 128), 128)
        out, at = [], 0
        for n in range(n_kv):
            n_rows = ks[n].shape[1]
            out.append(pltpu.make_async_copy(ks[n].at[planes[n], :, cols], kbuf.at[slot, pl.ds(at, n_rows), :], kv_sems.at[slot, 0, n]))
            out.append(pltpu.make_async_copy(vts[n].at[planes[n], cols, :], vbuf.at[slot, :, pl.ds(at, n_rows)], kv_sems.at[slot, 1, n]))
            at += n_rows
        return out

    def w_copies(j):
        cols = pl.ds(pl.multiple_of(j * ff, ff), ff)
        return (pltpu.make_async_copy(wg.at[layer, :, cols], wg_s.at[j], w_sems.at[0, j]),
                pltpu.make_async_copy(wu.at[layer, :, cols], wu_s.at[j], w_sems.at[1, j]),
                pltpu.make_async_copy(wd.at[layer, cols, :], wd_s.at[j], w_sems.at[2, j]))

    for cp in kv_copies(0, 0):
        cp.start()
    o_copy = pltpu.make_async_copy(wco.at[layer], wo_s, o_sem)

    n_chunks, last = jnp.int32(0), jnp.int32(0)
    for c in range(lim_ref.shape[0]):
        lim = lim_ref[c]

        @pl.when(lim > 0)
        def _(c=c, at=n_chunks):
            list_s[at] = c

        n_chunks = n_chunks + (lim > 0).astype(jnp.int32)
        last = last + jnp.where(lim < CH, lim, 0)
    key = lax.broadcasted_iota(jnp.int32, (CH, 128), 0)
    lane = lax.broadcasted_iota(jnp.int32, (CH, 128), 1)
    mask[0] = jnp.zeros((CH, 128), BF16)
    mask[1] = jnp.where((key >= last) & (lane == 0), NEG_BIG, 0.0).astype(BF16)
    ones = (lax.broadcasted_iota(jnp.int32, (rows, 128), 1) == 0).astype(F32).astype(BF16)

    def enter(i):
        @pl.when(i + 1 < pairs)
        def _():
            for cp in kv_copies(i + 1, lax.rem(i + 1, 3)):
                cp.start()

        @pl.when(i == 0)
        def _():
            o_copy.start()

        @pl.when(i < steps)
        def _():
            for cp in w_copies(i):
                cp.start()

        for cp in kv_copies(i, lax.rem(i, 3)):
            cp.wait()

    def chunk(j):
        return pl.ds(pl.multiple_of(list_s[j] * CH, CH), CH)

    def scores(i, j):
        k = kbuf[lax.rem(i, 3), chunk(j), :]
        partial = (lim_ref[list_s[j]] < CH).astype(jnp.int32)
        cols = pl.ds(pl.multiple_of(i * 128, 128), 128)
        k = jnp.concatenate([k, mask[partial]], axis=1)
        return [dot_nt(k, jnp.concatenate([q, ones], axis=1)) for q in pair_queries(q_ref[:, cols])]

    def values(i, j):
        return vbuf[lax.rem(i, 3), :, chunk(j)]

    attend_all(pairs, n_chunks, scores, values, enter, at_s, (s0, s1), (mx0, mx1), m_s, l_s, acc_s)

    a_s[...] = at_s[...].T
    o_copy.wait()

    def project_o(t, _):
        cols = pl.ds(pl.multiple_of(t * 256, 256), 256)
        out_ref[:, cols] = (hid_ref[:, cols].astype(F32) + dot(a_s[...], wo_s[:, cols])).astype(BF16)
        return 0

    lax.fori_loop(0, width // 256, project_o, 0)
    x_s[...] = rms(out_ref[...], gm_ref[layer:layer + 1, :])
    acc_o[...] = jnp.zeros_like(acc_o)

    def mlp_step(j, _):
        for cp in w_copies(j):
            cp.wait()
        x = x_s[...]
        gate = dot(x, wg_s[j])
        up = dot(x, wu_s[j])
        act = (gate / (1.0 + jnp.exp(-gate)) * up).astype(BF16)
        acc_o[...] += dot(act, wd_s[j])
        return 0

    lax.fori_loop(0, steps, mlp_step, 0)
    out_ref[...] = (out_ref[...].astype(F32) + acc_o[...]).astype(BF16)


def cross_mlp(layer, lims, q, hid, gm, kvs, wco, wg, wu, wd):
    rows, width = q.shape
    steps = 10
    ff = wg.shape[2] // steps
    planes = tuple(plane for _, _, plane in kvs)
    ks, vts = [k for k, _, _ in kvs], [v for _, v, _ in kvs]
    total = sum(k.shape[1] for k in ks)
    n = len(kvs)
    flops = 2 * rows * width * (width + 3 * wg.shape[2]) + 4 * rows * 3072 * width
    return pl.pallas_call(
        functools.partial(cross_kernel, layer, planes, n),
        in_specs=[SMEM, VMEM, VMEM, VMEM] + [ANY] * (2 * n + 4),
        out_specs=VMEM,
        out_shape=jax.ShapeDtypeStruct((rows, width), BF16),
        scratch_shapes=[
            pltpu.VMEM((3, total, 128), BF16),
            pltpu.VMEM((3, 128, total), BF16),
            pltpu.VMEM((width, rows), BF16),
            pltpu.VMEM((rows, width), BF16),
            pltpu.VMEM((rows, width), BF16),
            pltpu.VMEM((rows, width), F32),
            *attend_scratch(rows),
            pltpu.VMEM((2, CH, 128), BF16),
            pltpu.SMEM((8,), jnp.int32),
            pltpu.VMEM((width, width), BF16),
            pltpu.VMEM((steps, width, ff), BF16),
            pltpu.VMEM((steps, width, ff), BF16),
            pltpu.VMEM((steps, ff, width), BF16),
            pltpu.SemaphoreType.DMA((3, 2, n)),
            pltpu.SemaphoreType.DMA,
            pltpu.SemaphoreType.DMA((3, steps)),
        ],
        cost_estimate=pl.CostEstimate(flops=flops, bytes_accessed=2 * width * (width + 3 * wg.shape[2]), transcendentals=0),
        compiler_params=pltpu.CompilerParams(vmem_limit_bytes=VMEM_LIMIT),
        name="cross_mlp",
    )(lims, q, hid, gm, *ks, *vts, wco, wg, wu, wd)


NONE = 1 << 20
BASES = (
    (0, 512, 1024, 1536, 2048, NONE, NONE, 2560),
    (1024, 1536, 0, 512, NONE, 2048, 2560, NONE),
    (2048, NONE, 2560, NONE, 0, 1024, 512, 1536),
    (2560, NONE, 2048, NONE, 1024, 0, 1536, 512),
)


def solution(mesh):
    row_spec = P(('dp', 'sp'), None)

    def local_step(hidden, memory, mem_len, norm_self, norm_cross, norm_mlp, self_q, self_k, self_v, self_o, cross_q, cross_k, cross_v, cross_o, mlp_gate, mlp_up, mlp_down):
        layers, width = norm_self.shape
        w_so = self_o.reshape(layers, width, width)
        w_co = cross_o.reshape(layers, width, width)
        dev = lax.axis_index('sp')
        dev_arr = dev.astype(jnp.int32).reshape(1)
        bases = jnp.array(BASES, jnp.int32)[dev]
        lims = jnp.clip(mem_len[0] - bases, 0, CH)
        is3 = (dev_arr == 3).astype(jnp.int32)

        def swap(x):
            return lax.ppermute(x, 'sp', [(0, 1), (1, 0), (2, 3), (3, 2)])

        def earlier_rows(h):
            s2 = lax.ppermute(h, 'sp', [(0, 2), (1, 3)])
            s1 = lax.ppermute(h, 'sp', [(0, 1), (2, 3)])
            s3 = lax.ppermute(s2, 'sp', [(2, 3), (3, 2)])
            return s1, s2, s3

        def program(hidden):
            blocks = earlier_rows(hidden)
            mem_a, mem_b = memory[:CH], memory[CH:]
            c2b = lax.ppermute(mem_b, 'sp', [(2, 3)])
            rem_a = lax.ppermute(mem_a, 'sp', [(0, 2), (1, 3), (2, 0)])
            rem_b = lax.ppermute(mem_b, 'sp', [(0, 2), (1, 3), (2, 1)])

            both = (0, layers)
            ka, va = kv_project(lims[0:2], is3, [memory, c2b], cross_k, cross_v, 2 * CH, both)
            kas, vas = swap(ka), swap(va)
            kvs = []
            for layer in range(layers):
                kvs.append([(ka, va, layer), (kas, vas, layer)])
            for layer in range(layers):
                for rem, at in ((rem_a, 4), (rem_b, 6)):
                    k, v = kv_project(lims[at:at + 1], is3, [rem], cross_k, cross_v, CH, (layer, 1))
                    kvs[layer] += [(k, v, 0), (swap(k), swap(v), 0)]

            for layer in range(layers):
                hidden, q = self_attention(layer, dev_arr, hidden, *blocks, norm_self, norm_cross, self_q, self_k, self_v, w_so, cross_q)
                hidden = cross_mlp(layer, lims, q, hidden, norm_mlp, kvs[layer], w_co, mlp_gate, mlp_up, mlp_down)
                if layer + 1 < layers:
                    blocks = earlier_rows(hidden)
            return hidden

        return program(hidden)

    return jax.shard_map(local_step, mesh=mesh, in_specs=(row_spec, row_spec, P('dp')) + (P(),) * 14, out_specs=row_spec, check_vma=False)
```

```python
import functools

import jax
import jax.numpy as jnp
from jax import lax
from jax.experimental import pallas as pl
from jax.experimental.pallas import tpu as pltpu
from jax.sharding import PartitionSpec as P


EPS = 1e-6
NEG_BIG = -1e30
F32 = jnp.float32
BF16 = jnp.bfloat16
CH = 512
VMEM_LIMIT = 62 * 1024 * 1024
ANY = pl.BlockSpec(memory_space=pl.ANY)
SMEM = pl.BlockSpec(memory_space=pltpu.SMEM)
VMEM = pl.BlockSpec(memory_space=pltpu.VMEM)


def rms(h, gain):
    h32 = h.astype(F32)
    inv = lax.rsqrt(jnp.mean(h32 * h32, axis=-1, keepdims=True) + EPS)
    return (h32 * inv * gain.astype(F32)).astype(BF16)


def dot(a, b):
    return jnp.dot(a, b, preferred_element_type=F32)


def dot_nt(a, b):
    return lax.dot_general(a, b, (((1,), (1,)), ((), ())), preferred_element_type=F32)


def kv_kernel(layers, n_src, lim_ref, pick_ref, *refs):
    srcs, (wk, wv, k_out, vt_out, mem, w_s, k_s, vt_s, sem, w_sems, o_sems) = refs[:n_src], refs[n_src:]
    rows = mem.shape[0]
    lo, n = layers

    def from_src(go):
        if n_src == 1:
            go(pltpu.make_async_copy(srcs[0], mem, sem))
        else:
            @pl.when(pick_ref[0] == 0)
            def _():
                go(pltpu.make_async_copy(srcs[0], mem, sem))

            @pl.when(pick_ref[0] != 0)
            def _():
                go(pltpu.make_async_copy(srcs[1], mem.at[pl.ds(0, CH)], sem))

    w_copies = []
    for i in range(n):
        for v, src in enumerate((wk, wv)):
            w_copies.append(pltpu.make_async_copy(src.at[lo + i], w_s.at[2 * i + v], w_sems.at[2 * i + v]))
    w_copies[0].start()
    from_src(lambda cp: cp.start())
    for cp in w_copies[1:]:
        cp.start()
    from_src(lambda cp: cp.wait())

    def out_copy(i, v, c):
        at = pl.ds(c * CH, CH)
        if v == 0:
            return pltpu.make_async_copy(k_s.at[i, at, :], k_out.at[i, at, :], o_sems.at[i, v, c])
        return pltpu.make_async_copy(vt_s.at[i, :, at], vt_out.at[i, :, at], o_sems.at[i, v, c])

    for i in range(n):
        for v in range(2):
            w_copies[2 * i + v].wait()
            for c in range(rows // CH):
                @pl.when(lim_ref[c] > 0)
                def _(i=i, v=v, c=c):
                    def step(r, _):
                        at = pl.ds(pl.multiple_of(c * CH + r * 256, 256), 256)
                        out = dot(mem[at, :], w_s[2 * i + v]).astype(BF16)
                        if v == 0:
                            k_s[i, at, :] = out
                        else:
                            vt_s[i, :, at] = out.T
                        return 0

                    lax.fori_loop(0, CH // 256, step, 0)
                    out_copy(i, v, c).start()
    for i in range(n):
        for v in range(2):
            for c in range(rows // CH):
                @pl.when(lim_ref[c] > 0)
                def _(i=i, v=v, c=c):
                    out_copy(i, v, c).wait()


def kv_project(lims, pick, srcs, wk, wv, rows, layers):
    width, cols = wk.shape[1], wk.shape[2]
    n = layers[1]
    flops = n * 4 * rows * width * cols
    return pl.pallas_call(
        functools.partial(kv_kernel, layers, len(srcs)),
        in_specs=[SMEM, SMEM] + [ANY] * (len(srcs) + 2),
        out_specs=[ANY, ANY],
        out_shape=[jax.ShapeDtypeStruct((n, rows, cols), BF16), jax.ShapeDtypeStruct((n, cols, rows), BF16)],
        scratch_shapes=[
            pltpu.VMEM((rows, width), BF16),
            pltpu.VMEM((2 * n, width, cols), BF16),
            pltpu.VMEM((n, rows, cols), BF16),
            pltpu.VMEM((n, cols, rows), BF16),
            pltpu.SemaphoreType.DMA,
            pltpu.SemaphoreType.DMA((2 * n,)),
            pltpu.SemaphoreType.DMA((n, 2, rows // CH)),
        ],
        cost_estimate=pl.CostEstimate(flops=flops, bytes_accessed=n * 4 * width * cols, transcendentals=0),
        compiler_params=pltpu.CompilerParams(vmem_limit_bytes=48 * 1024 * 1024),
        name="kv_project",
    )(lims, pick, *srcs, wk, wv)


def pair_queries(q):
    lane = lax.broadcasted_iota(jnp.int32, q.shape, 1)
    zero = jnp.zeros_like(q)
    return jnp.where(lane < 64, q, zero), jnp.where(lane < 64, zero, q)


def attend_all(pairs, n_chunks, scores, values, enter, leave, scratch):
    s_refs, mx_refs, (m_ref, l_ref, acc_ref) = scratch[:2], scratch[2:4], scratch[4:]

    def stage1(pair, j, buf):
        for h, s in enumerate(scores(pair, j)):
            s_refs[buf][h] = s
            mx_refs[buf][h:h + 1, :] = jnp.max(s, axis=0, keepdims=True)

    def stage2(pair, j, buf):
        vt = values(pair, j)
        for h in range(2):
            m_old = m_ref[pair, h:h + 1, :]
            m_new = jnp.maximum(m_old, mx_refs[buf][h:h + 1, :])
            p = jnp.exp(s_refs[buf][h] - m_new)
            alpha = jnp.exp(m_old - m_new)
            m_ref[pair, h:h + 1, :] = m_new
            l_ref[pair, h:h + 1, :] = l_ref[pair, h:h + 1, :] * alpha + jnp.sum(p, axis=0, keepdims=True)
            acc_ref[pair, h] = acc_ref[pair, h] * alpha + dot(vt[h * 64:(h + 1) * 64, :], p.astype(BF16))

    def advance(pair, j):
        wrap = j + 1 == n_chunks
        return jnp.where(wrap, pair + 1, pair), jnp.where(wrap, 0, j + 1)

    enter(0)
    stage1(0, 0, 0)

    def step(_, now):
        pair, j = now
        for buf in range(2):
            pair_next, j_next = advance(pair, j)

            @pl.when((j_next == 0) & (pair_next < pairs))
            def _(pair_next=pair_next):
                enter(pair_next)

            stage1(jnp.minimum(pair_next, pairs - 1), j_next, 1 - buf)
            stage2(pair, j, buf)

            @pl.when(j_next == 0)
            def _(pair=pair):
                leave(pair)

            pair, j = pair_next, j_next
        return pair, j

    lax.fori_loop(0, pairs * n_chunks // 2, step, (jnp.int32(0), jnp.int32(0)))


def attend_reset(scratch):
    m_ref, l_ref, acc_ref = scratch[4:]
    m_ref[...] = jnp.full_like(m_ref, -jnp.inf)
    l_ref[...] = jnp.zeros_like(l_ref)
    acc_ref[...] = jnp.zeros_like(acc_ref)


def attend_finish(pair, at_ref, scratch):
    l_ref, acc_ref = scratch[5:]
    for h in range(2):
        rows = pl.ds(pl.multiple_of(pair * 128 + h * 64, 64), 64)
        at_ref[rows, :] = (acc_ref[pair, h] / l_ref[pair, h:h + 1, :]).astype(BF16)


def attend_scratch(pairs, rows):
    return [
        pltpu.VMEM((2, CH, rows), F32),
        pltpu.VMEM((2, CH, rows), F32),
        pltpu.VMEM((2, rows), F32),
        pltpu.VMEM((2, rows), F32),
        pltpu.VMEM((pairs, 2, rows), F32),
        pltpu.VMEM((pairs, 2, rows), F32),
        pltpu.VMEM((pairs, 2, 64, rows), F32),
    ]


def self_kernel(layer, far_given, *refs):
    own_ref, refs = refs[0], refs[1:]
    if far_given:
        s2, refs = refs[0], refs[1:]
    gs_ref, gc_ref, wq, wk, wv, wo, wcq, hid_ref, q_ref, w_s, x_s, k_s, vt_s, qs, bias, at_s, a_s, s1, s3 = refs[:19]
    refs = refs[19:]
    if not far_given:
        s2, refs = refs[0], refs[1:]
    scratch, (sems, near_sems, far_sems, fwd_sems) = refs[:7], refs[7:]
    rows, width = own_ref.shape
    tiles = width // 256
    parts = far_sems.shape[1]
    dev = lax.axis_index("sp")
    odd = lax.rem(dev, 2)
    chip1 = dev >= 2
    sibling = dev + 1 - 2 * odd
    across = lax.rem(dev + 2, 4)

    w_copies = [pltpu.make_async_copy(src.at[layer], w_s.at[n], sems.at[n]) for n, src in enumerate((wk, wv, wq, wo, wcq))]
    w_copies[0].start()
    w_copies[1].start()

    barrier = pltpu.get_barrier_semaphore()
    for other in (sibling, across):
        pl.semaphore_signal(barrier, inc=1, device_id={"sp": other}, device_id_type=pl.DeviceIdType.MESH)
    pl.semaphore_wait(barrier, 2)

    def send(src, dst, sem, other):
        return pltpu.make_async_remote_copy(src_ref=src, dst_ref=dst, send_sem=sem.at[0], recv_sem=sem.at[1],
                                            device_id={"sp": other}, device_id_type=pl.DeviceIdType.MESH)

    def part(i):
        return pl.ds(i * (rows // parts), rows // parts)

    near = send(own_ref, s1, near_sems, sibling)
    far = [send(own_ref.at[part(i)], s2.at[part(i)], far_sems.at[:, i], across) for i in range(parts)]
    fwd = [send(s2.at[part(i)], s3.at[part(i)], fwd_sems.at[:, i], sibling) for i in range(parts)]

    if not far_given:
        @pl.when(jnp.logical_not(chip1))
        def _():
            for cp in far:
                cp.start()

    @pl.when(odd == 0)
    def _():
        near.start()

    if far_given:
        @pl.when(chip1)
        def _():
            for cp in fwd:
                cp.start()

    gain = gs_ref[layer:layer + 1, :]
    x_s[pl.ds(0, rows), :] = rms(own_ref[...], gain)
    key = lax.broadcasted_iota(jnp.int32, (rows, rows), 0)
    query = lax.broadcasted_iota(jnp.int32, (rows, rows), 1)
    bias[pl.ds(0, rows), :] = jnp.where(key <= query, 0.0, NEG_BIG)
    bias[pl.ds(rows, rows), :] = jnp.full((rows, rows), jnp.where(odd == 1, 0.0, NEG_BIG), F32)
    attend_reset(scratch)

    @pl.when(odd == 1)
    def _():
        near.wait_recv()
        x_s[pl.ds(rows, rows), :] = rms(s1[...], gain)

    @pl.when(odd == 0)
    def _():
        x_s[pl.ds(rows, rows), :] = jnp.zeros((rows, width), BF16)

    def tile(t):
        return pl.ds(pl.multiple_of(t * 256, 256), 256)

    def project(n, first):
        def step(r, _):
            at = tile(first + r)
            out = dot(x_s[at, :], w_s[n]).astype(BF16)
            if n == 0:
                k_s[at, :] = out
            else:
                vt_s[:, at] = out.T
            return 0

        lax.fori_loop(0, 2, step, 0)

    def head_cols(i):
        return pl.ds(pl.multiple_of(i * 128, 128), 128)

    def attend(half, add):
        at = pl.ds(half * CH, CH)

        def scores(i, j):
            k = k_s[at, head_cols(i)]
            return [add(dot_nt(k, q)) for q in pair_queries(qs[:, head_cols(i)])]

        attend_all(width // 128, 1, scores, lambda i, j: vt_s[head_cols(i), at], lambda i: None, lambda i: None, scratch)

    w_copies[0].wait()
    w_copies[2].start()
    project(0, 0)
    w_copies[1].wait()
    w_copies[3].start()
    project(1, 0)
    w_copies[2].wait()
    w_copies[4].start()

    def project_q(t, _):
        qs[:, tile(t)] = dot(x_s[pl.ds(0, rows), :], w_s[2, :, tile(t)]).astype(BF16) * BF16(0.125)
        return 0

    lax.fori_loop(0, tiles, project_q, 0)
    attend(0, lambda s: s + bias[...])

    @pl.when(chip1)
    def _():
        if not far_given:
            for i in range(parts):
                far[i].wait_recv()
                fwd[i].start()
        x_s[pl.ds(2 * rows, rows), :] = rms(s2[...], gain)
        for cp in fwd:
            cp.wait_recv()
        x_s[pl.ds(3 * rows, rows), :] = rms(s3[...], gain)
        project(0, 2)
        project(1, 2)
        attend(1, lambda s: s)

    def finish(i, _):
        attend_finish(i, at_s, scratch)
        return 0

    lax.fori_loop(0, width // 128, finish, 0)
    a_s[...] = at_s[...].T
    w_copies[3].wait()

    def project_o(t, _):
        cols = tile(t)
        hid_ref[:, cols] = (own_ref[:, cols].astype(F32) + dot(a_s[...], w_s[3, :, cols])).astype(BF16)
        return 0

    lax.fori_loop(0, tiles, project_o, 0)
    a_s[...] = rms(hid_ref[...], gc_ref[layer:layer + 1, :])
    w_copies[4].wait()

    def project_cq(t, _):
        cols = tile(t)
        q_ref[:, cols] = dot(a_s[...], w_s[4, :, cols]).astype(BF16) * BF16(0.125)
        return 0

    lax.fori_loop(0, tiles, project_cq, 0)

    @pl.when(odd == 0)
    def _():
        near.wait_send()

    @pl.when(chip1)
    def _():
        for cp in fwd:
            cp.wait_send()

    if not far_given:
        @pl.when(jnp.logical_not(chip1))
        def _():
            for cp in far:
                cp.wait_send()


def self_attention(layer, own, far, gs, gc, wq, wk, wv, wo, wcq):
    rows, width = own.shape
    far_given = far is not None
    parts = 1 if far_given else 4
    shape = jax.ShapeDtypeStruct((rows, width), BF16)
    flops = 2 * rows * width * width * 11 + 4 * rows * 4 * rows * width
    block = pltpu.VMEM((rows, width), BF16)
    return pl.pallas_call(
        functools.partial(self_kernel, layer, far_given),
        in_specs=[VMEM] * (4 if far_given else 3) + [ANY] * 5,
        out_specs=[VMEM, VMEM],
        out_shape=[shape, shape],
        scratch_shapes=[
            pltpu.VMEM((5, width, width), BF16),
            pltpu.VMEM((4 * rows, width), BF16),
            pltpu.VMEM((4 * rows, width), BF16),
            pltpu.VMEM((width, 4 * rows), BF16),
            block,
            pltpu.VMEM((2 * rows, rows), F32),
            pltpu.VMEM((width, rows), BF16),
            block,
            block,
            block,
            *([] if far_given else [block]),
            *attend_scratch(width // 128, rows),
            pltpu.SemaphoreType.DMA((5,)),
            pltpu.SemaphoreType.DMA((2,)),
            pltpu.SemaphoreType.DMA((2, parts)),
            pltpu.SemaphoreType.DMA((2, parts)),
        ],
        cost_estimate=pl.CostEstimate(flops=flops, bytes_accessed=10 * width * width, transcendentals=0),
        compiler_params=pltpu.CompilerParams(vmem_limit_bytes=VMEM_LIMIT, collective_id=layer, has_side_effects=True),
        name="self_attention",
    )(own, *([far] if far_given else []), gs, gc, wq, wk, wv, wo, wcq)


def cross_kernel(layer, planes, n_kv, lim_ref, q_ref, hid_ref, gm_ref, *refs):
    ks, vts = refs[:n_kv], refs[n_kv:2 * n_kv]
    (wco, wg, wu, wd, out_ref, kbuf, vbuf, at_s, a_s, x_s, acc_o, mask, list_s, wo_s, wg_s, wu_s, wd_s,
     kv_sems, o_sem, w_sems) = refs[2 * n_kv:-7]
    scratch = refs[-7:]
    rows, width = q_ref.shape
    pairs = width // 128
    steps = wg_s.shape[0]
    ff = wg_s.shape[2]

    def kv_copies(i, slot):
        cols = pl.ds(pl.multiple_of(i * 128, 128), 128)
        out, at = [], 0
        for n in range(n_kv):
            n_rows = ks[n].shape[1]
            out.append(pltpu.make_async_copy(ks[n].at[planes[n], :, cols], kbuf.at[slot, pl.ds(at, n_rows), :], kv_sems.at[slot, 0, n]))
            out.append(pltpu.make_async_copy(vts[n].at[planes[n], cols, :], vbuf.at[slot, :, pl.ds(at, n_rows)], kv_sems.at[slot, 1, n]))
            at += n_rows
        return out

    def w_copies(j):
        cols = pl.ds(pl.multiple_of(j * ff, ff), ff)
        return (pltpu.make_async_copy(wg.at[layer, :, cols], wg_s.at[j], w_sems.at[0, j]),
                pltpu.make_async_copy(wu.at[layer, :, cols], wu_s.at[j], w_sems.at[1, j]),
                pltpu.make_async_copy(wd.at[layer, cols, :], wd_s.at[j], w_sems.at[2, j]))

    for cp in kv_copies(0, 0):
        cp.start()
    o_copy = pltpu.make_async_copy(wco.at[layer], wo_s, o_sem)

    n_chunks, last = jnp.int32(0), jnp.int32(0)
    for c in range(lim_ref.shape[0]):
        lim = lim_ref[c]

        @pl.when(lim > 0)
        def _(c=c, at=n_chunks):
            list_s[at] = c

        n_chunks = n_chunks + (lim > 0).astype(jnp.int32)
        last = last + jnp.where(lim < CH, lim, 0)
    key = lax.broadcasted_iota(jnp.int32, (CH, 128), 0)
    lane = lax.broadcasted_iota(jnp.int32, (CH, 128), 1)
    mask[0] = jnp.zeros((CH, 128), BF16)
    mask[1] = jnp.where((key >= last) & (lane == 0), NEG_BIG, 0.0).astype(BF16)
    ones = (lax.broadcasted_iota(jnp.int32, (rows, 128), 1) == 0).astype(F32).astype(BF16)

    def enter(i):
        @pl.when(i + 1 < pairs)
        def _():
            for cp in kv_copies(i + 1, lax.rem(i + 1, 3)):
                cp.start()

        @pl.when(i == 0)
        def _():
            o_copy.start()

        @pl.when(i < steps)
        def _():
            for cp in w_copies(i):
                cp.start()

        for cp in kv_copies(i, lax.rem(i, 3)):
            cp.wait()

    def chunk(j):
        return pl.ds(pl.multiple_of(list_s[j] * CH, CH), CH)

    def scores(i, j):
        k = kbuf[lax.rem(i, 3), chunk(j), :]
        partial = (lim_ref[list_s[j]] < CH).astype(jnp.int32)
        cols = pl.ds(pl.multiple_of(i * 128, 128), 128)
        k = jnp.concatenate([k, mask[partial]], axis=1)
        return [dot_nt(k, jnp.concatenate([q, ones], axis=1)) for q in pair_queries(q_ref[:, cols])]

    def values(i, j):
        return vbuf[lax.rem(i, 3), :, chunk(j)]

    attend_reset(scratch)
    attend_all(pairs, n_chunks, scores, values, enter, lambda i: attend_finish(i, at_s, scratch), scratch)

    a_s[...] = at_s[...].T
    o_copy.wait()

    def project_o(t, _):
        cols = pl.ds(pl.multiple_of(t * 256, 256), 256)
        out_ref[:, cols] = (hid_ref[:, cols].astype(F32) + dot(a_s[...], wo_s[:, cols])).astype(BF16)
        return 0

    lax.fori_loop(0, width // 256, project_o, 0)
    x_s[...] = rms(out_ref[...], gm_ref[layer:layer + 1, :])
    acc_o[...] = jnp.zeros_like(acc_o)

    def mlp_step(j, _):
        for cp in w_copies(j):
            cp.wait()
        x = x_s[...]
        gate = dot(x, wg_s[j])
        up = dot(x, wu_s[j])
        act = (gate / (1.0 + jnp.exp(-gate)) * up).astype(BF16)
        acc_o[...] += dot(act, wd_s[j])
        return 0

    lax.fori_loop(0, steps, mlp_step, 0)
    out_ref[...] = (out_ref[...].astype(F32) + acc_o[...]).astype(BF16)


def cross_mlp(layer, lims, q, hid, gm, kvs, wco, wg, wu, wd):
    rows, width = q.shape
    pairs = width // 128
    steps = 10
    ff = wg.shape[2] // steps
    planes = tuple(plane for _, _, plane in kvs)
    ks, vts = [k for k, _, _ in kvs], [v for _, v, _ in kvs]
    total = sum(k.shape[1] for k in ks)
    n = len(kvs)
    flops = 2 * rows * width * (width + 3 * wg.shape[2]) + 4 * rows * 3072 * width
    return pl.pallas_call(
        functools.partial(cross_kernel, layer, planes, n),
        in_specs=[SMEM, VMEM, VMEM, VMEM] + [ANY] * (2 * n + 4),
        out_specs=VMEM,
        out_shape=jax.ShapeDtypeStruct((rows, width), BF16),
        scratch_shapes=[
            pltpu.VMEM((3, total, 128), BF16),
            pltpu.VMEM((3, 128, total), BF16),
            pltpu.VMEM((width, rows), BF16),
            pltpu.VMEM((rows, width), BF16),
            pltpu.VMEM((rows, width), BF16),
            pltpu.VMEM((rows, width), F32),
            pltpu.VMEM((2, CH, 128), BF16),
            pltpu.SMEM((8,), jnp.int32),
            pltpu.VMEM((width, width), BF16),
            pltpu.VMEM((steps, width, ff), BF16),
            pltpu.VMEM((steps, width, ff), BF16),
            pltpu.VMEM((steps, ff, width), BF16),
            pltpu.SemaphoreType.DMA((3, 2, n)),
            pltpu.SemaphoreType.DMA,
            pltpu.SemaphoreType.DMA((3, steps)),
            *attend_scratch(pairs, rows),
        ],
        cost_estimate=pl.CostEstimate(flops=flops, bytes_accessed=2 * width * (width + 3 * wg.shape[2]), transcendentals=0),
        compiler_params=pltpu.CompilerParams(vmem_limit_bytes=VMEM_LIMIT),
        name="cross_mlp",
    )(lims, q, hid, gm, *ks, *vts, wco, wg, wu, wd)


NONE = 1 << 20
BASES = (
    (0, 512, 1024, 1536, 2048, NONE, NONE, 2560),
    (1024, 1536, 0, 512, NONE, 2048, 2560, NONE),
    (2048, NONE, 2560, NONE, 0, 1024, 512, 1536),
    (2560, NONE, 2048, NONE, 1024, 0, 1536, 512),
)


def solution(mesh):
    row_spec = P(('dp', 'sp'), None)

    def local_step(hidden, memory, mem_len, norm_self, norm_cross, norm_mlp, self_q, self_k, self_v, self_o, cross_q, cross_k, cross_v, cross_o, mlp_gate, mlp_up, mlp_down):
        layers, width = norm_self.shape
        w_so = self_o.reshape(layers, width, width)
        w_co = cross_o.reshape(layers, width, width)
        dev = lax.axis_index('sp')
        dev_arr = dev.astype(jnp.int32).reshape(1)
        bases = jnp.array(BASES, jnp.int32)[dev]
        lims = jnp.clip(mem_len[0] - bases, 0, CH)
        is3 = (dev_arr == 3).astype(jnp.int32)

        def swap(x):
            return lax.ppermute(x, 'sp', [(0, 1), (1, 0), (2, 3), (3, 2)])

        def program(hidden):
            far = lax.ppermute(hidden, 'sp', [(0, 2), (1, 3)])
            mem_a, mem_b = memory[:CH], memory[CH:]
            c2b = lax.ppermute(mem_b, 'sp', [(2, 3)])
            rem_a = lax.ppermute(mem_a, 'sp', [(0, 2), (1, 3), (2, 0)])
            rem_b = lax.ppermute(mem_b, 'sp', [(0, 2), (1, 3), (2, 1)])

            both = (0, layers)
            ka, va = kv_project(lims[0:2], is3, [memory, c2b], cross_k, cross_v, 2 * CH, both)
            kas, vas = swap(ka), swap(va)
            kvs = []
            for layer in range(layers):
                kvs.append([(ka, va, layer), (kas, vas, layer)])
            for layer in range(layers):
                for rem, at in ((rem_a, 4), (rem_b, 6)):
                    k, v = kv_project(lims[at:at + 1], is3, [rem], cross_k, cross_v, CH, (layer, 1))
                    kvs[layer] += [(k, v, 0), (swap(k), swap(v), 0)]

            for layer in range(layers):
                hidden, q = self_attention(layer, hidden, far, norm_self, norm_cross, self_q, self_k, self_v, w_so, cross_q)
                hidden = cross_mlp(layer, lims, q, hidden, norm_mlp, kvs[layer], w_co, mlp_gate, mlp_up, mlp_down)
                far = None
            return hidden

        return program(hidden)

    return jax.shard_map(local_step, mesh=mesh, in_specs=(row_spec, row_spec, P('dp')) + (P(),) * 14, out_specs=row_spec, check_vma=False)
```

```python
import functools

import jax
import jax.numpy as jnp
from jax import lax
from jax.experimental import pallas as pl
from jax.experimental.pallas import tpu as pltpu
from jax.sharding import PartitionSpec as P


EPS = 1e-6
NEG_BIG = -1e30
F32 = jnp.float32
BF16 = jnp.bfloat16
CH = 512
VMEM_LIMIT = 62 * 1024 * 1024
ANY = pl.BlockSpec(memory_space=pl.ANY)
SMEM = pl.BlockSpec(memory_space=pltpu.SMEM)
VMEM = pl.BlockSpec(memory_space=pltpu.VMEM)


def rms(h, gain):
    h32 = h.astype(F32)
    inv = lax.rsqrt(jnp.mean(h32 * h32, axis=-1, keepdims=True) + EPS)
    return (h32 * inv * gain.astype(F32)).astype(BF16)


def dot(a, b):
    return jnp.dot(a, b, preferred_element_type=F32)


def dot_nt(a, b):
    return lax.dot_general(a, b, (((1,), (1,)), ((), ())), preferred_element_type=F32)


def kv_kernel(layers, n_src, lim_ref, pick_ref, *refs):
    srcs, (wk, wv, k_out, vt_out, mem, w_s, k_s, vt_s, sem, w_sems, o_sems) = refs[:n_src], refs[n_src:]
    rows = mem.shape[0]
    lo, n = layers

    def from_src(go):
        if n_src == 1:
            go(pltpu.make_async_copy(srcs[0], mem, sem))
        else:
            @pl.when(pick_ref[0] == 0)
            def _():
                go(pltpu.make_async_copy(srcs[0], mem, sem))

            @pl.when(pick_ref[0] != 0)
            def _():
                go(pltpu.make_async_copy(srcs[1], mem.at[pl.ds(0, CH)], sem))

    w_copies = []
    for i in range(n):
        for v, src in enumerate((wk, wv)):
            w_copies.append(pltpu.make_async_copy(src.at[lo + i], w_s.at[2 * i + v], w_sems.at[2 * i + v]))
    w_copies[0].start()
    from_src(lambda cp: cp.start())
    for cp in w_copies[1:]:
        cp.start()
    from_src(lambda cp: cp.wait())

    def out_copy(i, v, c):
        at = pl.ds(c * CH, CH)
        if v == 0:
            return pltpu.make_async_copy(k_s.at[i, at, :], k_out.at[i, at, :], o_sems.at[i, v, c])
        return pltpu.make_async_copy(vt_s.at[i, :, at], vt_out.at[i, :, at], o_sems.at[i, v, c])

    for i in range(n):
        for v in range(2):
            w_copies[2 * i + v].wait()
            for c in range(rows // CH):
                @pl.when(lim_ref[c] > 0)
                def _(i=i, v=v, c=c):
                    def step(r, _):
                        at = pl.ds(pl.multiple_of(c * CH + r * 256, 256), 256)
                        out = dot(mem[at, :], w_s[2 * i + v]).astype(BF16)
                        if v == 0:
                            k_s[i, at, :] = out
                        else:
                            vt_s[i, :, at] = out.T
                        return 0

                    lax.fori_loop(0, CH // 256, step, 0)
                    out_copy(i, v, c).start()
    for i in range(n):
        for v in range(2):
            for c in range(rows // CH):
                @pl.when(lim_ref[c] > 0)
                def _(i=i, v=v, c=c):
                    out_copy(i, v, c).wait()


def kv_project(lims, pick, srcs, wk, wv, rows, layers):
    width, cols = wk.shape[1], wk.shape[2]
    n = layers[1]
    flops = n * 4 * rows * width * cols
    return pl.pallas_call(
        functools.partial(kv_kernel, layers, len(srcs)),
        in_specs=[SMEM, SMEM] + [ANY] * (len(srcs) + 2),
        out_specs=[ANY, ANY],
        out_shape=[jax.ShapeDtypeStruct((n, rows, cols), BF16), jax.ShapeDtypeStruct((n, cols, rows), BF16)],
        scratch_shapes=[
            pltpu.VMEM((rows, width), BF16),
            pltpu.VMEM((2 * n, width, cols), BF16),
            pltpu.VMEM((n, rows, cols), BF16),
            pltpu.VMEM((n, cols, rows), BF16),
            pltpu.SemaphoreType.DMA,
            pltpu.SemaphoreType.DMA((2 * n,)),
            pltpu.SemaphoreType.DMA((n, 2, rows // CH)),
        ],
        cost_estimate=pl.CostEstimate(flops=flops, bytes_accessed=n * 4 * width * cols, transcendentals=0),
        compiler_params=pltpu.CompilerParams(vmem_limit_bytes=48 * 1024 * 1024),
        name="kv_project",
    )(lims, pick, *srcs, wk, wv)


def pair_queries(q):
    lane = lax.broadcasted_iota(jnp.int32, q.shape, 1)
    zero = jnp.zeros_like(q)
    return jnp.where(lane < 64, q, zero), jnp.where(lane < 64, zero, q)


def attend_all(pairs, n_chunks, scores, values, enter, leave, scratch):
    s_refs, mx_refs, (m_ref, l_ref, acc_ref) = scratch[:2], scratch[2:4], scratch[4:]

    def stage1(pair, j, buf):
        for h, s in enumerate(scores(pair, j)):
            s_refs[buf][h] = s
            mx_refs[buf][h:h + 1, :] = jnp.max(s, axis=0, keepdims=True)

    def stage2(pair, j, buf):
        vt = values(pair, j)
        for h in range(2):
            m_old = m_ref[pair, h:h + 1, :]
            m_new = jnp.maximum(m_old, mx_refs[buf][h:h + 1, :])
            p = jnp.exp(s_refs[buf][h] - m_new)
            alpha = jnp.exp(m_old - m_new)
            m_ref[pair, h:h + 1, :] = m_new
            l_ref[pair, h:h + 1, :] = l_ref[pair, h:h + 1, :] * alpha + jnp.sum(p, axis=0, keepdims=True)
            acc_ref[pair, h] = acc_ref[pair, h] * alpha + dot(vt[h * 64:(h + 1) * 64, :], p.astype(BF16))

    def advance(pair, j):
        wrap = j + 1 == n_chunks
        return jnp.where(wrap, pair + 1, pair), jnp.where(wrap, 0, j + 1)

    enter(0)
    stage1(0, 0, 0)

    def step(_, now):
        pair, j = now
        for buf in range(2):
            pair_next, j_next = advance(pair, j)

            @pl.when((j_next == 0) & (pair_next < pairs))
            def _(pair_next=pair_next):
                enter(pair_next)

            stage1(jnp.minimum(pair_next, pairs - 1), j_next, 1 - buf)
            stage2(pair, j, buf)

            @pl.when(j_next == 0)
            def _(pair=pair):
                leave(pair)

            pair, j = pair_next, j_next
        return pair, j

    lax.fori_loop(0, pairs * n_chunks // 2, step, (jnp.int32(0), jnp.int32(0)))


def attend_reset(scratch):
    m_ref, l_ref, acc_ref = scratch[4:]
    m_ref[...] = jnp.full_like(m_ref, -jnp.inf)
    l_ref[...] = jnp.zeros_like(l_ref)
    acc_ref[...] = jnp.zeros_like(acc_ref)


def attend_finish(pair, at_ref, scratch):
    l_ref, acc_ref = scratch[5:]
    for h in range(2):
        rows = pl.ds(pl.multiple_of(pair * 128 + h * 64, 64), 64)
        at_ref[rows, :] = (acc_ref[pair, h] / l_ref[pair, h:h + 1, :]).astype(BF16)


def attend_scratch(pairs, rows):
    return [
        pltpu.VMEM((2, CH, rows), F32),
        pltpu.VMEM((2, CH, rows), F32),
        pltpu.VMEM((2, rows), F32),
        pltpu.VMEM((2, rows), F32),
        pltpu.VMEM((pairs, 2, rows), F32),
        pltpu.VMEM((pairs, 2, rows), F32),
        pltpu.VMEM((pairs, 2, 64, rows), F32),
    ]


def self_kernel(layer, far_given, *refs):
    own_ref, refs = refs[0], refs[1:]
    if far_given:
        s2, refs = refs[0], refs[1:]
    gs_ref, gc_ref, wq, wk, wv, wo, wcq, hid_ref, q_ref, w_s, x_s, k_s, vt_s, qs, bias, at_s, a_s, s1, s3 = refs[:19]
    refs = refs[19:]
    if not far_given:
        s2, refs = refs[0], refs[1:]
    scratch, (sems, near_sems, far_sems, fwd_sems) = refs[:7], refs[7:]
    rows, width = own_ref.shape
    tiles = width // 256
    parts = far_sems.shape[1]
    dev = lax.axis_index("sp")
    odd = lax.rem(dev, 2)
    chip1 = dev >= 2
    sibling = dev + 1 - 2 * odd
    across = lax.rem(dev + 2, 4)

    w_copies = [pltpu.make_async_copy(src.at[layer], w_s.at[n], sems.at[n]) for n, src in enumerate((wk, wv, wq, wo, wcq))]
    w_copies[0].start()
    w_copies[1].start()

    barrier = pltpu.get_barrier_semaphore()
    others = (sibling,) if far_given else (sibling, across)
    for other in others:
        pl.semaphore_signal(barrier, inc=1, device_id={"sp": other}, device_id_type=pl.DeviceIdType.MESH)
    pl.semaphore_wait(barrier, len(others))

    def send(src, dst, sem, other):
        return pltpu.make_async_remote_copy(src_ref=src, dst_ref=dst, send_sem=sem.at[0], recv_sem=sem.at[1],
                                            device_id={"sp": other}, device_id_type=pl.DeviceIdType.MESH)

    def part(i):
        return pl.ds(i * (rows // parts), rows // parts)

    near = send(own_ref, s1, near_sems, sibling)
    far = [send(own_ref.at[part(i)], s2.at[part(i)], far_sems.at[:, i], across) for i in range(parts)]
    fwd = [send(s2.at[part(i)], s3.at[part(i)], fwd_sems.at[:, i], sibling) for i in range(parts)]

    if not far_given:
        @pl.when(jnp.logical_not(chip1))
        def _():
            for cp in far:
                cp.start()

    @pl.when(odd == 0)
    def _():
        near.start()

    if far_given:
        @pl.when(chip1)
        def _():
            for cp in fwd:
                cp.start()

    gain = gs_ref[layer:layer + 1, :]
    x_s[pl.ds(0, rows), :] = rms(own_ref[...], gain)
    key = lax.broadcasted_iota(jnp.int32, (rows, rows), 0)
    query = lax.broadcasted_iota(jnp.int32, (rows, rows), 1)
    bias[0, pl.ds(0, rows), :] = jnp.where(key <= query, 0.0, NEG_BIG)
    bias[0, pl.ds(rows, rows), :] = jnp.full((rows, rows), jnp.where(odd == 1, 0.0, NEG_BIG), F32)
    bias[1] = jnp.zeros((2 * rows, rows), F32)
    attend_reset(scratch)

    @pl.when(odd == 1)
    def _():
        near.wait_recv()
        x_s[pl.ds(rows, rows), :] = rms(s1[...], gain)

    @pl.when(odd == 0)
    def _():
        x_s[pl.ds(rows, rows), :] = jnp.zeros((rows, width), BF16)

    def tile(t):
        return pl.ds(pl.multiple_of(t * 256, 256), 256)

    def head_cols(i):
        return pl.ds(pl.multiple_of(i * 128, 128), 128)

    def phase(half, _):
        at = pl.ds(pl.multiple_of(half * CH, CH), CH)

        @pl.when(half == 0)
        def _():
            w_copies[0].wait()
            w_copies[2].start()

        @pl.when(half == 1)
        def _():
            if not far_given:
                for i in range(parts):
                    far[i].wait_recv()
                    fwd[i].start()
            x_s[pl.ds(2 * rows, rows), :] = rms(s2[...], gain)
            for cp in fwd:
                cp.wait_recv()
            x_s[pl.ds(3 * rows, rows), :] = rms(s3[...], gain)

        def project_k(r, _):
            rows_at = tile(2 * half + r)
            k_s[rows_at, :] = dot(x_s[rows_at, :], w_s[0]).astype(BF16)
            return 0

        lax.fori_loop(0, 2, project_k, 0)

        @pl.when(half == 0)
        def _():
            w_copies[1].wait()
            w_copies[3].start()

        def project_v(r, _):
            rows_at = tile(2 * half + r)
            vt_s[:, rows_at] = dot(x_s[rows_at, :], w_s[1]).astype(BF16).T
            return 0

        lax.fori_loop(0, 2, project_v, 0)

        @pl.when(half == 0)
        def _():
            w_copies[2].wait()
            w_copies[4].start()

            def project_q(t, _):
                qs[:, tile(t)] = dot(x_s[pl.ds(0, rows), :], w_s[2, :, tile(t)]).astype(BF16) * BF16(0.125)
                return 0

            lax.fori_loop(0, tiles, project_q, 0)

        def scores(i, j):
            k = k_s[at, head_cols(i)]
            return [dot_nt(k, q) + bias[half] for q in pair_queries(qs[:, head_cols(i)])]

        attend_all(width // 128, 1, scores, lambda i, j: vt_s[head_cols(i), at], lambda i: None, lambda i: None, scratch)
        return 0

    lax.fori_loop(0, jnp.where(chip1, 2, 1), phase, 0)

    def finish(i, _):
        attend_finish(i, at_s, scratch)
        return 0

    lax.fori_loop(0, width // 128, finish, 0)
    a_s[...] = at_s[...].T
    w_copies[3].wait()

    def project_o(t, _):
        cols = tile(t)
        hid_ref[:, cols] = (own_ref[:, cols].astype(F32) + dot(a_s[...], w_s[3, :, cols])).astype(BF16)
        return 0

    lax.fori_loop(0, tiles, project_o, 0)
    a_s[...] = rms(hid_ref[...], gc_ref[layer:layer + 1, :])
    w_copies[4].wait()

    def project_cq(t, _):
        cols = tile(t)
        q_ref[:, cols] = dot(a_s[...], w_s[4, :, cols]).astype(BF16) * BF16(0.125)
        return 0

    lax.fori_loop(0, tiles, project_cq, 0)

    @pl.when(odd == 0)
    def _():
        near.wait_send()

    @pl.when(chip1)
    def _():
        for cp in fwd:
            cp.wait_send()

    if not far_given:
        @pl.when(jnp.logical_not(chip1))
        def _():
            for cp in far:
                cp.wait_send()


def self_attention(layer, own, far, gs, gc, wq, wk, wv, wo, wcq):
    rows, width = own.shape
    far_given = far is not None
    parts = 1 if far_given else 4
    shape = jax.ShapeDtypeStruct((rows, width), BF16)
    flops = 2 * rows * width * width * 11 + 4 * rows * 4 * rows * width
    block = pltpu.VMEM((rows, width), BF16)
    return pl.pallas_call(
        functools.partial(self_kernel, layer, far_given),
        in_specs=[VMEM] * (4 if far_given else 3) + [ANY] * 5,
        out_specs=[VMEM, VMEM],
        out_shape=[shape, shape],
        scratch_shapes=[
            pltpu.VMEM((5, width, width), BF16),
            pltpu.VMEM((4 * rows, width), BF16),
            pltpu.VMEM((4 * rows, width), BF16),
            pltpu.VMEM((width, 4 * rows), BF16),
            block,
            pltpu.VMEM((2, 2 * rows, rows), F32),
            pltpu.VMEM((width, rows), BF16),
            block,
            block,
            block,
            *([] if far_given else [block]),
            *attend_scratch(width // 128, rows),
            pltpu.SemaphoreType.DMA((5,)),
            pltpu.SemaphoreType.DMA((2,)),
            pltpu.SemaphoreType.DMA((2, parts)),
            pltpu.SemaphoreType.DMA((2, parts)),
        ],
        cost_estimate=pl.CostEstimate(flops=flops, bytes_accessed=10 * width * width, transcendentals=0),
        compiler_params=pltpu.CompilerParams(vmem_limit_bytes=VMEM_LIMIT, collective_id=layer, has_side_effects=True),
        name="self_attention",
    )(own, *([far] if far_given else []), gs, gc, wq, wk, wv, wo, wcq)


def cross_kernel(layer, planes, n_kv, state_in, mlp, lim_ref, q_ref, *refs):
    def take(n):
        nonlocal refs
        head, refs = refs[:n], refs[n:]
        return head

    ks, vts = take(n_kv), take(n_kv)
    state = take(3) if state_in else None
    if mlp:
        hid_ref, gm_ref, wco, wg, wu, wd, out_ref = take(7)
    else:
        outs = take(3)
    scratch = take(7)
    kbuf, vbuf, mask, list_s, kv_sems = take(5)
    if mlp:
        at_s, a_s, x_s, acc_o, wo_s, wg_s, wu_s, wd_s, o_sem, w_sems = take(10)
        steps, ff = wg_s.shape[0], wg_s.shape[2]
    rows, width = q_ref.shape
    pairs = width // 128

    def kv_copies(i, slot):
        cols = pl.ds(pl.multiple_of(i * 128, 128), 128)
        out, at = [], 0
        for n in range(n_kv):
            n_rows = ks[n].shape[1]
            out.append(pltpu.make_async_copy(ks[n].at[planes[n], :, cols], kbuf.at[slot, pl.ds(at, n_rows), :], kv_sems.at[slot, 0, n]))
            out.append(pltpu.make_async_copy(vts[n].at[planes[n], cols, :], vbuf.at[slot, :, pl.ds(at, n_rows)], kv_sems.at[slot, 1, n]))
            at += n_rows
        return out

    for cp in kv_copies(0, 0):
        cp.start()
    if mlp:
        o_copy = pltpu.make_async_copy(wco.at[layer], wo_s, o_sem)

        def w_copies(j):
            cols = pl.ds(pl.multiple_of(j * ff, ff), ff)
            return (pltpu.make_async_copy(wg.at[layer, :, cols], wg_s.at[j], w_sems.at[0, j]),
                    pltpu.make_async_copy(wu.at[layer, :, cols], wu_s.at[j], w_sems.at[1, j]),
                    pltpu.make_async_copy(wd.at[layer, cols, :], wd_s.at[j], w_sems.at[2, j]))

        def start_weights(j):
            for cp in w_copies(j):
                cp.start()

        o_copy.start()

    if state_in:
        for src, dst in zip(state, scratch[4:]):
            dst[...] = src[...]
    else:
        attend_reset(scratch)

    n_chunks, last = jnp.int32(0), jnp.int32(0)
    list_s[0] = 0
    for c in range(lim_ref.shape[0]):
        lim = lim_ref[c]

        @pl.when(lim > 0)
        def _(c=c, at=n_chunks):
            list_s[at] = c

        n_chunks = n_chunks + (lim > 0).astype(jnp.int32)
        last = last + jnp.where(lim < CH, lim, 0)
    key = lax.broadcasted_iota(jnp.int32, (CH, 128), 0)
    lane = lax.broadcasted_iota(jnp.int32, (CH, 128), 1)
    mask[0] = jnp.zeros((CH, 128), BF16)
    mask[1] = jnp.where((key >= last) & (lane == 0), NEG_BIG, 0.0).astype(BF16)
    ones = (lax.broadcasted_iota(jnp.int32, (rows, 128), 1) == 0).astype(F32).astype(BF16)

    def enter(i):
        @pl.when(i + 1 < pairs)
        def _():
            for cp in kv_copies(i + 1, lax.rem(i + 1, 3)):
                cp.start()

        if mlp:
            @pl.when(i < steps)
            def _():
                start_weights(i)

        for cp in kv_copies(i, lax.rem(i, 3)):
            cp.wait()

    def chunk(j):
        return pl.ds(pl.multiple_of(list_s[j] * CH, CH), CH)

    def scores(i, j):
        k = kbuf[lax.rem(i, 3), chunk(j), :]
        partial = (lim_ref[list_s[j]] < CH).astype(jnp.int32)
        cols = pl.ds(pl.multiple_of(i * 128, 128), 128)
        k = jnp.concatenate([k, mask[partial]], axis=1)
        return [dot_nt(k, jnp.concatenate([q, ones], axis=1)) for q in pair_queries(q_ref[:, cols])]

    def values(i, j):
        return vbuf[lax.rem(i, 3), :, chunk(j)]

    @pl.when(n_chunks > 0)
    def _():
        attend_all(pairs, n_chunks, scores, values, enter, lambda i: None, scratch)

    @pl.when(n_chunks == 0)
    def _():
        for cp in kv_copies(0, 0):
            cp.wait()
        if mlp:
            for j in range(steps):
                start_weights(j)

    if not mlp:
        for src, dst in zip(scratch[4:], outs):
            dst[...] = src[...]
        return

    def finish(i, _):
        attend_finish(i, at_s, scratch)
        return 0

    lax.fori_loop(0, pairs, finish, 0)
    a_s[...] = at_s[...].T
    o_copy.wait()

    def project_o(t, _):
        cols = pl.ds(pl.multiple_of(t * 256, 256), 256)
        out_ref[:, cols] = (hid_ref[:, cols].astype(F32) + dot(a_s[...], wo_s[:, cols])).astype(BF16)
        return 0

    lax.fori_loop(0, width // 256, project_o, 0)
    x_s[...] = rms(out_ref[...], gm_ref[layer:layer + 1, :])
    acc_o[...] = jnp.zeros_like(acc_o)

    def mlp_step(j, _):
        for cp in w_copies(j):
            cp.wait()
        x = x_s[...]
        gate = dot(x, wg_s[j])
        up = dot(x, wu_s[j])
        act = (gate / (1.0 + jnp.exp(-gate)) * up).astype(BF16)
        acc_o[...] += dot(act, wd_s[j])
        return 0

    lax.fori_loop(0, steps, mlp_step, 0)
    out_ref[...] = (out_ref[...].astype(F32) + acc_o[...]).astype(BF16)


def cross(layer, lims, q, kvs, state=None, after=None):
    rows, width = q.shape
    pairs = width // 128
    planes = tuple(plane for _, _, plane in kvs)
    ks, vts = [k for k, _, _ in kvs], [v for _, v, _ in kvs]
    total = sum(k.shape[1] for k in ks)
    n = len(kvs)
    operands, specs = [lims, q, *ks, *vts], [SMEM, VMEM] + [ANY] * (2 * n)
    if state is not None:
        operands, specs = operands + list(state), specs + [VMEM] * 3
    scratch = attend_scratch(pairs, rows) + [
        pltpu.VMEM((3, total, 128), BF16),
        pltpu.VMEM((3, 128, total), BF16),
        pltpu.VMEM((2, CH, 128), BF16),
        pltpu.SMEM((8,), jnp.int32),
        pltpu.SemaphoreType.DMA((3, 2, n)),
    ]
    flops = 4 * rows * min(total, 3072) * width
    if after is None:
        out_shape = [jax.ShapeDtypeStruct((pairs, 2, rows), F32)] * 2 + [jax.ShapeDtypeStruct((pairs, 2, 64, rows), F32)]
        out_specs = [VMEM] * 3
        moved = 8 * total * width
        limit = 32 * 1024 * 1024
    else:
        _, _, _, wg, _, _ = after
        operands, specs = operands + list(after), specs + [VMEM] * 2 + [ANY] * 4
        out_shape, out_specs = jax.ShapeDtypeStruct((rows, width), BF16), VMEM
        steps = 10
        ff = wg.shape[2] // steps
        scratch += [
            pltpu.VMEM((width, rows), BF16),
            pltpu.VMEM((rows, width), BF16),
            pltpu.VMEM((rows, width), BF16),
            pltpu.VMEM((rows, width), F32),
            pltpu.VMEM((width, width), BF16),
            pltpu.VMEM((steps, width, ff), BF16),
            pltpu.VMEM((steps, width, ff), BF16),
            pltpu.VMEM((steps, ff, width), BF16),
            pltpu.SemaphoreType.DMA,
            pltpu.SemaphoreType.DMA((3, steps)),
        ]
        flops += 2 * rows * width * (width + 3 * wg.shape[2])
        moved = 2 * width * (width + 3 * wg.shape[2])
        limit = VMEM_LIMIT
    return pl.pallas_call(
        functools.partial(cross_kernel, layer, planes, n, state is not None, after is not None),
        in_specs=specs,
        out_specs=out_specs,
        out_shape=out_shape,
        scratch_shapes=scratch,
        cost_estimate=pl.CostEstimate(flops=flops, bytes_accessed=moved, transcendentals=0),
        compiler_params=pltpu.CompilerParams(vmem_limit_bytes=limit),
        name="cross_attention" if after is None else "cross_mlp",
    )(*operands)


NONE = 1 << 20
BASES = (
    (0, 512, 1024, 1536, 2048, NONE, NONE, 2560),
    (1024, 1536, 0, 512, NONE, 2048, 2560, NONE),
    (2048, NONE, 2560, NONE, 0, 1024, 512, 1536),
    (2560, NONE, 2048, NONE, 1024, 0, 1536, 512),
)


def solution(mesh):
    row_spec = P(('dp', 'sp'), None)

    def local_step(hidden, memory, mem_len, norm_self, norm_cross, norm_mlp, self_q, self_k, self_v, self_o, cross_q, cross_k, cross_v, cross_o, mlp_gate, mlp_up, mlp_down):
        layers, width = norm_self.shape
        w_so = self_o.reshape(layers, width, width)
        w_co = cross_o.reshape(layers, width, width)
        dev = lax.axis_index('sp')
        dev_arr = dev.astype(jnp.int32).reshape(1)
        bases = jnp.array(BASES, jnp.int32)[dev]
        lims = jnp.clip(mem_len[0] - bases, 0, CH)
        is3 = (dev_arr == 3).astype(jnp.int32)

        def swap(x):
            return lax.ppermute(x, 'sp', [(0, 1), (1, 0), (2, 3), (3, 2)])

        def program(hidden):
            far = lax.ppermute(hidden, 'sp', [(0, 2), (1, 3)])
            mem_a, mem_b = memory[:CH], memory[CH:]
            c2b = lax.ppermute(mem_b, 'sp', [(2, 3)])
            rem_a = lax.ppermute(mem_a, 'sp', [(0, 2), (1, 3), (2, 0)])
            rem_b = lax.ppermute(mem_b, 'sp', [(0, 2), (1, 3), (2, 1)])

            both = (0, layers)
            ka, va = kv_project(lims[0:2], is3, [memory, c2b], cross_k, cross_v, 2 * CH, both)
            kas, vas = swap(ka), swap(va)
            kvs = []
            for layer in range(layers):
                kvs.append([(ka, va, layer), (kas, vas, layer)])
            for layer in range(layers):
                for rem, at in ((rem_a, 4), (rem_b, 6)):
                    k, v = kv_project(lims[at:at + 1], is3, [rem], cross_k, cross_v, CH, (layer, 1))
                    kvs[layer] += [(k, v, 0), (swap(k), swap(v), 0)]

            for layer in range(layers):
                hidden, q = self_attention(layer, hidden, far, norm_self, norm_cross, self_q, self_k, self_v, w_so, cross_q)
                after = (hidden, norm_mlp, w_co, mlp_gate, mlp_up, mlp_down)
                if layer == 0:
                    state = cross(layer, lims[:6], q, kvs[layer][:4])
                    hidden = cross(layer, lims[6:], q, kvs[layer][4:], state, after)
                else:
                    hidden = cross(layer, lims, q, kvs[layer], None, after)
                far = None
            return hidden

        return program(hidden)

    return jax.shard_map(local_step, mesh=mesh, in_specs=(row_spec, row_spec, P('dp')) + (P(),) * 14, out_specs=row_spec, check_vma=False)
```

```python
import functools

import jax
import jax.numpy as jnp
from jax import lax
from jax.experimental import pallas as pl
from jax.experimental.pallas import tpu as pltpu
from jax.sharding import PartitionSpec as P


EPS = 1e-6
NEG_BIG = -1e30
F32 = jnp.float32
BF16 = jnp.bfloat16
CH = 512
HEADS = 4
GW = HEADS * 64
VMEM_LIMIT = 62 * 1024 * 1024
ANY = pl.BlockSpec(memory_space=pl.ANY)
SMEM = pl.BlockSpec(memory_space=pltpu.SMEM)
VMEM = pl.BlockSpec(memory_space=pltpu.VMEM)


def rms(h, gain):
    h32 = h.astype(F32)
    inv = lax.rsqrt(jnp.mean(h32 * h32, axis=-1, keepdims=True) + EPS)
    return (h32 * inv * gain.astype(F32)).astype(BF16)


def dot(a, b):
    return jnp.dot(a, b, preferred_element_type=F32)


def kv_kernel(layers, n_src, lim_ref, pick_ref, *refs):
    srcs, (wk, wv, k_out, vt_out, mem, w_s, k_s, vt_s, sem, w_sems, o_sems) = refs[:n_src], refs[n_src:]
    rows = mem.shape[0]
    lo, n = layers

    def from_src(go):
        if n_src == 1:
            go(pltpu.make_async_copy(srcs[0], mem, sem))
        else:
            @pl.when(pick_ref[0] == 0)
            def _():
                go(pltpu.make_async_copy(srcs[0], mem, sem))

            @pl.when(pick_ref[0] != 0)
            def _():
                go(pltpu.make_async_copy(srcs[1], mem.at[pl.ds(0, CH)], sem))

    w_copies = []
    for i in range(n):
        for v, src in enumerate((wk, wv)):
            w_copies.append(pltpu.make_async_copy(src.at[lo + i], w_s.at[2 * i + v], w_sems.at[2 * i + v]))
    w_copies[0].start()
    from_src(lambda cp: cp.start())
    for cp in w_copies[1:]:
        cp.start()
    from_src(lambda cp: cp.wait())

    def out_copy(i, v, c):
        at = pl.ds(c * CH, CH)
        if v == 0:
            return pltpu.make_async_copy(k_s.at[i, at, :], k_out.at[i, at, :], o_sems.at[i, v, c])
        return pltpu.make_async_copy(vt_s.at[i, :, at], vt_out.at[i, :, at], o_sems.at[i, v, c])

    for i in range(n):
        for v in range(2):
            w_copies[2 * i + v].wait()
            for c in range(rows // CH):
                @pl.when(lim_ref[c] > 0)
                def _(i=i, v=v, c=c):
                    def step(r, _):
                        at = pl.ds(pl.multiple_of(c * CH + r * 256, 256), 256)
                        out = dot(mem[at, :], w_s[2 * i + v]).astype(BF16)
                        if v == 0:
                            k_s[i, at, :] = out
                        else:
                            vt_s[i, :, at] = out.T
                        return 0

                    lax.fori_loop(0, CH // 256, step, 0)
                    out_copy(i, v, c).start()
    for i in range(n):
        for v in range(2):
            for c in range(rows // CH):
                @pl.when(lim_ref[c] > 0)
                def _(i=i, v=v, c=c):
                    out_copy(i, v, c).wait()


def kv_project(lims, pick, srcs, wk, wv, rows, layers):
    width, cols = wk.shape[1], wk.shape[2]
    n = layers[1]
    flops = n * 4 * rows * width * cols
    return pl.pallas_call(
        functools.partial(kv_kernel, layers, len(srcs)),
        in_specs=[SMEM, SMEM] + [ANY] * (len(srcs) + 2),
        out_specs=[ANY, ANY],
        out_shape=[jax.ShapeDtypeStruct((n, rows, cols), BF16), jax.ShapeDtypeStruct((n, cols, rows), BF16)],
        scratch_shapes=[
            pltpu.VMEM((rows, width), BF16),
            pltpu.VMEM((2 * n, width, cols), BF16),
            pltpu.VMEM((n, rows, cols), BF16),
            pltpu.VMEM((n, cols, rows), BF16),
            pltpu.SemaphoreType.DMA,
            pltpu.SemaphoreType.DMA((2 * n,)),
            pltpu.SemaphoreType.DMA((n, 2, rows // CH)),
        ],
        cost_estimate=pl.CostEstimate(flops=flops, bytes_accessed=n * 4 * width * cols, transcendentals=0),
        compiler_params=pltpu.CompilerParams(vmem_limit_bytes=48 * 1024 * 1024),
        name="kv_project",
    )(lims, pick, *srcs, wk, wv)


def head_queries(qt, extra=None):
    row = lax.broadcasted_iota(jnp.int32, (128, qt.shape[1]), 0)
    out = []
    for h in range(HEADS):
        pair = qt[h // 2 * 128:(h // 2 + 1) * 128, :]
        q = jnp.where((row < 64) == (h % 2 == 0), pair, jnp.zeros_like(pair))
        out.append(q if extra is None else jnp.concatenate([q, extra], axis=0))
    return out


def attend_all(groups, n_chunks, scores, values, enter, leave, scratch):
    s_refs, mx_refs, (m_ref, l_ref, acc_ref) = scratch[:2], scratch[2:4], scratch[4:]
    total = groups * n_chunks

    def stage1(group, j, buf):
        for h, s in enumerate(scores(group, j)):
            s_refs[buf][h] = s
            mx_refs[buf][h:h + 1, :] = jnp.max(s, axis=0, keepdims=True)

    def stage2(group, j, buf):
        vt = values(group, j)
        for h in range(HEADS):
            m_old = m_ref[group, h:h + 1, :]
            m_new = jnp.maximum(m_old, mx_refs[buf][h:h + 1, :])
            p = jnp.exp(s_refs[buf][h] - m_new)
            alpha = jnp.exp(m_old - m_new)
            m_ref[group, h:h + 1, :] = m_new
            l_ref[group, h:h + 1, :] = l_ref[group, h:h + 1, :] * alpha + jnp.sum(p, axis=0, keepdims=True)
            acc_ref[group, h] = acc_ref[group, h] * alpha + dot(vt[h * 64:(h + 1) * 64, :], p.astype(BF16))

    def advance(group, j):
        wrap = j + 1 == n_chunks
        return jnp.where(wrap, group + 1, group), jnp.where(wrap, 0, j + 1)

    enter(0)
    stage1(0, 0, 0)

    def item(group, j, buf):
        group_next, j_next = advance(group, j)

        @pl.when((j_next == 0) & (group_next < groups))
        def _():
            enter(group_next)

        stage1(jnp.minimum(group_next, groups - 1), j_next, 1 - buf)
        stage2(group, j, buf)

        @pl.when(j_next == 0)
        def _():
            leave(group)

    def step(u, now):
        item(*now, 0)
        now = advance(*now)

        @pl.when(2 * u + 1 < total)
        def _():
            item(*now, 1)

        return advance(*now)

    lax.fori_loop(0, (total + 1) // 2, step, (jnp.int32(0), jnp.int32(0)))


def attend_reset(scratch):
    m_ref, l_ref, acc_ref = scratch[4:]
    m_ref[...] = jnp.full_like(m_ref, -jnp.inf)
    l_ref[...] = jnp.zeros_like(l_ref)
    acc_ref[...] = jnp.zeros_like(acc_ref)


def attend_finish(group, at_ref, scratch):
    l_ref, acc_ref = scratch[5:]
    for h in range(HEADS):
        rows = pl.ds(pl.multiple_of(group * HEADS * 64 + h * 64, 64), 64)
        at_ref[rows, :] = (acc_ref[group, h] / l_ref[group, h:h + 1, :]).astype(BF16)


def attend_scratch(groups, rows):
    return [
        pltpu.VMEM((HEADS, CH, rows), F32),
        pltpu.VMEM((HEADS, CH, rows), F32),
        pltpu.VMEM((HEADS, rows), F32),
        pltpu.VMEM((HEADS, rows), F32),
        pltpu.VMEM((groups, HEADS, rows), F32),
        pltpu.VMEM((groups, HEADS, rows), F32),
        pltpu.VMEM((groups, HEADS, 64, rows), F32),
    ]


def self_kernel(layer, far_given, *refs):
    own_ref, refs = refs[0], refs[1:]
    if far_given:
        s2, refs = refs[0], refs[1:]
    gs_ref, gc_ref, wq, wk, wv, wo, wcq, hid_ref, q_ref, w_s, x_s, k_s, vt_s, qs, bias, at_s, a_s, s1, s3 = refs[:19]
    refs = refs[19:]
    if not far_given:
        s2, refs = refs[0], refs[1:]
    scratch, (sems, near_sems, far_sems, fwd_sems) = refs[:7], refs[7:]
    rows, width = own_ref.shape
    tiles = width // 256
    parts = far_sems.shape[1]
    dev = lax.axis_index("sp")
    odd = lax.rem(dev, 2)
    chip1 = dev >= 2
    sibling = dev + 1 - 2 * odd
    across = lax.rem(dev + 2, 4)

    w_copies = [pltpu.make_async_copy(src.at[layer], w_s.at[n], sems.at[n]) for n, src in enumerate((wk, wv, wq, wo, wcq))]
    w_copies[0].start()
    w_copies[1].start()

    barrier = pltpu.get_barrier_semaphore()
    others = (sibling,) if far_given else (sibling, across)
    for other in others:
        pl.semaphore_signal(barrier, inc=1, device_id={"sp": other}, device_id_type=pl.DeviceIdType.MESH)
    pl.semaphore_wait(barrier, len(others))

    def send(src, dst, sem, other):
        return pltpu.make_async_remote_copy(src_ref=src, dst_ref=dst, send_sem=sem.at[0], recv_sem=sem.at[1],
                                            device_id={"sp": other}, device_id_type=pl.DeviceIdType.MESH)

    def part(i):
        return pl.ds(i * (rows // parts), rows // parts)

    near = send(own_ref, s1, near_sems, sibling)
    far = [send(own_ref.at[part(i)], s2.at[part(i)], far_sems.at[:, i], across) for i in range(parts)]
    fwd = [send(s2.at[part(i)], s3.at[part(i)], fwd_sems.at[:, i], sibling) for i in range(parts)]

    if not far_given:
        @pl.when(jnp.logical_not(chip1))
        def _():
            for cp in far:
                cp.start()

    @pl.when(odd == 0)
    def _():
        near.start()

    if far_given:
        @pl.when(chip1)
        def _():
            for cp in fwd:
                cp.start()

    gain = gs_ref[layer:layer + 1, :]
    x_s[pl.ds(0, rows), :] = rms(own_ref[...], gain)
    key = lax.broadcasted_iota(jnp.int32, (rows, rows), 0)
    query = lax.broadcasted_iota(jnp.int32, (rows, rows), 1)
    bias[0, pl.ds(0, rows), :] = jnp.where(key <= query, 0.0, NEG_BIG)
    bias[0, pl.ds(rows, rows), :] = jnp.full((rows, rows), jnp.where(odd == 1, 0.0, NEG_BIG), F32)
    bias[1] = jnp.zeros((2 * rows, rows), F32)
    attend_reset(scratch)

    @pl.when(odd == 1)
    def _():
        near.wait_recv()
        x_s[pl.ds(rows, rows), :] = rms(s1[...], gain)

    @pl.when(odd == 0)
    def _():
        x_s[pl.ds(rows, rows), :] = jnp.zeros((rows, width), BF16)

    def tile(t):
        return pl.ds(pl.multiple_of(t * 256, 256), 256)

    def head_cols(i):
        return pl.ds(pl.multiple_of(i * GW, GW), GW)

    def phase(half, _):
        at = pl.ds(pl.multiple_of(half * CH, CH), CH)

        @pl.when(half == 0)
        def _():
            w_copies[0].wait()
            w_copies[2].start()

        @pl.when(half == 1)
        def _():
            if not far_given:
                for i in range(parts):
                    far[i].wait_recv()
                    fwd[i].start()
            x_s[pl.ds(2 * rows, rows), :] = rms(s2[...], gain)
            for cp in fwd:
                cp.wait_recv()
            x_s[pl.ds(3 * rows, rows), :] = rms(s3[...], gain)

        def project_k(r, _):
            rows_at = tile(2 * half + r)
            k_s[rows_at, :] = dot(x_s[rows_at, :], w_s[0]).astype(BF16)
            return 0

        lax.fori_loop(0, 2, project_k, 0)

        @pl.when(half == 0)
        def _():
            w_copies[1].wait()
            w_copies[3].start()

        def project_v(r, _):
            rows_at = tile(2 * half + r)
            vt_s[:, rows_at] = dot(x_s[rows_at, :], w_s[1]).astype(BF16).T
            return 0

        lax.fori_loop(0, 2, project_v, 0)

        @pl.when(half == 0)
        def _():
            w_copies[2].wait()
            w_copies[4].start()

            def project_q(t, _):
                qs[tile(t), :] = (dot(x_s[pl.ds(0, rows), :], w_s[2, :, tile(t)]).astype(BF16) * BF16(0.125)).T
                return 0

            lax.fori_loop(0, tiles, project_q, 0)

        def scores(i, j):
            k = k_s[at, head_cols(i)]
            return [dot(k[:, h // 2 * 128:(h // 2 + 1) * 128], q) + bias[half] for h, q in enumerate(head_queries(qs[head_cols(i), :]))]

        attend_all(width // GW, 1, scores, lambda i, j: vt_s[head_cols(i), at], lambda i: None, lambda i: None, scratch)
        return 0

    lax.fori_loop(0, jnp.where(chip1, 2, 1), phase, 0)

    def finish(i, _):
        attend_finish(i, at_s, scratch)
        return 0

    lax.fori_loop(0, width // GW, finish, 0)
    a_s[...] = at_s[...].T
    w_copies[3].wait()

    def project_o(t, _):
        cols = tile(t)
        hid_ref[:, cols] = (own_ref[:, cols].astype(F32) + dot(a_s[...], w_s[3, :, cols])).astype(BF16)
        return 0

    lax.fori_loop(0, tiles, project_o, 0)
    a_s[...] = rms(hid_ref[...], gc_ref[layer:layer + 1, :])
    w_copies[4].wait()

    def project_cq(t, _):
        cols = tile(t)
        q_ref[cols, :] = (dot(a_s[...], w_s[4, :, cols]).astype(BF16) * BF16(0.125)).T
        return 0

    lax.fori_loop(0, tiles, project_cq, 0)

    @pl.when(odd == 0)
    def _():
        near.wait_send()

    @pl.when(chip1)
    def _():
        for cp in fwd:
            cp.wait_send()

    if not far_given:
        @pl.when(jnp.logical_not(chip1))
        def _():
            for cp in far:
                cp.wait_send()


def self_attention(layer, own, far, gs, gc, wq, wk, wv, wo, wcq):
    rows, width = own.shape
    far_given = far is not None
    parts = 1 if far_given else 4
    shape = jax.ShapeDtypeStruct((rows, width), BF16)
    flops = 2 * rows * width * width * 11 + 4 * rows * 4 * rows * width
    block = pltpu.VMEM((rows, width), BF16)
    return pl.pallas_call(
        functools.partial(self_kernel, layer, far_given),
        in_specs=[VMEM] * (4 if far_given else 3) + [ANY] * 5,
        out_specs=[VMEM, VMEM],
        out_shape=[shape, jax.ShapeDtypeStruct((width, rows), BF16)],
        scratch_shapes=[
            pltpu.VMEM((5, width, width), BF16),
            pltpu.VMEM((4 * rows, width), BF16),
            pltpu.VMEM((4 * rows, width), BF16),
            pltpu.VMEM((width, 4 * rows), BF16),
            pltpu.VMEM((width, rows), BF16),
            pltpu.VMEM((2, 2 * rows, rows), F32),
            pltpu.VMEM((width, rows), BF16),
            block,
            block,
            block,
            *([] if far_given else [block]),
            *attend_scratch(width // GW, rows),
            pltpu.SemaphoreType.DMA((5,)),
            pltpu.SemaphoreType.DMA((2,)),
            pltpu.SemaphoreType.DMA((2, parts)),
            pltpu.SemaphoreType.DMA((2, parts)),
        ],
        cost_estimate=pl.CostEstimate(flops=flops, bytes_accessed=10 * width * width, transcendentals=0),
        compiler_params=pltpu.CompilerParams(vmem_limit_bytes=VMEM_LIMIT, collective_id=layer, has_side_effects=True),
        name="self_attention",
    )(own, *([far] if far_given else []), gs, gc, wq, wk, wv, wo, wcq)


def cross_kernel(layer, planes, n_kv, lim_ref, q_ref, *refs):
    def take(n):
        nonlocal refs
        head, refs = refs[:n], refs[n:]
        return head

    ks, vts = take(n_kv), take(n_kv)
    hid_ref, gm_ref, wco, wg, wu, wd, out_ref = take(7)
    scratch = take(7)
    kbuf, vbuf, mask, list_s, kv_sems = take(5)
    at_s, a_s, x_s, acc_o, wo_s, wg_s, wu_s, wd_s, o_sem, w_sems = take(10)
    steps, ff = wg_s.shape[0], wg_s.shape[2]
    width, rows = q_ref.shape
    groups = width // GW

    def kv_copies(i):
        slot = lax.rem(i, 2)
        cols = pl.ds(pl.multiple_of(i * GW, GW), GW)
        out, at = [], 0
        for n in range(n_kv):
            n_rows = ks[n].shape[1]
            out.append(pltpu.make_async_copy(ks[n].at[planes[n], :, cols], kbuf.at[slot, pl.ds(at, n_rows), :], kv_sems.at[slot, 0, n]))
            out.append(pltpu.make_async_copy(vts[n].at[planes[n], cols, :], vbuf.at[slot, :, pl.ds(at, n_rows)], kv_sems.at[slot, 1, n]))
            at += n_rows
        return out

    for i in range(2):
        for cp in kv_copies(i):
            cp.start()
    o_copy = pltpu.make_async_copy(wco.at[layer], wo_s, o_sem)

    def w_copies(j):
        cols = pl.ds(pl.multiple_of(j * ff, ff), ff)
        return (pltpu.make_async_copy(wg.at[layer, :, cols], wg_s.at[j], w_sems.at[0, j]),
                pltpu.make_async_copy(wu.at[layer, :, cols], wu_s.at[j], w_sems.at[1, j]),
                pltpu.make_async_copy(wd.at[layer, cols, :], wd_s.at[j], w_sems.at[2, j]))

    attend_reset(scratch)

    n_chunks, last = jnp.int32(0), jnp.int32(0)
    list_s[0] = 0
    for c in range(lim_ref.shape[0]):
        lim = lim_ref[c]

        @pl.when(lim > 0)
        def _(c=c, at=n_chunks):
            list_s[at] = c

        n_chunks = n_chunks + (lim > 0).astype(jnp.int32)
        last = last + jnp.where(lim < CH, lim, 0)
    key = lax.broadcasted_iota(jnp.int32, (CH, 128), 0)
    lane = lax.broadcasted_iota(jnp.int32, (CH, 128), 1)
    mask[0] = jnp.zeros((CH, 128), BF16)
    mask[1] = jnp.where((key >= last) & (lane == 0), NEG_BIG, 0.0).astype(BF16)
    ones = (lax.broadcasted_iota(jnp.int32, (128, rows), 0) == 0).astype(F32).astype(BF16)

    def enter(i):
        for cp in kv_copies(i):
            cp.wait()

        @pl.when(i == 0)
        def _():
            o_copy.start()

        for j in range(2):
            for cp in w_copies(2 * i + j):
                cp.start()

    def leave(i):
        @pl.when(i + 2 < groups)
        def _():
            for cp in kv_copies(i + 2):
                cp.start()

    def chunk(j):
        return pl.ds(pl.multiple_of(list_s[j] * CH, CH), CH)

    def scores(i, j):
        partial = (lim_ref[list_s[j]] < CH).astype(jnp.int32)
        k = kbuf[lax.rem(i, 2), chunk(j), :]
        ks = [jnp.concatenate([k[:, p * 128:(p + 1) * 128], mask[partial]], axis=1) for p in range(HEADS // 2)]
        queries = head_queries(q_ref[pl.ds(pl.multiple_of(i * GW, GW), GW), :], ones)
        return [dot(ks[h // 2], q) for h, q in enumerate(queries)]

    def values(i, j):
        return vbuf[lax.rem(i, 2), :, chunk(j)]

    attend_all(groups, n_chunks, scores, values, enter, leave, scratch)

    def finish(i, _):
        attend_finish(i, at_s, scratch)
        return 0

    lax.fori_loop(0, groups, finish, 0)
    a_s[...] = at_s[...].T
    o_copy.wait()

    def project_o(t, _):
        cols = pl.ds(pl.multiple_of(t * 256, 256), 256)
        out_ref[:, cols] = (hid_ref[:, cols].astype(F32) + dot(a_s[...], wo_s[:, cols])).astype(BF16)
        return 0

    lax.fori_loop(0, width // 256, project_o, 0)
    x_s[...] = rms(out_ref[...], gm_ref[layer:layer + 1, :])
    acc_o[...] = jnp.zeros_like(acc_o)

    def mlp_step(j, _):
        for cp in w_copies(j):
            cp.wait()
        x = x_s[...]
        gate = dot(x, wg_s[j])
        up = dot(x, wu_s[j])
        act = (gate / (1.0 + jnp.exp(-gate)) * up).astype(BF16)
        acc_o[...] += dot(act, wd_s[j])
        return 0

    lax.fori_loop(0, steps, mlp_step, 0)
    out_ref[...] = (out_ref[...].astype(F32) + acc_o[...]).astype(BF16)


def cross_mlp(layer, lims, q, kvs, hid, gm, wco, wg, wu, wd):
    width, rows = q.shape
    groups = width // GW
    planes = tuple(plane for _, _, plane in kvs)
    ks, vts = [k for k, _, _ in kvs], [v for _, v, _ in kvs]
    total = sum(k.shape[1] for k in ks)
    n = len(kvs)
    steps = 2 * groups
    ff = wg.shape[2] // steps
    return pl.pallas_call(
        functools.partial(cross_kernel, layer, planes, n),
        in_specs=[SMEM, VMEM] + [ANY] * (2 * n) + [VMEM] * 2 + [ANY] * 4,
        out_specs=VMEM,
        out_shape=jax.ShapeDtypeStruct((rows, width), BF16),
        scratch_shapes=attend_scratch(groups, rows) + [
            pltpu.VMEM((2, total, GW), BF16),
            pltpu.VMEM((2, GW, total), BF16),
            pltpu.VMEM((2, CH, 128), BF16),
            pltpu.SMEM((8,), jnp.int32),
            pltpu.SemaphoreType.DMA((2, 2, n)),
            pltpu.VMEM((width, rows), BF16),
            pltpu.VMEM((rows, width), BF16),
            pltpu.VMEM((rows, width), BF16),
            pltpu.VMEM((rows, width), F32),
            pltpu.VMEM((width, width), BF16),
            pltpu.VMEM((steps, width, ff), BF16),
            pltpu.VMEM((steps, width, ff), BF16),
            pltpu.VMEM((steps, ff, width), BF16),
            pltpu.SemaphoreType.DMA,
            pltpu.SemaphoreType.DMA((3, steps)),
        ],
        cost_estimate=pl.CostEstimate(
            flops=4 * rows * 3072 * width + 2 * rows * width * (width + 3 * wg.shape[2]),
            bytes_accessed=2 * width * (width + 3 * wg.shape[2]), transcendentals=0),
        compiler_params=pltpu.CompilerParams(vmem_limit_bytes=VMEM_LIMIT),
        name="cross_mlp",
    )(lims, q, *ks, *vts, hid, gm, wco, wg, wu, wd)


NONE = 1 << 20
BASES = (
    (0, 512, 1024, 1536, 2048, NONE, NONE, 2560),
    (1024, 1536, 0, 512, NONE, 2048, 2560, NONE),
    (2048, NONE, 2560, NONE, 0, 1024, 512, 1536),
    (2560, NONE, 2048, NONE, 1024, 0, 1536, 512),
)


def solution(mesh):
    row_spec = P(('dp', 'sp'), None)

    def local_step(hidden, memory, mem_len, norm_self, norm_cross, norm_mlp, self_q, self_k, self_v, self_o, cross_q, cross_k, cross_v, cross_o, mlp_gate, mlp_up, mlp_down):
        layers, width = norm_self.shape
        w_so = self_o.reshape(layers, width, width)
        w_co = cross_o.reshape(layers, width, width)
        dev = lax.axis_index('sp')
        dev_arr = dev.astype(jnp.int32).reshape(1)
        bases = jnp.array(BASES, jnp.int32)[dev]
        lims = jnp.clip(mem_len[0] - bases, 0, CH)
        is3 = (dev_arr == 3).astype(jnp.int32)

        def swap(x):
            return lax.ppermute(x, 'sp', [(0, 1), (1, 0), (2, 3), (3, 2)])

        def program(hidden):
            far = lax.ppermute(hidden, 'sp', [(0, 2), (1, 3)])
            mem_a, mem_b = memory[:CH], memory[CH:]
            c2b = lax.ppermute(mem_b, 'sp', [(2, 3)])
            rem_a = lax.ppermute(mem_a, 'sp', [(0, 2), (1, 3), (2, 0)])
            rem_b = lax.ppermute(mem_b, 'sp', [(0, 2), (1, 3), (2, 1)])

            both = (0, layers)
            ka, va = kv_project(lims[0:2], is3, [memory, c2b], cross_k, cross_v, 2 * CH, both)
            kas, vas = swap(ka), swap(va)
            kb, vb = kv_project(lims[4:5], is3, [rem_a], cross_k, cross_v, CH, both)
            kbs, vbs = swap(kb), swap(vb)
            kvs = []
            for layer in range(layers):
                kc, vc = kv_project(lims[6:7], is3, [rem_b], cross_k, cross_v, CH, (layer, 1))
                kcs, vcs = swap(kc), swap(vc)
                kvs.append([(ka, va, layer), (kas, vas, layer), (kb, vb, layer), (kbs, vbs, layer), (kc, vc, 0), (kcs, vcs, 0)])

            for layer in range(layers):
                hidden, q = self_attention(layer, hidden, far, norm_self, norm_cross, self_q, self_k, self_v, w_so, cross_q)
                hidden = cross_mlp(layer, lims, q, kvs[layer], hidden, norm_mlp, w_co, mlp_gate, mlp_up, mlp_down)
                far = None
            return hidden

        return program(hidden)

    return jax.shard_map(local_step, mesh=mesh, in_specs=(row_spec, row_spec, P('dp')) + (P(),) * 14, out_specs=row_spec, check_vma=False)
```

```python
import functools

import jax
import jax.numpy as jnp
from jax import lax
from jax.experimental import pallas as pl
from jax.experimental.pallas import tpu as pltpu
from jax.sharding import PartitionSpec as P


EPS = 1e-6
NEG_BIG = -1e30
F32 = jnp.float32
BF16 = jnp.bfloat16
CH = 512
HEADS = 4
GW = HEADS * 64
VMEM_LIMIT = 62 * 1024 * 1024
ANY = pl.BlockSpec(memory_space=pl.ANY)
SMEM = pl.BlockSpec(memory_space=pltpu.SMEM)
VMEM = pl.BlockSpec(memory_space=pltpu.VMEM)


def rms(h, gain):
    h32 = h.astype(F32)
    inv = lax.rsqrt(jnp.mean(h32 * h32, axis=-1, keepdims=True) + EPS)
    return (h32 * inv * gain.astype(F32)).astype(BF16)


def dot(a, b):
    return jnp.dot(a, b, preferred_element_type=F32)


def kv_kernel(layers, n_src, lim_ref, pick_ref, *refs):
    srcs, (wk, wv, k_out, vt_out, mem, w_s, k_s, vt_s, sem, w_sems, o_sems) = refs[:n_src], refs[n_src:]
    rows = mem.shape[0]
    lo, n = layers

    def from_src(go):
        if n_src == 1:
            go(pltpu.make_async_copy(srcs[0], mem, sem))
        else:
            @pl.when(pick_ref[0] == 0)
            def _():
                go(pltpu.make_async_copy(srcs[0], mem, sem))

            @pl.when(pick_ref[0] != 0)
            def _():
                go(pltpu.make_async_copy(srcs[1], mem.at[pl.ds(0, CH)], sem))

    def w_copy(i, v):
        return pltpu.make_async_copy((wk, wv)[v].at[lo + i], w_s.at[2 * i + v], w_sems.at[2 * i + v])

    w_copy(0, 0).start()
    from_src(lambda cp: cp.start())
    for i in range(n):
        for v in range(2):
            if i + v > 0:
                w_copy(i, v).start()
    from_src(lambda cp: cp.wait())

    def out_copy(i, v, c):
        at = pl.ds(pl.multiple_of(c * CH, CH), CH)
        if v == 0:
            return pltpu.make_async_copy(k_s.at[i, at, :], k_out.at[i, at, :], o_sems.at[i, v, c])
        return pltpu.make_async_copy(vt_s.at[i, :, at], vt_out.at[i, :, at], o_sems.at[i, v, c])

    def valid(c, go):
        @pl.when(lim_ref[c] > 0)
        def _():
            go()

    def layer_step(i, _):
        for v in range(2):
            w_copy(i, v).wait()

            def chunk_step(c, _):
                def work():
                    def step(r, _):
                        at = pl.ds(pl.multiple_of(c * CH + r * 256, 256), 256)
                        out = dot(mem[at, :], w_s[2 * i + v]).astype(BF16)
                        if v == 0:
                            k_s[i, at, :] = out
                        else:
                            vt_s[i, :, at] = out.T
                        return 0

                    lax.fori_loop(0, CH // 256, step, 0)
                    out_copy(i, v, c).start()

                valid(c, work)
                return 0

            lax.fori_loop(0, rows // CH, chunk_step, 0)
        return 0

    lax.fori_loop(0, n, layer_step, 0)
    for i in range(n):
        for v in range(2):
            for c in range(rows // CH):
                valid(c, lambda i=i, v=v, c=c: out_copy(i, v, c).wait())


def kv_project(lims, pick, srcs, wk, wv, rows, layers):
    width, cols = wk.shape[1], wk.shape[2]
    n = layers[1]
    flops = n * 4 * rows * width * cols
    return pl.pallas_call(
        functools.partial(kv_kernel, layers, len(srcs)),
        in_specs=[SMEM, SMEM] + [ANY] * (len(srcs) + 2),
        out_specs=[ANY, ANY],
        out_shape=[jax.ShapeDtypeStruct((n, rows, cols), BF16), jax.ShapeDtypeStruct((n, cols, rows), BF16)],
        scratch_shapes=[
            pltpu.VMEM((rows, width), BF16),
            pltpu.VMEM((2 * n, width, cols), BF16),
            pltpu.VMEM((n, rows, cols), BF16),
            pltpu.VMEM((n, cols, rows), BF16),
            pltpu.SemaphoreType.DMA,
            pltpu.SemaphoreType.DMA((2 * n,)),
            pltpu.SemaphoreType.DMA((n, 2, rows // CH)),
        ],
        cost_estimate=pl.CostEstimate(flops=flops, bytes_accessed=n * 4 * width * cols, transcendentals=0),
        compiler_params=pltpu.CompilerParams(vmem_limit_bytes=48 * 1024 * 1024),
        name="kv_project",
    )(lims, pick, *srcs, wk, wv)


def head_queries(qt, extra=None):
    row = lax.broadcasted_iota(jnp.int32, (128, qt.shape[1]), 0)
    out = []
    for h in range(HEADS):
        pair = qt[h // 2 * 128:(h // 2 + 1) * 128, :]
        q = jnp.where((row < 64) == (h % 2 == 0), pair, jnp.zeros_like(pair))
        out.append(q if extra is None else jnp.concatenate([q, extra], axis=0))
    return out


def attend_all(groups, n_chunks, scores, values, enter, leave, scratch):
    s_refs, mx_refs, (m_ref, l_ref, acc_ref) = scratch[:2], scratch[2:4], scratch[4:]
    total = groups * n_chunks

    def stage1(group, j, buf):
        for h, s in enumerate(scores(group, j)):
            first(h, s, buf)

    def first(h, s, buf):
        s_refs[buf][h] = s
        mx_refs[buf][h:h + 1, :] = jnp.max(s, axis=0, keepdims=True)

    def second(group, h, vt, buf):
        m_old = m_ref[group, h:h + 1, :]
        m_new = jnp.maximum(m_old, mx_refs[buf][h:h + 1, :])
        p = jnp.exp(s_refs[buf][h] - m_new)
        alpha = jnp.exp(m_old - m_new)
        m_ref[group, h:h + 1, :] = m_new
        l_ref[group, h:h + 1, :] = l_ref[group, h:h + 1, :] * alpha + jnp.sum(p, axis=0, keepdims=True)
        acc_ref[group, h] = acc_ref[group, h] * alpha + dot(vt[h * 64:(h + 1) * 64, :], p.astype(BF16))

    def advance(group, j):
        wrap = j + 1 == n_chunks
        return jnp.where(wrap, group + 1, group), jnp.where(wrap, 0, j + 1)

    enter(0)
    stage1(0, 0, 0)

    def item(group, j, buf):
        group_next, j_next = advance(group, j)

        @pl.when((j_next == 0) & (group_next < groups))
        def _():
            enter(group_next)

        made = scores(jnp.minimum(group_next, groups - 1), j_next)
        vt = values(group, j)
        for h in range(HEADS):
            first(h, next(made), 1 - buf)
            second(group, h, vt, buf)

        @pl.when(j_next == 0)
        def _():
            leave(group)

    def step(u, now):
        item(*now, 0)
        now = advance(*now)

        @pl.when(2 * u + 1 < total)
        def _():
            item(*now, 1)

        return advance(*now)

    lax.fori_loop(0, (total + 1) // 2, step, (jnp.int32(0), jnp.int32(0)))


def attend_reset(scratch):
    m_ref, l_ref, acc_ref = scratch[4:]
    m_ref[...] = jnp.full_like(m_ref, -jnp.inf)
    l_ref[...] = jnp.zeros_like(l_ref)
    acc_ref[...] = jnp.zeros_like(acc_ref)


def attend_finish(group, at_ref, scratch):
    l_ref, acc_ref = scratch[5:]
    for h in range(HEADS):
        rows = pl.ds(pl.multiple_of(group * HEADS * 64 + h * 64, 64), 64)
        at_ref[rows, :] = (acc_ref[group, h] / l_ref[group, h:h + 1, :]).astype(BF16)


def attend_scratch(groups, rows):
    return [
        pltpu.VMEM((HEADS, CH, rows), F32),
        pltpu.VMEM((HEADS, CH, rows), F32),
        pltpu.VMEM((HEADS, rows), F32),
        pltpu.VMEM((HEADS, rows), F32),
        pltpu.VMEM((groups, HEADS, rows), F32),
        pltpu.VMEM((groups, HEADS, rows), F32),
        pltpu.VMEM((groups, HEADS, 64, rows), F32),
    ]


def self_kernel(layer, far_given, *refs):
    own_ref, refs = refs[0], refs[1:]
    if far_given:
        s2, refs = refs[0], refs[1:]
    gs_ref, gc_ref, wq, wk, wv, wo, wcq, hid_ref, q_ref, w_s, x_s, k_s, vt_s, qs, bias, at_s, a_s, s1, s3 = refs[:19]
    refs = refs[19:]
    if not far_given:
        s2, refs = refs[0], refs[1:]
    scratch, (sems, near_sems, far_sems, fwd_sems) = refs[:7], refs[7:]
    rows, width = own_ref.shape
    parts = far_sems.shape[1]
    parts_half = parts // 2
    dev = lax.axis_index("sp")
    odd = lax.rem(dev, 2)
    chip1 = dev >= 2
    sibling = dev + 1 - 2 * odd
    across = lax.rem(dev + 2, 4)

    w_copies = [pltpu.make_async_copy(src.at[layer], w_s.at[n], sems.at[n]) for n, src in enumerate((wk, wv, wq, wo, wcq))]
    w_copies[0].start()
    w_copies[1].start()

    barrier = pltpu.get_barrier_semaphore()
    others = (sibling,) if far_given else (sibling, across)
    for other in others:
        pl.semaphore_signal(barrier, inc=1, device_id={"sp": other}, device_id_type=pl.DeviceIdType.MESH)
    pl.semaphore_wait(barrier, len(others))

    def send(src, dst, sem, other):
        return pltpu.make_async_remote_copy(src_ref=src, dst_ref=dst, send_sem=sem.at[0], recv_sem=sem.at[1],
                                            device_id={"sp": other}, device_id_type=pl.DeviceIdType.MESH)

    def part(i):
        return pl.ds(i * (rows // parts), rows // parts)

    near = send(own_ref, s1, near_sems, sibling)
    far = [send(own_ref.at[part(i)], s2.at[part(i)], far_sems.at[:, i], across) for i in range(parts)]
    fwd = [send(s2.at[part(i)], s3.at[part(i)], fwd_sems.at[:, i], sibling) for i in range(parts)]

    if not far_given:
        @pl.when(jnp.logical_not(chip1))
        def _():
            for cp in far:
                cp.start()

    @pl.when(odd == 0)
    def _():
        near.start()

    if far_given:
        @pl.when(chip1)
        def _():
            for cp in fwd:
                cp.start()

    gain = gs_ref[layer:layer + 1, :]
    x_s[pl.ds(0, rows), :] = rms(own_ref[...], gain)
    key = lax.broadcasted_iota(jnp.int32, (rows, rows), 0)
    query = lax.broadcasted_iota(jnp.int32, (rows, rows), 1)
    bias[0, pl.ds(0, rows), :] = jnp.where(key <= query, 0.0, NEG_BIG)
    bias[0, pl.ds(rows, rows), :] = jnp.full((rows, rows), jnp.where(odd == 1, 0.0, NEG_BIG), F32)
    bias[1] = jnp.zeros((2 * rows, rows), F32)
    attend_reset(scratch)

    @pl.when(odd == 1)
    def _():
        near.wait_recv()
        x_s[pl.ds(rows, rows), :] = rms(s1[...], gain)

    @pl.when(odd == 0)
    def _():
        x_s[pl.ds(rows, rows), :] = jnp.zeros((rows, width), BF16)

    def tile(t):
        return pl.ds(pl.multiple_of(t * 256, 256), 256)

    def head_cols(i):
        return pl.ds(pl.multiple_of(i * GW, GW), GW)

    def phase(half, _):
        at = pl.ds(pl.multiple_of(half * CH, CH), CH)

        @pl.when(half == 0)
        def _():
            w_copies[0].wait()
            w_copies[2].start()

        def project_step(r, _):
            rows_at = tile(2 * half + r)
            for first in range(0, parts, parts_half):
                @pl.when((half == 1) & (r == first // parts_half))
                def _(first=first):
                    some = range(first, first + parts_half)
                    if not far_given:
                        for i in some:
                            far[i].wait_recv()
                            fwd[i].start()
                    here = pl.ds(first * (rows // parts), rows // 2)
                    x_s[pl.ds(2 * rows + 2 * first * (rows // parts), rows // 2), :] = rms(s2[here, :], gain)
                    for i in some:
                        fwd[i].wait_recv()
                    x_s[pl.ds(2 * rows + 2 * first * (rows // parts) + rows // 2, rows // 2), :] = rms(s3[here, :], gain)

            k_s[rows_at, :] = dot(x_s[rows_at, :], w_s[0]).astype(BF16)

            @pl.when((half == 0) & (r == 0))
            def _():
                w_copies[1].wait()
                w_copies[3].start()

            vt_s[:, rows_at] = dot(x_s[rows_at, :], w_s[1]).astype(BF16).T
            return 0

        lax.fori_loop(0, 2, project_step, 0)

        @pl.when(half == 0)
        def _():
            w_copies[2].wait()
            w_copies[4].start()

            qs[...] = (dot(x_s[pl.ds(0, rows), :], w_s[2]).astype(BF16) * BF16(0.125)).T

        def scores(i, j):
            k = k_s[at, head_cols(i)]
            return (dot(k[:, h // 2 * 128:(h // 2 + 1) * 128], q) + bias[half] for h, q in enumerate(head_queries(qs[head_cols(i), :])))

        attend_all(width // GW, 1, scores, lambda i, j: vt_s[head_cols(i), at], lambda i: None, lambda i: None, scratch)
        return 0

    lax.fori_loop(0, jnp.where(chip1, 2, 1), phase, 0)

    def finish(i, _):
        attend_finish(i, at_s, scratch)
        return 0

    lax.fori_loop(0, width // GW, finish, 0)
    a_s[...] = at_s[...].T
    w_copies[3].wait()

    hid_ref[...] = (own_ref[...].astype(F32) + dot(a_s[...], w_s[3])).astype(BF16)
    a_s[...] = rms(hid_ref[...], gc_ref[layer:layer + 1, :])
    w_copies[4].wait()

    q_ref[...] = (dot(a_s[...], w_s[4]).astype(BF16) * BF16(0.125)).T

    @pl.when(odd == 0)
    def _():
        near.wait_send()

    @pl.when(chip1)
    def _():
        for cp in fwd:
            cp.wait_send()

    if not far_given:
        @pl.when(jnp.logical_not(chip1))
        def _():
            for cp in far:
                cp.wait_send()


def self_attention(layer, own, far, gs, gc, wq, wk, wv, wo, wcq):
    rows, width = own.shape
    far_given = far is not None
    parts = 2 if far_given else 4
    shape = jax.ShapeDtypeStruct((rows, width), BF16)
    flops = 2 * rows * width * width * 11 + 4 * rows * 4 * rows * width
    block = pltpu.VMEM((rows, width), BF16)
    return pl.pallas_call(
        functools.partial(self_kernel, layer, far_given),
        in_specs=[VMEM] * (4 if far_given else 3) + [ANY] * 5,
        out_specs=[VMEM, VMEM],
        out_shape=[shape, jax.ShapeDtypeStruct((width, rows), BF16)],
        scratch_shapes=[
            pltpu.VMEM((5, width, width), BF16),
            pltpu.VMEM((4 * rows, width), BF16),
            pltpu.VMEM((4 * rows, width), BF16),
            pltpu.VMEM((width, 4 * rows), BF16),
            pltpu.VMEM((width, rows), BF16),
            pltpu.VMEM((2, 2 * rows, rows), F32),
            pltpu.VMEM((width, rows), BF16),
            block,
            block,
            block,
            *([] if far_given else [block]),
            *attend_scratch(width // GW, rows),
            pltpu.SemaphoreType.DMA((5,)),
            pltpu.SemaphoreType.DMA((2,)),
            pltpu.SemaphoreType.DMA((2, parts)),
            pltpu.SemaphoreType.DMA((2, parts)),
        ],
        cost_estimate=pl.CostEstimate(flops=flops, bytes_accessed=10 * width * width, transcendentals=0),
        compiler_params=pltpu.CompilerParams(vmem_limit_bytes=VMEM_LIMIT, collective_id=layer, has_side_effects=True),
        name="self_attention",
    )(own, *([far] if far_given else []), gs, gc, wq, wk, wv, wo, wcq)


def cross_kernel(layer, planes, n_kv, lim_ref, q_ref, *refs):
    def take(n):
        nonlocal refs
        head, refs = refs[:n], refs[n:]
        return head

    ks, vts = take(n_kv), take(n_kv)
    hid_ref, gm_ref, wco, wg, wu, wd, out_ref = take(7)
    scratch = take(7)
    kbuf, vbuf, mask, list_s, kv_sems = take(5)
    at_s, a_s, act0, act1, acc_o, wo_s, wg_s, wu_s, wd_s, o_sem, w_sems = take(11)
    steps, ff, down = wg_s.shape[0], wg_s.shape[2], wd_s.shape[0]
    width, rows = q_ref.shape
    groups = width // GW

    def kv_copies(i):
        slot = lax.rem(i, 2)
        cols = pl.ds(pl.multiple_of(i * GW, GW), GW)
        out, at = [], 0
        for n in range(n_kv):
            n_rows = ks[n].shape[1]
            out.append(pltpu.make_async_copy(ks[n].at[planes[n], :, cols], kbuf.at[slot, pl.ds(at, n_rows), :], kv_sems.at[slot, 0, n]))
            out.append(pltpu.make_async_copy(vts[n].at[planes[n], cols, :], vbuf.at[slot, :, pl.ds(at, n_rows)], kv_sems.at[slot, 1, n]))
            at += n_rows
        return out

    for i in range(2):
        for cp in kv_copies(i):
            cp.start()
    o_copy = pltpu.make_async_copy(wco.at[layer], wo_s, o_sem)

    def w_copies(j):
        cols = pl.ds(pl.multiple_of(j * ff, ff), ff)
        return (pltpu.make_async_copy(wg.at[layer, :, cols], wg_s.at[j], w_sems.at[0, j]),
                pltpu.make_async_copy(wu.at[layer, :, cols], wu_s.at[j], w_sems.at[1, j]),
                pltpu.make_async_copy(wd.at[layer, cols, :], wd_s.at[lax.rem(j, down)], w_sems.at[2, j]))

    attend_reset(scratch)

    n_chunks, last = jnp.int32(0), jnp.int32(0)
    list_s[0] = 0
    for c in range(lim_ref.shape[0]):
        lim = lim_ref[c]

        @pl.when(lim > 0)
        def _(c=c, at=n_chunks):
            list_s[at] = c

        n_chunks = n_chunks + (lim > 0).astype(jnp.int32)
        last = last + jnp.where(lim < CH, lim, 0)
    key = lax.broadcasted_iota(jnp.int32, (CH, 128), 0)
    lane = lax.broadcasted_iota(jnp.int32, (CH, 128), 1)
    mask[0] = jnp.zeros((CH, 128), BF16)
    mask[1] = jnp.where((key >= last) & (lane == 0), NEG_BIG, 0.0).astype(BF16)
    ones = (lax.broadcasted_iota(jnp.int32, (128, rows), 0) == 0).astype(F32).astype(BF16)

    def enter(i):
        for cp in kv_copies(i):
            cp.wait()

        @pl.when(i == 0)
        def _():
            o_copy.start()

        for j in range(2):
            gate_copy, up_copy, down_copy = w_copies(2 * i + j)
            gate_copy.start()
            up_copy.start()

            @pl.when(2 * i + j < down)
            def _(down_copy=down_copy):
                down_copy.start()

    def leave(i):
        @pl.when(i + 2 < groups)
        def _():
            for cp in kv_copies(i + 2):
                cp.start()

    def chunk(j):
        return pl.ds(pl.multiple_of(list_s[j] * CH, CH), CH)

    def scores(i, j):
        partial = (lim_ref[list_s[j]] < CH).astype(jnp.int32)
        k = kbuf[lax.rem(i, 2), chunk(j), :]
        ks = [jnp.concatenate([k[:, p * 128:(p + 1) * 128], mask[partial]], axis=1) for p in range(HEADS // 2)]
        queries = head_queries(q_ref[pl.ds(pl.multiple_of(i * GW, GW), GW), :], ones)
        return (dot(ks[h // 2], q) for h, q in enumerate(queries))

    def values(i, j):
        return vbuf[lax.rem(i, 2), :, chunk(j)]

    attend_all(groups, n_chunks, scores, values, enter, leave, scratch)

    def finish(i, _):
        attend_finish(i, at_s, scratch)
        return 0

    lax.fori_loop(0, groups, finish, 0)
    a_s[...] = at_s[...].T
    o_copy.wait()

    out_ref[...] = (hid_ref[...].astype(F32) + dot(a_s[...], wo_s[...])).astype(BF16)
    a_s[...] = rms(out_ref[...], gm_ref[layer:layer + 1, :])
    acc_o[...] = jnp.zeros_like(acc_o)

    def wait_gate_up(j):
        for cp in w_copies(j)[:2]:
            cp.wait()

    def gate_up(j, act_ref):
        x = a_s[...]
        gate = dot(x, wg_s[j])
        up = dot(x, wu_s[j])
        act_ref[...] = (gate / (1.0 + jnp.exp(-gate)) * up).astype(BF16)

    wait_gate_up(0)
    gate_up(0, act0)

    def mlp_step(u, _):
        for now, later, at in ((act0, act1, 0), (act1, act0, 1)):
            j = 2 * u + at
            w_copies(j)[2].wait()
            following = jnp.minimum(j + 1, steps - 1)

            @pl.when(j + 1 < steps)
            def _(j=j):
                wait_gate_up(j + 1)

            acc_o[...] += dot(now[...], wd_s[lax.rem(j, down)])
            gate_up(following, later)

            @pl.when(j + down < steps)
            def _(j=j):
                w_copies(j + down)[2].start()
        return 0

    lax.fori_loop(0, steps // 2, mlp_step, 0)
    out_ref[...] = (out_ref[...].astype(F32) + acc_o[...]).astype(BF16)


def cross_mlp(layer, lims, q, kvs, hid, gm, wco, wg, wu, wd):
    width, rows = q.shape
    groups = width // GW
    planes = tuple(plane for _, _, plane in kvs)
    ks, vts = [k for k, _, _ in kvs], [v for _, v, _ in kvs]
    total = sum(k.shape[1] for k in ks)
    n = len(kvs)
    steps = 2 * groups
    ff = wg.shape[2] // steps
    return pl.pallas_call(
        functools.partial(cross_kernel, layer, planes, n),
        in_specs=[SMEM, VMEM] + [ANY] * (2 * n) + [VMEM] * 2 + [ANY] * 4,
        out_specs=VMEM,
        out_shape=jax.ShapeDtypeStruct((rows, width), BF16),
        scratch_shapes=attend_scratch(groups, rows) + [
            pltpu.VMEM((2, total, GW), BF16),
            pltpu.VMEM((2, GW, total), BF16),
            pltpu.VMEM((2, CH, 128), BF16),
            pltpu.SMEM((8,), jnp.int32),
            pltpu.SemaphoreType.DMA((2, 2, n)),
            pltpu.VMEM((width, rows), BF16),
            pltpu.VMEM((rows, width), BF16),
            pltpu.VMEM((rows, ff), BF16),
            pltpu.VMEM((rows, ff), BF16),
            pltpu.VMEM((rows, width), F32),
            pltpu.VMEM((width, width), BF16),
            pltpu.VMEM((steps, width, ff), BF16),
            pltpu.VMEM((steps, width, ff), BF16),
            pltpu.VMEM((steps - 2, ff, width), BF16),
            pltpu.SemaphoreType.DMA,
            pltpu.SemaphoreType.DMA((3, steps)),
        ],
        cost_estimate=pl.CostEstimate(
            flops=4 * rows * 3072 * width + 2 * rows * width * (width + 3 * wg.shape[2]),
            bytes_accessed=2 * width * (width + 3 * wg.shape[2]), transcendentals=0),
        compiler_params=pltpu.CompilerParams(vmem_limit_bytes=VMEM_LIMIT),
        name="cross_mlp",
    )(lims, q, *ks, *vts, hid, gm, wco, wg, wu, wd)


NONE = 1 << 20
BASES = (
    (0, 512, 1024, 1536, 2048, NONE, NONE, 2560),
    (1024, 1536, 0, 512, NONE, 2048, 2560, NONE),
    (2048, NONE, 2560, NONE, 0, 1024, 512, 1536),
    (2560, NONE, 2048, NONE, 1024, 0, 1536, 512),
)


def solution(mesh):
    row_spec = P(('dp', 'sp'), None)

    def local_step(hidden, memory, mem_len, norm_self, norm_cross, norm_mlp, self_q, self_k, self_v, self_o, cross_q, cross_k, cross_v, cross_o, mlp_gate, mlp_up, mlp_down):
        layers, width = norm_self.shape
        w_so = self_o.reshape(layers, width, width)
        w_co = cross_o.reshape(layers, width, width)
        dev = lax.axis_index('sp')
        dev_arr = dev.astype(jnp.int32).reshape(1)
        bases = jnp.array(BASES, jnp.int32)[dev]
        lims = jnp.clip(mem_len[0] - bases, 0, CH)
        is3 = (dev_arr == 3).astype(jnp.int32)

        def swap(x):
            return lax.ppermute(x, 'sp', [(0, 1), (1, 0), (2, 3), (3, 2)])

        def program(hidden):
            far = lax.ppermute(hidden, 'sp', [(0, 2), (1, 3)])
            mem_a, mem_b = memory[:CH], memory[CH:]
            c2b = lax.ppermute(mem_b, 'sp', [(2, 3)])
            rem_a = lax.ppermute(mem_a, 'sp', [(0, 2), (1, 3), (2, 0)])
            rem_b = lax.ppermute(mem_b, 'sp', [(0, 2), (1, 3), (2, 1)])

            both = (0, layers)
            ka, va = kv_project(lims[0:2], is3, [memory, c2b], cross_k, cross_v, 2 * CH, both)
            kas, vas = swap(ka), swap(va)
            kb, vb = kv_project(lims[4:5], is3, [rem_a], cross_k, cross_v, CH, both)
            kbs, vbs = swap(kb), swap(vb)
            kvs = []
            for layer in range(layers):
                kc, vc = kv_project(lims[6:7], is3, [rem_b], cross_k, cross_v, CH, (layer, 1))
                kcs, vcs = swap(kc), swap(vc)
                kvs.append([(ka, va, layer), (kas, vas, layer), (kb, vb, layer), (kbs, vbs, layer), (kc, vc, 0), (kcs, vcs, 0)])

            for layer in range(layers):
                hidden, q = self_attention(layer, hidden, far, norm_self, norm_cross, self_q, self_k, self_v, w_so, cross_q)
                hidden = cross_mlp(layer, lims, q, kvs[layer], hidden, norm_mlp, w_co, mlp_gate, mlp_up, mlp_down)
                far = None
            return hidden

        return program(hidden)

    return jax.shard_map(local_step, mesh=mesh, in_specs=(row_spec, row_spec, P('dp')) + (P(),) * 14, out_specs=row_spec, check_vma=False)
```

```python
import functools

import jax
import jax.numpy as jnp
from jax import lax
from jax.experimental import pallas as pl
from jax.experimental.pallas import tpu as pltpu
from jax.sharding import PartitionSpec as P


EPS = 1e-6
NEG_BIG = -1e30
F32 = jnp.float32
BF16 = jnp.bfloat16
CH = 512
HEADS = 4
GW = HEADS * 64
VMEM_LIMIT = 62 * 1024 * 1024
ANY = pl.BlockSpec(memory_space=pltpu.HBM)
SMEM = pl.BlockSpec(memory_space=pltpu.SMEM)
VMEM = pl.BlockSpec(memory_space=pltpu.VMEM)


def rms(h, gain):
    h32 = h.astype(F32)
    inv = lax.rsqrt(jnp.mean(h32 * h32, axis=-1, keepdims=True) + EPS)
    return (h32 * inv * gain.astype(F32)).astype(BF16)


def dot(a, b):
    return jnp.dot(a, b, preferred_element_type=F32)


def kv_kernel(layers, n_src, lim_ref, pick_ref, *refs):
    srcs, (wk, wv, k_out, vt_out, mem, w_s, k_s, vt_s, sem, w_sems, o_sems) = refs[:n_src], refs[n_src:]
    rows = mem.shape[0]
    lo, n = layers

    def from_src(go):
        if n_src == 1:
            go(pltpu.make_async_copy(srcs[0], mem, sem))
        else:
            @pl.when(pick_ref[0] == 0)
            def _():
                go(pltpu.make_async_copy(srcs[0], mem, sem))

            @pl.when(pick_ref[0] != 0)
            def _():
                go(pltpu.make_async_copy(srcs[1], mem.at[pl.ds(0, CH)], sem))

    def w_copy(i, v):
        return pltpu.make_async_copy((wk, wv)[v].at[lo + i], w_s.at[2 * i + v], w_sems.at[2 * i + v])

    w_copy(0, 0).start()
    from_src(lambda cp: cp.start())
    for i in range(n):
        for v in range(2):
            if i + v > 0:
                w_copy(i, v).start()
    from_src(lambda cp: cp.wait())

    def out_copy(i, v, c):
        at = pl.ds(pl.multiple_of(c * CH, CH), CH)
        if v == 0:
            return pltpu.make_async_copy(k_s.at[i, at, :], k_out.at[i, at, :], o_sems.at[i, v, c])
        return pltpu.make_async_copy(vt_s.at[i, :, at], vt_out.at[i, :, at], o_sems.at[i, v, c])

    def valid(c, go):
        @pl.when(lim_ref[c] > 0)
        def _():
            go()

    def layer_step(i, _):
        for v in range(2):
            w_copy(i, v).wait()

            def chunk_step(c, _):
                def work():
                    def step(r, _):
                        at = pl.ds(pl.multiple_of(c * CH + r * 256, 256), 256)
                        out = dot(mem[at, :], w_s[2 * i + v]).astype(BF16)
                        if v == 0:
                            k_s[i, at, :] = out
                        else:
                            vt_s[i, :, at] = out.T
                        return 0

                    lax.fori_loop(0, CH // 256, step, 0)
                    out_copy(i, v, c).start()

                valid(c, work)
                return 0

            lax.fori_loop(0, rows // CH, chunk_step, 0)
        return 0

    lax.fori_loop(0, n, layer_step, 0)
    for i in range(n):
        for v in range(2):
            for c in range(rows // CH):
                valid(c, lambda i=i, v=v, c=c: out_copy(i, v, c).wait())


def kv_project(lims, pick, srcs, wk, wv, rows, layers):
    width, cols = wk.shape[1], wk.shape[2]
    n = layers[1]
    flops = n * 4 * rows * width * cols
    return pl.pallas_call(
        functools.partial(kv_kernel, layers, len(srcs)),
        in_specs=[SMEM, SMEM] + [ANY] * (len(srcs) + 2),
        out_specs=[ANY, ANY],
        out_shape=[jax.ShapeDtypeStruct((n, rows, cols), BF16), jax.ShapeDtypeStruct((n, cols, rows), BF16)],
        scratch_shapes=[
            pltpu.VMEM((rows, width), BF16),
            pltpu.VMEM((2 * n, width, cols), BF16),
            pltpu.VMEM((n, rows, cols), BF16),
            pltpu.VMEM((n, cols, rows), BF16),
            pltpu.SemaphoreType.DMA,
            pltpu.SemaphoreType.DMA((2 * n,)),
            pltpu.SemaphoreType.DMA((n, 2, rows // CH)),
        ],
        cost_estimate=pl.CostEstimate(flops=flops, bytes_accessed=n * 4 * width * cols, transcendentals=0),
        compiler_params=pltpu.CompilerParams(vmem_limit_bytes=VMEM_LIMIT),
        name="kv_project",
    )(lims, pick, *srcs, wk, wv)


def head_queries(qt, extra=None):
    row = lax.broadcasted_iota(jnp.int32, (128, qt.shape[1]), 0)
    out = []
    for h in range(HEADS):
        pair = qt[h // 2 * 128:(h // 2 + 1) * 128, :]
        q = jnp.where((row < 64) == (h % 2 == 0), pair, jnp.zeros_like(pair))
        out.append(q if extra is None else jnp.concatenate([q, extra], axis=0))
    return out


def attend_all(groups, n_chunks, scores, values, enter, leave, scratch):
    s_refs, mx_refs, (m_ref, l_ref, acc_ref) = scratch[:2], scratch[2:4], scratch[4:]
    total = groups * n_chunks

    def stage1(group, j, buf):
        for h, s in enumerate(scores(group, j)):
            first(h, s, buf)

    def first(h, s, buf):
        s_refs[buf][h] = s
        mx_refs[buf][h:h + 1, :] = jnp.max(s, axis=0, keepdims=True)

    def second(group, h, vt, buf):
        m_old = m_ref[group, h:h + 1, :]
        m_new = jnp.maximum(m_old, mx_refs[buf][h:h + 1, :])
        p = jnp.exp(s_refs[buf][h] - m_new)
        alpha = jnp.exp(m_old - m_new)
        m_ref[group, h:h + 1, :] = m_new
        l_ref[group, h:h + 1, :] = l_ref[group, h:h + 1, :] * alpha + jnp.sum(p, axis=0, keepdims=True)
        acc_ref[group, h] = acc_ref[group, h] * alpha + dot(vt[h * 64:(h + 1) * 64, :], p.astype(BF16))

    def advance(group, j):
        wrap = j + 1 == n_chunks
        return jnp.where(wrap, group + 1, group), jnp.where(wrap, 0, j + 1)

    enter(0)
    stage1(0, 0, 0)

    def item(group, j, buf):
        group_next, j_next = advance(group, j)

        @pl.when((j_next == 0) & (group_next < groups))
        def _():
            enter(group_next)

        made = scores(jnp.minimum(group_next, groups - 1), j_next)
        vt = values(group, j)
        for h in range(HEADS):
            first(h, next(made), 1 - buf)
            second(group, h, vt, buf)

        @pl.when(j_next == 0)
        def _():
            leave(group)

    def step(u, now):
        item(*now, 0)
        now = advance(*now)

        @pl.when(2 * u + 1 < total)
        def _():
            item(*now, 1)

        return advance(*now)

    lax.fori_loop(0, (total + 1) // 2, step, (jnp.int32(0), jnp.int32(0)))


def attend_reset(scratch):
    m_ref, l_ref, acc_ref = scratch[4:]
    m_ref[...] = jnp.full_like(m_ref, -jnp.inf)
    l_ref[...] = jnp.zeros_like(l_ref)
    acc_ref[...] = jnp.zeros_like(acc_ref)


def attend_finish(group, at_ref, scratch):
    l_ref, acc_ref = scratch[5:]
    for h in range(HEADS):
        rows = pl.ds(pl.multiple_of(group * HEADS * 64 + h * 64, 64), 64)
        at_ref[rows, :] = (acc_ref[group, h] / l_ref[group, h:h + 1, :]).astype(BF16)


def attend_scratch(groups, rows):
    return [
        pltpu.VMEM((HEADS, CH, rows), F32),
        pltpu.VMEM((HEADS, CH, rows), F32),
        pltpu.VMEM((HEADS, rows), F32),
        pltpu.VMEM((HEADS, rows), F32),
        pltpu.VMEM((groups, HEADS, rows), F32),
        pltpu.VMEM((groups, HEADS, rows), F32),
        pltpu.VMEM((groups, HEADS, 64, rows), F32),
    ]


def self_kernel(layer, far_given, *refs):
    own_ref, refs = refs[0], refs[1:]
    if far_given:
        s2, refs = refs[0], refs[1:]
    gs_ref, gc_ref, wq, wk, wv, wo, wcq, hid_ref, q_ref, w_s, x_s, k_s, vt_s, qs, bias, at_s, a_s, s1, s3 = refs[:19]
    refs = refs[19:]
    if not far_given:
        s2, refs = refs[0], refs[1:]
    scratch, (sems, near_sems, far_sems, fwd_sems) = refs[:7], refs[7:]
    rows, width = own_ref.shape
    parts = far_sems.shape[1]
    parts_half = parts // 2
    dev = lax.axis_index("sp")
    odd = lax.rem(dev, 2)
    chip1 = dev >= 2
    sibling = dev + 1 - 2 * odd
    across = lax.rem(dev + 2, 4)

    w_copies = [pltpu.make_async_copy(src.at[layer], w_s.at[n], sems.at[n]) for n, src in enumerate((wk, wv, wq, wo, wcq))]
    w_copies[0].start()
    w_copies[1].start()

    barrier = pltpu.get_barrier_semaphore()
    others = (sibling,) if far_given else (sibling, across)
    for other in others:
        pl.semaphore_signal(barrier, inc=1, device_id={"sp": other}, device_id_type=pl.DeviceIdType.MESH)
    pl.semaphore_wait(barrier, len(others))

    def send(src, dst, sem, other):
        return pltpu.make_async_remote_copy(src_ref=src, dst_ref=dst, send_sem=sem.at[0], recv_sem=sem.at[1],
                                            device_id={"sp": other}, device_id_type=pl.DeviceIdType.MESH)

    def part(i):
        return pl.ds(i * (rows // parts), rows // parts)

    near = send(own_ref, s1, near_sems, sibling)
    far = [send(own_ref.at[part(i)], s2.at[part(i)], far_sems.at[:, i], across) for i in range(parts)]
    fwd = [send(s2.at[part(i)], s3.at[part(i)], fwd_sems.at[:, i], sibling) for i in range(parts)]

    if not far_given:
        @pl.when(jnp.logical_not(chip1))
        def _():
            for cp in far:
                cp.start()

    @pl.when(odd == 0)
    def _():
        near.start()

    if far_given:
        @pl.when(chip1)
        def _():
            for cp in fwd:
                cp.start()

    gain = gs_ref[layer:layer + 1, :]
    x_s[pl.ds(0, rows), :] = rms(own_ref[...], gain)
    key = lax.broadcasted_iota(jnp.int32, (rows, rows), 0)
    query = lax.broadcasted_iota(jnp.int32, (rows, rows), 1)
    bias[0, pl.ds(0, rows), :] = jnp.where(key <= query, 0.0, NEG_BIG)
    bias[0, pl.ds(rows, rows), :] = jnp.full((rows, rows), jnp.where(odd == 1, 0.0, NEG_BIG), F32)
    bias[1] = jnp.zeros((2 * rows, rows), F32)
    attend_reset(scratch)

    @pl.when(odd == 1)
    def _():
        near.wait_recv()
        x_s[pl.ds(rows, rows), :] = rms(s1[...], gain)

    @pl.when(odd == 0)
    def _():
        x_s[pl.ds(rows, rows), :] = jnp.zeros((rows, width), BF16)

    def tile(t):
        return pl.ds(pl.multiple_of(t * 256, 256), 256)

    def head_cols(i):
        return pl.ds(pl.multiple_of(i * GW, GW), GW)

    def phase(half, _):
        at = pl.ds(pl.multiple_of(half * CH, CH), CH)

        @pl.when(half == 0)
        def _():
            w_copies[0].wait()
            w_copies[2].start()

        def project_step(r, _):
            rows_at = tile(2 * half + r)
            for first in range(0, parts, parts_half):
                @pl.when((half == 1) & (r == first // parts_half))
                def _(first=first):
                    some = range(first, first + parts_half)
                    if not far_given:
                        for i in some:
                            far[i].wait_recv()
                            fwd[i].start()
                    here = pl.ds(first * (rows // parts), rows // 2)
                    x_s[pl.ds(2 * rows + 2 * first * (rows // parts), rows // 2), :] = rms(s2[here, :], gain)
                    for i in some:
                        fwd[i].wait_recv()
                    x_s[pl.ds(2 * rows + 2 * first * (rows // parts) + rows // 2, rows // 2), :] = rms(s3[here, :], gain)

            k_s[rows_at, :] = dot(x_s[rows_at, :], w_s[0]).astype(BF16)

            @pl.when((half == 0) & (r == 0))
            def _():
                w_copies[1].wait()
                w_copies[3].start()

            vt_s[:, rows_at] = dot(x_s[rows_at, :], w_s[1]).astype(BF16).T
            return 0

        lax.fori_loop(0, 2, project_step, 0)

        @pl.when(half == 0)
        def _():
            w_copies[2].wait()
            w_copies[4].start()

            qs[...] = (dot(x_s[pl.ds(0, rows), :], w_s[2]).astype(BF16) * BF16(0.125)).T

        def scores(i, j):
            k = k_s[at, head_cols(i)]
            return (dot(k[:, h // 2 * 128:(h // 2 + 1) * 128], q) + bias[half] for h, q in enumerate(head_queries(qs[head_cols(i), :])))

        attend_all(width // GW, 1, scores, lambda i, j: vt_s[head_cols(i), at], lambda i: None, lambda i: None, scratch)
        return 0

    lax.fori_loop(0, jnp.where(chip1, 2, 1), phase, 0)

    def finish(i, _):
        attend_finish(i, at_s, scratch)
        return 0

    lax.fori_loop(0, width // GW, finish, 0)
    a_s[...] = at_s[...].T
    w_copies[3].wait()

    hid_ref[...] = (own_ref[...].astype(F32) + dot(a_s[...], w_s[3])).astype(BF16)
    a_s[...] = rms(hid_ref[...], gc_ref[layer:layer + 1, :])
    w_copies[4].wait()

    q_ref[...] = (dot(a_s[...], w_s[4]).astype(BF16) * BF16(0.125)).T

    @pl.when(odd == 0)
    def _():
        near.wait_send()

    @pl.when(chip1)
    def _():
        for cp in fwd:
            cp.wait_send()

    if not far_given:
        @pl.when(jnp.logical_not(chip1))
        def _():
            for cp in far:
                cp.wait_send()


def self_attention(layer, own, far, gs, gc, wq, wk, wv, wo, wcq):
    rows, width = own.shape
    far_given = far is not None
    parts = 2 if far_given else 4
    shape = jax.ShapeDtypeStruct((rows, width), BF16)
    flops = 2 * rows * width * width * 11 + 4 * rows * 4 * rows * width
    block = pltpu.VMEM((rows, width), BF16)
    return pl.pallas_call(
        functools.partial(self_kernel, layer, far_given),
        in_specs=[VMEM] * (4 if far_given else 3) + [ANY] * 5,
        out_specs=[VMEM, VMEM],
        out_shape=[shape, jax.ShapeDtypeStruct((width, rows), BF16)],
        scratch_shapes=[
            pltpu.VMEM((5, width, width), BF16),
            pltpu.VMEM((4 * rows, width), BF16),
            pltpu.VMEM((4 * rows, width), BF16),
            pltpu.VMEM((width, 4 * rows), BF16),
            pltpu.VMEM((width, rows), BF16),
            pltpu.VMEM((2, 2 * rows, rows), F32),
            pltpu.VMEM((width, rows), BF16),
            block,
            block,
            block,
            *([] if far_given else [block]),
            *attend_scratch(width // GW, rows),
            pltpu.SemaphoreType.DMA((5,)),
            pltpu.SemaphoreType.DMA((2,)),
            pltpu.SemaphoreType.DMA((2, parts)),
            pltpu.SemaphoreType.DMA((2, parts)),
        ],
        cost_estimate=pl.CostEstimate(flops=flops, bytes_accessed=10 * width * width, transcendentals=0),
        compiler_params=pltpu.CompilerParams(vmem_limit_bytes=VMEM_LIMIT, collective_id=layer, has_side_effects=True),
        name="self_attention",
    )(own, *([far] if far_given else []), gs, gc, wq, wk, wv, wo, wcq)


def cross_kernel(layer, planes, n_kv, lim_ref, q_ref, *refs):
    def take(n):
        nonlocal refs
        head, refs = refs[:n], refs[n:]
        return head

    ks, vts = take(n_kv), take(n_kv)
    hid_ref, gm_ref, wco, wg, wu, wd, out_ref = take(7)
    scratch = take(7)
    kbuf, vbuf, mask, list_s, kv_sems = take(5)
    at_s, a_s, act0, act1, acc_o, wo_s, wg_s, wu_s, wd_s, o_sem, w_sems = take(11)
    ring, ff = wg_s.shape[0], wg_s.shape[2]
    steps = wg.shape[2] // ff
    width, rows = q_ref.shape
    groups = width // GW

    def kv_copies(i, go):
        slot = lax.rem(i, 2)
        cols = pl.ds(pl.multiple_of(i * GW, GW), GW)
        at = 0
        for n in range(n_kv):
            there = pl.ds(at, ks[n].shape[1])
            go(pltpu.make_async_copy(ks[n].at[planes[n], :, cols], kbuf.at[slot, there, :], kv_sems.at[slot, 0, n]))
            go(pltpu.make_async_copy(vts[n].at[planes[n], cols, :], vbuf.at[slot, :, there], kv_sems.at[slot, 1, n]))
            at += ks[n].shape[1]

    def kv_start(i):
        kv_copies(i, lambda cp: cp.start())

    kv_start(0)
    kv_start(1)
    o_copy = pltpu.make_async_copy(wco.at[layer], wo_s, o_sem)

    def w_copies(j):
        cols = pl.ds(pl.multiple_of(j * ff, ff), ff)
        slot = lax.rem(j, ring)
        return (pltpu.make_async_copy(wg.at[layer, :, cols], wg_s.at[slot], w_sems.at[0, slot]),
                pltpu.make_async_copy(wu.at[layer, :, cols], wu_s.at[slot], w_sems.at[1, slot]),
                pltpu.make_async_copy(wd.at[layer, cols, :], wd_s.at[slot], w_sems.at[2, slot]))

    def w_start(j):
        for cp in w_copies(j):
            cp.start()

    attend_reset(scratch)

    n_chunks, last = jnp.int32(0), jnp.int32(0)
    list_s[0] = 0
    for c in range(lim_ref.shape[0]):
        lim = lim_ref[c]

        @pl.when(lim > 0)
        def _(c=c, at=n_chunks):
            list_s[at] = c

        n_chunks = n_chunks + (lim > 0).astype(jnp.int32)
        last = last + jnp.where(lim < CH, lim, 0)
    key = lax.broadcasted_iota(jnp.int32, (CH, 128), 0)
    lane = lax.broadcasted_iota(jnp.int32, (CH, 128), 1)
    mask[0] = jnp.zeros((CH, 128), BF16)
    mask[1] = jnp.where((key >= last) & (lane == 0), NEG_BIG, 0.0).astype(BF16)
    ones = (lax.broadcasted_iota(jnp.int32, (128, rows), 0) == 0).astype(F32).astype(BF16)

    def enter(i):
        kv_copies(i, lambda cp: cp.wait())

        @pl.when(i == 0)
        def _():
            o_copy.start()
            for j in range(ring - groups):
                w_start(j)

        w_start(ring - groups + i)

    def leave(i):
        @pl.when(i + 2 < groups)
        def _():
            kv_start(i + 2)

    def chunk(j):
        return pl.ds(pl.multiple_of(list_s[j] * CH, CH), CH)

    def scores(i, j):
        partial = (lim_ref[list_s[j]] < CH).astype(jnp.int32)
        k = kbuf[lax.rem(i, 2), chunk(j), :]
        ks = [jnp.concatenate([k[:, p * 128:(p + 1) * 128], mask[partial]], axis=1) for p in range(HEADS // 2)]
        queries = head_queries(q_ref[pl.ds(pl.multiple_of(i * GW, GW), GW), :], ones)
        return (dot(ks[h // 2], q) for h, q in enumerate(queries))

    def values(i, j):
        return vbuf[lax.rem(i, 2), :, chunk(j)]

    attend_all(groups, n_chunks, scores, values, enter, leave, scratch)

    def finish(i, _):
        attend_finish(i, at_s, scratch)
        return 0

    lax.fori_loop(0, groups, finish, 0)
    a_s[...] = at_s[...].T
    o_copy.wait()

    out_ref[...] = (hid_ref[...].astype(F32) + dot(a_s[...], wo_s[...])).astype(BF16)
    a_s[...] = rms(out_ref[...], gm_ref[layer:layer + 1, :])
    acc_o[...] = jnp.zeros_like(acc_o)

    def wait_gate_up(j):
        for cp in w_copies(j)[:2]:
            cp.wait()

    def gate_up(j, act_ref):
        x = a_s[...]
        gate = dot(x, wg_s[lax.rem(j, ring)])
        up = dot(x, wu_s[lax.rem(j, ring)])
        act_ref[...] = (gate / (1.0 + jnp.exp(-gate)) * up).astype(BF16)

    wait_gate_up(0)
    gate_up(0, act0)

    def mlp_step(u, _):
        for now, later, at in ((act0, act1, 0), (act1, act0, 1)):
            j = 2 * u + at
            w_copies(j)[2].wait()

            @pl.when(j + 1 < steps)
            def _(j=j):
                wait_gate_up(j + 1)

            acc_o[...] += dot(now[...], wd_s[lax.rem(j, ring)])
            gate_up(jnp.minimum(j + 1, steps - 1), later)

            @pl.when(j + ring < steps)
            def _(j=j):
                w_start(j + ring)
        return 0

    lax.fori_loop(0, steps // 2, mlp_step, 0)
    out_ref[...] = (out_ref[...].astype(F32) + acc_o[...]).astype(BF16)


def cross_mlp(layer, lims, q, kvs, hid, gm, wco, wg, wu, wd):
    width, rows = q.shape
    groups = width // GW
    planes = tuple(plane for _, _, plane in kvs)
    ks, vts = [k for k, _, _ in kvs], [v for _, v, _ in kvs]
    total = sum(k.shape[1] for k in ks)
    n = len(kvs)
    ff, ring = 512, 6
    return pl.pallas_call(
        functools.partial(cross_kernel, layer, planes, n),
        in_specs=[SMEM, VMEM] + [ANY] * (2 * n) + [VMEM] * 2 + [ANY] * 4,
        out_specs=VMEM,
        out_shape=jax.ShapeDtypeStruct((rows, width), BF16),
        scratch_shapes=attend_scratch(groups, rows) + [
            pltpu.VMEM((2, total, GW), BF16),
            pltpu.VMEM((2, GW, total), BF16),
            pltpu.VMEM((2, CH, 128), BF16),
            pltpu.SMEM((8,), jnp.int32),
            pltpu.SemaphoreType.DMA((2, 2, n)),
            pltpu.VMEM((width, rows), BF16),
            pltpu.VMEM((rows, width), BF16),
            pltpu.VMEM((rows, ff), BF16),
            pltpu.VMEM((rows, ff), BF16),
            pltpu.VMEM((rows, width), F32),
            pltpu.VMEM((width, width), BF16),
            pltpu.VMEM((ring, width, ff), BF16),
            pltpu.VMEM((ring, width, ff), BF16),
            pltpu.VMEM((ring, ff, width), BF16),
            pltpu.SemaphoreType.DMA,
            pltpu.SemaphoreType.DMA((3, ring)),
        ],
        cost_estimate=pl.CostEstimate(
            flops=4 * rows * 3072 * width + 2 * rows * width * (width + 3 * wg.shape[2]),
            bytes_accessed=2 * width * (width + 3 * wg.shape[2]), transcendentals=0),
        compiler_params=pltpu.CompilerParams(vmem_limit_bytes=VMEM_LIMIT),
        name="cross_mlp",
    )(lims, q, *ks, *vts, hid, gm, wco, wg, wu, wd)


NONE = 1 << 20
BASES = (
    (0, 512, 1024, 1536, 2048, NONE, NONE, 2560),
    (1024, 1536, 0, 512, NONE, 2048, 2560, NONE),
    (2048, NONE, 2560, NONE, 0, 1024, 512, 1536),
    (2560, NONE, 2048, NONE, 1024, 0, 1536, 512),
)


def solution(mesh):
    row_spec = P(('dp', 'sp'), None)

    def local_step(hidden, memory, mem_len, norm_self, norm_cross, norm_mlp, self_q, self_k, self_v, self_o, cross_q, cross_k, cross_v, cross_o, mlp_gate, mlp_up, mlp_down):
        layers, width = norm_self.shape
        w_so = self_o.reshape(layers, width, width)
        w_co = cross_o.reshape(layers, width, width)
        dev = lax.axis_index('sp')
        dev_arr = dev.astype(jnp.int32).reshape(1)
        bases = jnp.array(BASES, jnp.int32)[dev]
        lims = jnp.clip(mem_len[0] - bases, 0, CH)
        is3 = (dev_arr == 3).astype(jnp.int32)

        def swap(x):
            return lax.ppermute(x, 'sp', [(0, 1), (1, 0), (2, 3), (3, 2)])

        def program(hidden):
            far = lax.ppermute(hidden, 'sp', [(0, 2), (1, 3)])
            mem_a, mem_b = memory[:CH], memory[CH:]
            c2b = lax.ppermute(mem_b, 'sp', [(2, 3)])
            rem_a = lax.ppermute(mem_a, 'sp', [(0, 2), (1, 3), (2, 0)])
            rem_b = lax.ppermute(mem_b, 'sp', [(0, 2), (1, 3), (2, 1)])

            both = (0, layers)
            ka, va = kv_project(lims[0:2], is3, [memory, c2b], cross_k, cross_v, 2 * CH, both)
            kas, vas = swap(ka), swap(va)
            kb, vb = kv_project(lims[4:5], is3, [rem_a], cross_k, cross_v, CH, both)
            kbs, vbs = swap(kb), swap(vb)
            kvs = []
            for layer in range(layers):
                kc, vc = kv_project(lims[6:7], is3, [rem_b], cross_k, cross_v, CH, (layer, 1))
                kcs, vcs = swap(kc), swap(vc)
                kvs.append([(ka, va, layer), (kas, vas, layer), (kb, vb, layer), (kbs, vbs, layer), (kc, vc, 0), (kcs, vcs, 0)])

            for layer in range(layers):
                hidden, q = self_attention(layer, hidden, far, norm_self, norm_cross, self_q, self_k, self_v, w_so, cross_q)
                hidden = cross_mlp(layer, lims, q, kvs[layer], hidden, norm_mlp, w_co, mlp_gate, mlp_up, mlp_down)
                far = None
            return hidden

        return program(hidden)

    return jax.shard_map(local_step, mesh=mesh, in_specs=(row_spec, row_spec, P('dp')) + (P(),) * 14, out_specs=row_spec, check_vma=False)
```

```python
import functools

import jax
import jax.numpy as jnp
from jax import lax
from jax.experimental import pallas as pl
from jax.experimental.pallas import tpu as pltpu
from jax.sharding import PartitionSpec as P


EPS = 1e-6
NEG_BIG = -1e30
F32 = jnp.float32
BF16 = jnp.bfloat16
CH = 512
HEADS = 4
GW = HEADS * 64
ORDER = (("F", 0), ("F", 1), ("S", 0), ("S", 1), ("F", 2), ("F", 3), ("S", 2), ("S", 3))
VMEM_LIMIT = 62 * 1024 * 1024
ANY = pl.BlockSpec(memory_space=pltpu.HBM)
SMEM = pl.BlockSpec(memory_space=pltpu.SMEM)
VMEM = pl.BlockSpec(memory_space=pltpu.VMEM)


def rms(h, gain):
    h32 = h.astype(F32)
    inv = lax.rsqrt(jnp.mean(h32 * h32, axis=-1, keepdims=True) + EPS)
    return (h32 * inv * gain.astype(F32)).astype(BF16)


def dot(a, b):
    return jnp.dot(a, b, preferred_element_type=F32)


def kv_kernel(layers, n_src, lim_ref, pick_ref, *refs):
    srcs, (wk, wv, k_out, vt_out, mem, w_s, k_s, vt_s, sem, w_sems, o_sems) = refs[:n_src], refs[n_src:]
    rows = mem.shape[0]
    lo, n = layers

    def from_src(go):
        if n_src == 1:
            go(pltpu.make_async_copy(srcs[0], mem, sem))
        else:
            @pl.when(pick_ref[0] == 0)
            def _():
                go(pltpu.make_async_copy(srcs[0], mem, sem))

            @pl.when(pick_ref[0] != 0)
            def _():
                go(pltpu.make_async_copy(srcs[1], mem.at[pl.ds(0, CH)], sem))

    def w_copy(i, v):
        return pltpu.make_async_copy((wk, wv)[v].at[lo + i], w_s.at[2 * i + v], w_sems.at[2 * i + v])

    w_copy(0, 0).start()
    from_src(lambda cp: cp.start())
    from_src(lambda cp: cp.wait())
    w_copy(0, 1).start()

    def out_copy(i, v, c):
        at = pl.ds(pl.multiple_of(c * CH, CH), CH)
        if v == 0:
            return pltpu.make_async_copy(k_s.at[i, at, :], k_out.at[i, at, :], o_sems.at[i, v, c])
        return pltpu.make_async_copy(vt_s.at[i, :, at], vt_out.at[i, :, at], o_sems.at[i, v, c])

    def valid(c, go):
        @pl.when(lim_ref[c] > 0)
        def _():
            go()

    def layer_step(i, _):
        for v in range(2):
            w_copy(i, v).wait()

            @pl.when(i + 1 < n)
            def _(v=v):
                w_copy(i + 1, v).start()

            def chunk_step(c, _):
                def work():
                    def step(r, _):
                        at = pl.ds(pl.multiple_of(c * CH + r * 256, 256), 256)
                        out = dot(mem[at, :], w_s[2 * i + v]).astype(BF16)
                        if v == 0:
                            k_s[i, at, :] = out
                        else:
                            vt_s[i, :, at] = out.T
                        return 0

                    lax.fori_loop(0, CH // 256, step, 0)
                    out_copy(i, v, c).start()

                valid(c, work)
                return 0

            lax.fori_loop(0, rows // CH, chunk_step, 0)
        return 0

    lax.fori_loop(0, n, layer_step, 0)
    for i in range(n):
        for v in range(2):
            for c in range(rows // CH):
                valid(c, lambda i=i, v=v, c=c: out_copy(i, v, c).wait())


def kv_project(lims, pick, srcs, wk, wv, rows, layers):
    width, cols = wk.shape[1], wk.shape[2]
    n = layers[1]
    flops = n * 4 * rows * width * cols
    return pl.pallas_call(
        functools.partial(kv_kernel, layers, len(srcs)),
        in_specs=[SMEM, SMEM] + [ANY] * (len(srcs) + 2),
        out_specs=[ANY, ANY],
        out_shape=[jax.ShapeDtypeStruct((n, rows, cols), BF16), jax.ShapeDtypeStruct((n, cols, rows), BF16)],
        scratch_shapes=[
            pltpu.VMEM((rows, width), BF16),
            pltpu.VMEM((2 * n, width, cols), BF16),
            pltpu.VMEM((n, rows, cols), BF16),
            pltpu.VMEM((n, cols, rows), BF16),
            pltpu.SemaphoreType.DMA,
            pltpu.SemaphoreType.DMA((2 * n,)),
            pltpu.SemaphoreType.DMA((n, 2, rows // CH)),
        ],
        cost_estimate=pl.CostEstimate(flops=flops, bytes_accessed=n * 4 * width * cols, transcendentals=0),
        compiler_params=pltpu.CompilerParams(vmem_limit_bytes=VMEM_LIMIT),
        name="kv_project",
    )(lims, pick, *srcs, wk, wv)


def head_queries(qt, extra=None):
    row = lax.broadcasted_iota(jnp.int32, (128, qt.shape[1]), 0)
    out = []
    for h in range(HEADS):
        pair = qt[h // 2 * 128:(h // 2 + 1) * 128, :]
        q = jnp.where((row < 64) == (h % 2 == 0), pair, jnp.zeros_like(pair))
        out.append(q if extra is None else jnp.concatenate([q, extra], axis=0))
    return out


def attend_all(groups, n_chunks, scores, values, enter, leave, scratch):
    s_refs, mx_refs, (m_ref, l_ref, acc_ref) = scratch[:2], scratch[2:4], scratch[4:]
    total = groups * n_chunks

    def stage1(group, j, buf):
        for h, s in enumerate(scores(group, j)):
            first(h, s, buf)

    def first(h, s, buf):
        s_refs[buf][h] = s
        mx_refs[buf][h:h + 1, :] = jnp.max(s, axis=0, keepdims=True)

    def second(group, h, vt, buf):
        m_old = m_ref[group, h:h + 1, :]
        m_new = jnp.maximum(m_old, mx_refs[buf][h:h + 1, :])
        p = jnp.exp(s_refs[buf][h] - m_new)
        alpha = jnp.exp(m_old - m_new)
        m_ref[group, h:h + 1, :] = m_new
        l_ref[group, h:h + 1, :] = l_ref[group, h:h + 1, :] * alpha + jnp.sum(p, axis=0, keepdims=True)
        acc_ref[group, h] = acc_ref[group, h] * alpha + dot(vt[h * 64:(h + 1) * 64, :], p.astype(BF16))

    def advance(group, j):
        wrap = j + 1 == n_chunks
        return jnp.where(wrap, group + 1, group), jnp.where(wrap, 0, j + 1)

    enter(0)
    stage1(0, 0, 0)

    def item(group, j, buf):
        group_next, j_next = advance(group, j)

        @pl.when((j_next == 0) & (group_next < groups))
        def _():
            enter(group_next)

        made = scores(jnp.minimum(group_next, groups - 1), j_next)
        vt = values(group, j)
        for what, h in ORDER:
            if what == "F":
                first(h, next(made), 1 - buf)
            else:
                second(group, h, vt, buf)

        @pl.when(j_next == 0)
        def _():
            leave(group)

    def step(u, now):
        item(*now, 0)
        now = advance(*now)

        @pl.when(2 * u + 1 < total)
        def _():
            item(*now, 1)

        return advance(*now)

    lax.fori_loop(0, (total + 1) // 2, step, (jnp.int32(0), jnp.int32(0)))


def attend_reset(scratch):
    m_ref, l_ref, acc_ref = scratch[4:]
    m_ref[...] = jnp.full_like(m_ref, -jnp.inf)
    l_ref[...] = jnp.zeros_like(l_ref)
    acc_ref[...] = jnp.zeros_like(acc_ref)


def attend_finish(group, at_ref, scratch):
    l_ref, acc_ref = scratch[5:]
    for h in range(HEADS):
        rows = pl.ds(pl.multiple_of(group * HEADS * 64 + h * 64, 64), 64)
        at_ref[rows, :] = (acc_ref[group, h] / l_ref[group, h:h + 1, :]).astype(BF16)


def attend_scratch(groups, rows):
    return [
        pltpu.VMEM((HEADS, CH, rows), F32),
        pltpu.VMEM((HEADS, CH, rows), F32),
        pltpu.VMEM((HEADS, rows), F32),
        pltpu.VMEM((HEADS, rows), F32),
        pltpu.VMEM((groups, HEADS, rows), F32),
        pltpu.VMEM((groups, HEADS, rows), F32),
        pltpu.VMEM((groups, HEADS, 64, rows), F32),
    ]


def self_kernel(layer, far_given, *refs):
    own_ref, refs = refs[0], refs[1:]
    if far_given:
        s2, refs = refs[0], refs[1:]
    gs_ref, gc_ref, wq, wk, wv, wo, wcq, hid_ref, q_ref, w_s, x_s, k_s, vt_s, qs, bias, at_s, a_s, s1, s3 = refs[:19]
    refs = refs[19:]
    if not far_given:
        s2, refs = refs[0], refs[1:]
    scratch, (sems, near_sems, far_sems, fwd_sems) = refs[:7], refs[7:]
    rows, width = own_ref.shape
    parts = far_sems.shape[1]
    parts_half = parts // 2
    dev = lax.axis_index("sp")
    odd = lax.rem(dev, 2)
    chip1 = dev >= 2
    sibling = dev + 1 - 2 * odd
    across = lax.rem(dev + 2, 4)

    w_copies = [pltpu.make_async_copy(src.at[layer], w_s.at[n], sems.at[n]) for n, src in enumerate((wk, wv, wq, wo, wcq))]
    w_copies[0].start()
    w_copies[1].start()

    barrier = pltpu.get_barrier_semaphore()
    others = (sibling,) if far_given else (sibling, across)
    for other in others:
        pl.semaphore_signal(barrier, inc=1, device_id={"sp": other}, device_id_type=pl.DeviceIdType.MESH)
    pl.semaphore_wait(barrier, len(others))

    def send(src, dst, sem, other):
        return pltpu.make_async_remote_copy(src_ref=src, dst_ref=dst, send_sem=sem.at[0], recv_sem=sem.at[1],
                                            device_id={"sp": other}, device_id_type=pl.DeviceIdType.MESH)

    def part(i):
        return pl.ds(i * (rows // parts), rows // parts)

    near = send(own_ref, s1, near_sems, sibling)
    far = [send(own_ref.at[part(i)], s2.at[part(i)], far_sems.at[:, i], across) for i in range(parts)]
    fwd = [send(s2.at[part(i)], s3.at[part(i)], fwd_sems.at[:, i], sibling) for i in range(parts)]

    if not far_given:
        @pl.when(jnp.logical_not(chip1))
        def _():
            for cp in far:
                cp.start()

    @pl.when(odd == 0)
    def _():
        near.start()

    if far_given:
        @pl.when(chip1)
        def _():
            for cp in fwd:
                cp.start()

    gain = gs_ref[layer:layer + 1, :]
    x_s[pl.ds(0, rows), :] = rms(own_ref[...], gain)
    key = lax.broadcasted_iota(jnp.int32, (rows, rows), 0)
    query = lax.broadcasted_iota(jnp.int32, (rows, rows), 1)
    bias[0, pl.ds(0, rows), :] = jnp.where(key <= query, 0.0, NEG_BIG)
    bias[0, pl.ds(rows, rows), :] = jnp.full((rows, rows), jnp.where(odd == 1, 0.0, NEG_BIG), F32)
    bias[1] = jnp.zeros((2 * rows, rows), F32)
    attend_reset(scratch)

    @pl.when(odd == 1)
    def _():
        near.wait_recv()
        x_s[pl.ds(rows, rows), :] = rms(s1[...], gain)

    @pl.when(odd == 0)
    def _():
        x_s[pl.ds(rows, rows), :] = jnp.zeros((rows, width), BF16)

    def tile(t):
        return pl.ds(pl.multiple_of(t * 256, 256), 256)

    def head_cols(i):
        return pl.ds(pl.multiple_of(i * GW, GW), GW)

    def phase(half, _):
        at = pl.ds(pl.multiple_of(half * CH, CH), CH)

        @pl.when(half == 0)
        def _():
            w_copies[0].wait()
            w_copies[2].start()

        def project_step(r, _):
            rows_at = tile(2 * half + r)
            for first in range(0, parts, parts_half):
                @pl.when((half == 1) & (r == first // parts_half))
                def _(first=first):
                    some = range(first, first + parts_half)
                    if not far_given:
                        for i in some:
                            far[i].wait_recv()
                            fwd[i].start()
                    here = pl.ds(first * (rows // parts), rows // 2)
                    x_s[pl.ds(2 * rows + 2 * first * (rows // parts), rows // 2), :] = rms(s2[here, :], gain)
                    for i in some:
                        fwd[i].wait_recv()
                    x_s[pl.ds(2 * rows + 2 * first * (rows // parts) + rows // 2, rows // 2), :] = rms(s3[here, :], gain)

            k_s[rows_at, :] = dot(x_s[rows_at, :], w_s[0]).astype(BF16)

            @pl.when((half == 0) & (r == 0))
            def _():
                w_copies[1].wait()
                w_copies[3].start()

            vt_s[:, rows_at] = dot(x_s[rows_at, :], w_s[1]).astype(BF16).T
            return 0

        lax.fori_loop(0, 2, project_step, 0)

        @pl.when(half == 0)
        def _():
            w_copies[2].wait()
            w_copies[4].start()

            qs[...] = (dot(x_s[pl.ds(0, rows), :], w_s[2]).astype(BF16) * BF16(0.125)).T

        def scores(i, j):
            k = k_s[at, head_cols(i)]
            return (dot(k[:, h // 2 * 128:(h // 2 + 1) * 128], q) + bias[half] for h, q in enumerate(head_queries(qs[head_cols(i), :])))

        attend_all(width // GW, 1, scores, lambda i, j: vt_s[head_cols(i), at], lambda i: None, lambda i: None, scratch)
        return 0

    lax.fori_loop(0, jnp.where(chip1, 2, 1), phase, 0)

    def finish(i, _):
        attend_finish(i, at_s, scratch)
        return 0

    lax.fori_loop(0, width // GW, finish, 0)
    a_s[...] = at_s[...].T
    w_copies[3].wait()

    hid_ref[...] = (own_ref[...].astype(F32) + dot(a_s[...], w_s[3])).astype(BF16)
    a_s[...] = rms(hid_ref[...], gc_ref[layer:layer + 1, :])
    w_copies[4].wait()

    q_ref[...] = (dot(a_s[...], w_s[4]).astype(BF16) * BF16(0.125)).T

    @pl.when(odd == 0)
    def _():
        near.wait_send()

    @pl.when(chip1)
    def _():
        for cp in fwd:
            cp.wait_send()

    if not far_given:
        @pl.when(jnp.logical_not(chip1))
        def _():
            for cp in far:
                cp.wait_send()


def self_attention(layer, own, far, gs, gc, wq, wk, wv, wo, wcq):
    rows, width = own.shape
    far_given = far is not None
    parts = 2 if far_given else 4
    shape = jax.ShapeDtypeStruct((rows, width), BF16)
    flops = 2 * rows * width * width * 11 + 4 * rows * 4 * rows * width
    block = pltpu.VMEM((rows, width), BF16)
    return pl.pallas_call(
        functools.partial(self_kernel, layer, far_given),
        in_specs=[VMEM] * (4 if far_given else 3) + [ANY] * 5,
        out_specs=[VMEM, VMEM],
        out_shape=[shape, jax.ShapeDtypeStruct((width, rows), BF16)],
        scratch_shapes=[
            pltpu.VMEM((5, width, width), BF16),
            pltpu.VMEM((4 * rows, width), BF16),
            pltpu.VMEM((4 * rows, width), BF16),
            pltpu.VMEM((width, 4 * rows), BF16),
            pltpu.VMEM((width, rows), BF16),
            pltpu.VMEM((2, 2 * rows, rows), F32),
            pltpu.VMEM((width, rows), BF16),
            block,
            block,
            block,
            *([] if far_given else [block]),
            *attend_scratch(width // GW, rows),
            pltpu.SemaphoreType.DMA((5,)),
            pltpu.SemaphoreType.DMA((2,)),
            pltpu.SemaphoreType.DMA((2, parts)),
            pltpu.SemaphoreType.DMA((2, parts)),
        ],
        cost_estimate=pl.CostEstimate(flops=flops, bytes_accessed=10 * width * width, transcendentals=0),
        compiler_params=pltpu.CompilerParams(vmem_limit_bytes=VMEM_LIMIT, collective_id=layer, has_side_effects=True),
        name="self_attention",
    )(own, *([far] if far_given else []), gs, gc, wq, wk, wv, wo, wcq)


def cross_kernel(layer, planes, n_kv, lim_ref, q_ref, *refs):
    def take(n):
        nonlocal refs
        head, refs = refs[:n], refs[n:]
        return head

    ks, vts = take(n_kv), take(n_kv)
    hid_ref, gm_ref, wco, wg, wu, wd, out_ref = take(7)
    scratch = take(7)
    kbuf, vbuf, mask, list_s, kv_sems = take(5)
    at_s, a_s, act0, act1, acc_o, wo_s, wg_s, wu_s, wd_s, o_sem, w_sems = take(11)
    ring, ff = wg_s.shape[0], wg_s.shape[2]
    steps = wg.shape[2] // ff
    width, rows = q_ref.shape
    groups = width // GW

    def kv_copies(i, go):
        slot = lax.rem(i, 2)
        cols = pl.ds(pl.multiple_of(i * GW, GW), GW)
        at = 0
        for n in range(n_kv):
            there = pl.ds(at, ks[n].shape[1])
            go(pltpu.make_async_copy(ks[n].at[planes[n], :, cols], kbuf.at[slot, there, :], kv_sems.at[slot, 0, n]))
            go(pltpu.make_async_copy(vts[n].at[planes[n], cols, :], vbuf.at[slot, :, there], kv_sems.at[slot, 1, n]))
            at += ks[n].shape[1]

    def kv_start(i):
        kv_copies(i, lambda cp: cp.start())

    kv_start(0)
    kv_start(1)
    o_copy = pltpu.make_async_copy(wco.at[layer], wo_s, o_sem)

    def w_copies(j):
        cols = pl.ds(pl.multiple_of(j * ff, ff), ff)
        slot = lax.rem(j, ring)
        return (pltpu.make_async_copy(wg.at[layer, :, cols], wg_s.at[slot], w_sems.at[0, slot]),
                pltpu.make_async_copy(wu.at[layer, :, cols], wu_s.at[slot], w_sems.at[1, slot]),
                pltpu.make_async_copy(wd.at[layer, cols, :], wd_s.at[slot], w_sems.at[2, slot]))

    def w_start(j):
        for cp in w_copies(j):
            cp.start()

    attend_reset(scratch)

    n_chunks, last = jnp.int32(0), jnp.int32(0)
    list_s[0] = 0
    for c in range(lim_ref.shape[0]):
        lim = lim_ref[c]

        @pl.when(lim > 0)
        def _(c=c, at=n_chunks):
            list_s[at] = c

        n_chunks = n_chunks + (lim > 0).astype(jnp.int32)
        last = last + jnp.where(lim < CH, lim, 0)
    key = lax.broadcasted_iota(jnp.int32, (CH, 128), 0)
    lane = lax.broadcasted_iota(jnp.int32, (CH, 128), 1)
    mask[0] = jnp.zeros((CH, 128), BF16)
    mask[1] = jnp.where((key >= last) & (lane == 0), NEG_BIG, 0.0).astype(BF16)
    ones = (lax.broadcasted_iota(jnp.int32, (128, rows), 0) == 0).astype(F32).astype(BF16)

    def enter(i):
        kv_copies(i, lambda cp: cp.wait())

        @pl.when(i == 0)
        def _():
            o_copy.start()
            for j in range(ring - groups):
                w_start(j)

        w_start(ring - groups + i)

    def leave(i):
        @pl.when(i + 2 < groups)
        def _():
            kv_start(i + 2)

    def chunk(j):
        return pl.ds(pl.multiple_of(list_s[j] * CH, CH), CH)

    def scores(i, j):
        partial = (lim_ref[list_s[j]] < CH).astype(jnp.int32)
        k = kbuf[lax.rem(i, 2), chunk(j), :]
        ks = [jnp.concatenate([k[:, p * 128:(p + 1) * 128], mask[partial]], axis=1) for p in range(HEADS // 2)]
        queries = head_queries(q_ref[pl.ds(pl.multiple_of(i * GW, GW), GW), :], ones)
        return (dot(ks[h // 2], q) for h, q in enumerate(queries))

    def values(i, j):
        return vbuf[lax.rem(i, 2), :, chunk(j)]

    attend_all(groups, n_chunks, scores, values, enter, leave, scratch)

    def finish(i, _):
        attend_finish(i, at_s, scratch)
        return 0

    lax.fori_loop(0, groups, finish, 0)
    a_s[...] = at_s[...].T
    o_copy.wait()

    out_ref[...] = (hid_ref[...].astype(F32) + dot(a_s[...], wo_s[...])).astype(BF16)
    a_s[...] = rms(out_ref[...], gm_ref[layer:layer + 1, :])
    acc_o[...] = jnp.zeros_like(acc_o)

    def wait_gate_up(j):
        for cp in w_copies(j)[:2]:
            cp.wait()

    def gate_up(j, act_ref):
        x = a_s[...]
        gate = dot(x, wg_s[lax.rem(j, ring)])
        up = dot(x, wu_s[lax.rem(j, ring)])
        act_ref[...] = (gate / (1.0 + jnp.exp(-gate)) * up).astype(BF16)

    wait_gate_up(0)
    gate_up(0, act0)

    def mlp_step(u, _):
        first = 2 * u
        w_copies(first)[2].wait()
        wait_gate_up(first + 1)
        w_copies(first + 1)[2].wait()

        @pl.when(first + 2 < steps)
        def _():
            wait_gate_up(first + 2)

        acc_o[...] += dot(act0[...], wd_s[lax.rem(first, ring)])
        gate_up(first + 1, act1)
        acc_o[...] += dot(act1[...], wd_s[lax.rem(first + 1, ring)])
        gate_up(jnp.minimum(first + 2, steps - 1), act0)

        for j in (first, first + 1):
            @pl.when(j + ring < steps)
            def _(j=j):
                w_start(j + ring)
        return 0

    lax.fori_loop(0, steps // 2, mlp_step, 0)
    out_ref[...] = (out_ref[...].astype(F32) + acc_o[...]).astype(BF16)


def cross_mlp(layer, lims, q, kvs, hid, gm, wco, wg, wu, wd):
    width, rows = q.shape
    groups = width // GW
    planes = tuple(plane for _, _, plane in kvs)
    ks, vts = [k for k, _, _ in kvs], [v for _, v, _ in kvs]
    total = sum(k.shape[1] for k in ks)
    n = len(kvs)
    ff, ring = 512, 6
    return pl.pallas_call(
        functools.partial(cross_kernel, layer, planes, n),
        in_specs=[SMEM, VMEM] + [ANY] * (2 * n) + [VMEM] * 2 + [ANY] * 4,
        out_specs=VMEM,
        out_shape=jax.ShapeDtypeStruct((rows, width), BF16),
        scratch_shapes=attend_scratch(groups, rows) + [
            pltpu.VMEM((2, total, GW), BF16),
            pltpu.VMEM((2, GW, total), BF16),
            pltpu.VMEM((2, CH, 128), BF16),
            pltpu.SMEM((8,), jnp.int32),
            pltpu.SemaphoreType.DMA((2, 2, n)),
            pltpu.VMEM((width, rows), BF16),
            pltpu.VMEM((rows, width), BF16),
            pltpu.VMEM((rows, ff), BF16),
            pltpu.VMEM((rows, ff), BF16),
            pltpu.VMEM((rows, width), F32),
            pltpu.VMEM((width, width), BF16),
            pltpu.VMEM((ring, width, ff), BF16),
            pltpu.VMEM((ring, width, ff), BF16),
            pltpu.VMEM((ring, ff, width), BF16),
            pltpu.SemaphoreType.DMA,
            pltpu.SemaphoreType.DMA((3, ring)),
        ],
        cost_estimate=pl.CostEstimate(
            flops=4 * rows * 3072 * width + 2 * rows * width * (width + 3 * wg.shape[2]),
            bytes_accessed=2 * width * (width + 3 * wg.shape[2]), transcendentals=0),
        compiler_params=pltpu.CompilerParams(vmem_limit_bytes=VMEM_LIMIT),
        name="cross_mlp",
    )(lims, q, *ks, *vts, hid, gm, wco, wg, wu, wd)


NONE = 1 << 20
BASES = (
    (0, 512, 1024, 1536, 2048, NONE, NONE, 2560),
    (1024, 1536, 0, 512, NONE, 2048, 2560, NONE),
    (2048, NONE, 2560, NONE, 0, 1024, 512, 1536),
    (2560, NONE, 2048, NONE, 1024, 0, 1536, 512),
)


def solution(mesh):
    row_spec = P(('dp', 'sp'), None)

    def local_step(hidden, memory, mem_len, norm_self, norm_cross, norm_mlp, self_q, self_k, self_v, self_o, cross_q, cross_k, cross_v, cross_o, mlp_gate, mlp_up, mlp_down):
        layers, width = norm_self.shape
        w_so = self_o.reshape(layers, width, width)
        w_co = cross_o.reshape(layers, width, width)
        dev = lax.axis_index('sp')
        dev_arr = dev.astype(jnp.int32).reshape(1)
        bases = jnp.array(BASES, jnp.int32)[dev]
        lims = jnp.clip(mem_len[0] - bases, 0, CH)
        is3 = (dev_arr == 3).astype(jnp.int32)

        def swap(x):
            return lax.ppermute(x, 'sp', [(0, 1), (1, 0), (2, 3), (3, 2)])

        def program(hidden):
            far = lax.ppermute(hidden, 'sp', [(0, 2), (1, 3)])
            mem_a, mem_b = memory[:CH], memory[CH:]
            c2b = lax.ppermute(mem_b, 'sp', [(2, 3)])
            rem_a = lax.ppermute(mem_a, 'sp', [(0, 2), (1, 3), (2, 0)])
            rem_b = lax.ppermute(mem_b, 'sp', [(0, 2), (1, 3), (2, 1)])

            both = (0, layers)
            ka, va = kv_project(lims[0:2], is3, [memory, c2b], cross_k, cross_v, 2 * CH, both)
            kas, vas = swap(ka), swap(va)
            kb, vb = kv_project(lims[4:5], is3, [rem_a], cross_k, cross_v, CH, both)
            kbs, vbs = swap(kb), swap(vb)
            kvs = []
            for layer in range(layers):
                kc, vc = kv_project(lims[6:7], is3, [rem_b], cross_k, cross_v, CH, (layer, 1))
                kcs, vcs = swap(kc), swap(vc)
                kvs.append([(ka, va, layer), (kas, vas, layer), (kb, vb, layer), (kbs, vbs, layer), (kc, vc, 0), (kcs, vcs, 0)])

            for layer in range(layers):
                hidden, q = self_attention(layer, hidden, far, norm_self, norm_cross, self_q, self_k, self_v, w_so, cross_q)
                hidden = cross_mlp(layer, lims, q, kvs[layer], hidden, norm_mlp, w_co, mlp_gate, mlp_up, mlp_down)
                far = None
            return hidden

        return program(hidden)

    return jax.shard_map(local_step, mesh=mesh, in_specs=(row_spec, row_spec, P('dp')) + (P(),) * 14, out_specs=row_spec, check_vma=False)
```

```python
import functools

import jax
import jax.numpy as jnp
from jax import lax
from jax.experimental import pallas as pl
from jax.experimental.pallas import tpu as pltpu
from jax.sharding import PartitionSpec as P


EPS = 1e-6
NEG_BIG = -1e30
F32 = jnp.float32
BF16 = jnp.bfloat16
CH = 512
TILE = 256
HEADS = 4
GW = HEADS * 64
VMEM_LIMIT = 62 * 1024 * 1024
ANY = pl.BlockSpec(memory_space=pltpu.HBM)
SMEM = pl.BlockSpec(memory_space=pltpu.SMEM)
VMEM = pl.BlockSpec(memory_space=pltpu.VMEM)


def rms(h, gain):
    h32 = h.astype(F32)
    inv = lax.rsqrt(jnp.mean(h32 * h32, axis=-1, keepdims=True) + EPS)
    return (h32 * inv * gain.astype(F32)).astype(BF16)


def dot(a, b):
    return jnp.dot(a, b, preferred_element_type=F32)


def kv_kernel(layers, n_src, lim_ref, pick_ref, *refs):
    srcs, (wk, wv, k_out, vt_out, mem, w_s, k_s, vt_s, sem, w_sems, o_sems) = refs[:n_src], refs[n_src:]
    rows = mem.shape[0]
    lo, n = layers

    def from_src(go):
        if n_src == 1:
            go(pltpu.make_async_copy(srcs[0], mem, sem))
        else:
            @pl.when(pick_ref[0] == 0)
            def _():
                go(pltpu.make_async_copy(srcs[0], mem, sem))

            @pl.when(pick_ref[0] != 0)
            def _():
                go(pltpu.make_async_copy(srcs[1], mem.at[pl.ds(0, srcs[1].shape[0])], sem))

    def w_copy(i, v):
        return pltpu.make_async_copy((wk, wv)[v].at[lo + i], w_s.at[2 * i + v], w_sems.at[2 * i + v])

    w_copy(0, 0).start()
    from_src(lambda cp: cp.start())
    from_src(lambda cp: cp.wait())
    w_copy(0, 1).start()

    def out_copy(i, v, c):
        at = pl.ds(pl.multiple_of(c * TILE, TILE), TILE)
        if v == 0:
            return pltpu.make_async_copy(k_s.at[i, at, :], k_out.at[i, at, :], o_sems.at[i, v, c])
        return pltpu.make_async_copy(vt_s.at[i, :, at], vt_out.at[i, :, at], o_sems.at[i, v, c])

    def valid(c, go):
        @pl.when(lim_ref[c * TILE // CH] > 0)
        def _():
            go()

    def layer_step(i, _):
        for v in range(2):
            w_copy(i, v).wait()

            @pl.when(i + 1 < n)
            def _(v=v):
                w_copy(i + 1, v).start()

            def tile_step(c, _):
                def work():
                    at = pl.ds(pl.multiple_of(c * TILE, TILE), TILE)
                    out = dot(mem[at, :], w_s[2 * i + v]).astype(BF16)
                    if v == 0:
                        k_s[i, at, :] = out
                    else:
                        vt_s[i, :, at] = out.T
                    out_copy(i, v, c).start()

                valid(c, work)
                return 0

            lax.fori_loop(0, rows // TILE, tile_step, 0)
        return 0

    lax.fori_loop(0, n, layer_step, 0)
    for i in range(n):
        for v in range(2):
            for c in range(rows // TILE):
                valid(c, lambda i=i, v=v, c=c: out_copy(i, v, c).wait())


def kv_project(lims, pick, srcs, wk, wv, rows, layers):
    width, cols = wk.shape[1], wk.shape[2]
    n = layers[1]
    flops = n * 4 * rows * width * cols
    return pl.pallas_call(
        functools.partial(kv_kernel, layers, len(srcs)),
        in_specs=[SMEM, SMEM] + [ANY] * (len(srcs) + 2),
        out_specs=[ANY, ANY],
        out_shape=[jax.ShapeDtypeStruct((n, rows, cols), BF16), jax.ShapeDtypeStruct((n, cols, rows), BF16)],
        scratch_shapes=[
            pltpu.VMEM((rows, width), BF16),
            pltpu.VMEM((2 * n, width, cols), BF16),
            pltpu.VMEM((n, rows, cols), BF16),
            pltpu.VMEM((n, cols, rows), BF16),
            pltpu.SemaphoreType.DMA,
            pltpu.SemaphoreType.DMA((2 * n,)),
            pltpu.SemaphoreType.DMA((n, 2, rows // TILE)),
        ],
        cost_estimate=pl.CostEstimate(flops=flops, bytes_accessed=n * 4 * width * cols, transcendentals=0),
        compiler_params=pltpu.CompilerParams(vmem_limit_bytes=VMEM_LIMIT),
        name="kv_project",
    )(lims, pick, *srcs, wk, wv)


def head_queries(qt, extra=None):
    row = lax.broadcasted_iota(jnp.int32, (128, qt.shape[1]), 0)
    out = []
    for h in range(HEADS):
        pair = qt[h // 2 * 128:(h // 2 + 1) * 128, :]
        q = jnp.where((row < 64) == (h % 2 == 0), pair, jnp.zeros_like(pair))
        out.append(q if extra is None else jnp.concatenate([q, extra], axis=0))
    return out


def attend_all(groups, n_chunks, scores, values, enter, leave, scratch):
    s_refs, mx_refs, (m_ref, l_ref, acc_ref) = scratch[:2], scratch[2:4], scratch[4:]
    total = groups * n_chunks

    def stage1(group, j, buf):
        for h, s in enumerate(scores(group, j)):
            first(h, s, buf)

    def first(h, s, buf):
        s_refs[buf][h] = s
        mx_refs[buf][h:h + 1, :] = jnp.max(s, axis=0, keepdims=True)

    def second(group, h, vt, buf):
        m_old = m_ref[group, h:h + 1, :]
        m_new = jnp.maximum(m_old, mx_refs[buf][h:h + 1, :])
        p = jnp.exp(s_refs[buf][h] - m_new)
        alpha = jnp.exp(m_old - m_new)
        m_ref[group, h:h + 1, :] = m_new
        l_ref[group, h:h + 1, :] = l_ref[group, h:h + 1, :] * alpha + jnp.sum(p, axis=0, keepdims=True)
        acc_ref[group, h] = acc_ref[group, h] * alpha + dot(vt[h * 64:(h + 1) * 64, :], p.astype(BF16))

    def advance(group, j):
        wrap = j + 1 == n_chunks
        return jnp.where(wrap, group + 1, group), jnp.where(wrap, 0, j + 1)

    enter(0)
    stage1(0, 0, 0)

    def item(group, j, buf):
        group_next, j_next = advance(group, j)

        @pl.when((j_next == 0) & (group_next < groups))
        def _():
            enter(group_next)

        made = scores(jnp.minimum(group_next, groups - 1), j_next)
        vt = values(group, j)
        for h in range(HEADS):
            first(h, next(made), 1 - buf)
            second(group, h, vt, buf)

        @pl.when(j_next == 0)
        def _():
            leave(group)

    def step(u, now):
        item(*now, 0)
        now = advance(*now)

        @pl.when(2 * u + 1 < total)
        def _():
            item(*now, 1)

        return advance(*now)

    lax.fori_loop(0, (total + 1) // 2, step, (jnp.int32(0), jnp.int32(0)))


def attend_reset(scratch):
    m_ref, l_ref, acc_ref = scratch[4:]
    m_ref[...] = jnp.full_like(m_ref, -jnp.inf)
    l_ref[...] = jnp.zeros_like(l_ref)
    acc_ref[...] = jnp.zeros_like(acc_ref)


def attend_finish(group, at_ref, scratch):
    l_ref, acc_ref = scratch[5:]
    for h in range(HEADS):
        rows = pl.ds(pl.multiple_of(group * HEADS * 64 + h * 64, 64), 64)
        at_ref[rows, :] = (acc_ref[group, h] / l_ref[group, h:h + 1, :]).astype(BF16)


def attend_scratch(groups, rows):
    return [
        pltpu.VMEM((HEADS, CH, rows), F32),
        pltpu.VMEM((HEADS, CH, rows), F32),
        pltpu.VMEM((HEADS, rows), F32),
        pltpu.VMEM((HEADS, rows), F32),
        pltpu.VMEM((groups, HEADS, rows), F32),
        pltpu.VMEM((groups, HEADS, rows), F32),
        pltpu.VMEM((groups, HEADS, 64, rows), F32),
    ]


def self_kernel(layer, far_given, *refs):
    own_ref, refs = refs[0], refs[1:]
    if far_given:
        s2, refs = refs[0], refs[1:]
    gs_ref, gc_ref, wq, wk, wv, wo, wcq, hid_ref, q_ref, w_s, x_s, k_s, vt_s, qs, bias, at_s, a_s, s1, s3 = refs[:19]
    refs = refs[19:]
    if not far_given:
        s2, refs = refs[0], refs[1:]
    scratch, (sems, near_sems, far_sems, fwd_sems) = refs[:7], refs[7:]
    rows, width = own_ref.shape
    parts = far_sems.shape[1]
    parts_half = parts // 2
    dev = lax.axis_index("sp")
    odd = lax.rem(dev, 2)
    chip1 = dev >= 2
    sibling = dev + 1 - 2 * odd
    across = lax.rem(dev + 2, 4)

    w_copies = [pltpu.make_async_copy(src.at[layer], w_s.at[n], sems.at[n]) for n, src in enumerate((wk, wv, wq, wo, wcq))]
    w_copies[0].start()
    w_copies[1].start()

    barrier = pltpu.get_barrier_semaphore()
    others = (sibling,) if far_given else (sibling, across)
    for other in others:
        pl.semaphore_signal(barrier, inc=1, device_id={"sp": other}, device_id_type=pl.DeviceIdType.MESH)
    pl.semaphore_wait(barrier, len(others))

    def send(src, dst, sem, other):
        return pltpu.make_async_remote_copy(src_ref=src, dst_ref=dst, send_sem=sem.at[0], recv_sem=sem.at[1],
                                            device_id={"sp": other}, device_id_type=pl.DeviceIdType.MESH)

    def part(i):
        return pl.ds(i * (rows // parts), rows // parts)

    near = send(own_ref, s1, near_sems, sibling)
    far = [send(own_ref.at[part(i)], s2.at[part(i)], far_sems.at[:, i], across) for i in range(parts)]
    fwd = [send(s2.at[part(i)], s3.at[part(i)], fwd_sems.at[:, i], sibling) for i in range(parts)]

    if not far_given:
        @pl.when(jnp.logical_not(chip1))
        def _():
            for cp in far:
                cp.start()

    @pl.when(odd == 0)
    def _():
        near.start()

    if far_given:
        @pl.when(chip1)
        def _():
            for cp in fwd:
                cp.start()

    gain = gs_ref[layer:layer + 1, :]
    x_s[pl.ds(0, rows), :] = rms(own_ref[...], gain)
    key = lax.broadcasted_iota(jnp.int32, (rows, rows), 0)
    query = lax.broadcasted_iota(jnp.int32, (rows, rows), 1)
    bias[0, pl.ds(0, rows), :] = jnp.where(key <= query, 0.0, NEG_BIG)
    bias[0, pl.ds(rows, rows), :] = jnp.full((rows, rows), jnp.where(odd == 1, 0.0, NEG_BIG), F32)
    bias[1] = jnp.zeros((2 * rows, rows), F32)
    attend_reset(scratch)

    @pl.when(odd == 1)
    def _():
        near.wait_recv()
        x_s[pl.ds(rows, rows), :] = rms(s1[...], gain)

    @pl.when(odd == 0)
    def _():
        x_s[pl.ds(rows, rows), :] = jnp.zeros((rows, width), BF16)

    def tile(t):
        return pl.ds(pl.multiple_of(t * 256, 256), 256)

    def head_cols(i):
        return pl.ds(pl.multiple_of(i * GW, GW), GW)

    def phase(half, _):
        at = pl.ds(pl.multiple_of(half * CH, CH), CH)

        @pl.when(half == 0)
        def _():
            w_copies[0].wait()
            w_copies[2].start()

        def project_step(r, _):
            rows_at = tile(2 * half + r)
            for first in range(0, parts, parts_half):
                @pl.when((half == 1) & (r == first // parts_half))
                def _(first=first):
                    some = range(first, first + parts_half)
                    if not far_given:
                        for i in some:
                            far[i].wait_recv()
                            fwd[i].start()
                    here = pl.ds(first * (rows // parts), rows // 2)
                    x_s[pl.ds(2 * rows + 2 * first * (rows // parts), rows // 2), :] = rms(s2[here, :], gain)
                    for i in some:
                        fwd[i].wait_recv()
                    x_s[pl.ds(2 * rows + 2 * first * (rows // parts) + rows // 2, rows // 2), :] = rms(s3[here, :], gain)

            k_s[rows_at, :] = dot(x_s[rows_at, :], w_s[0]).astype(BF16)

            @pl.when((half == 0) & (r == 0))
            def _():
                w_copies[1].wait()
                w_copies[3].start()

            vt_s[:, rows_at] = dot(x_s[rows_at, :], w_s[1]).astype(BF16).T
            return 0

        lax.fori_loop(0, 2, project_step, 0)

        @pl.when(half == 0)
        def _():
            w_copies[2].wait()
            w_copies[4].start()

            qs[...] = (dot(x_s[pl.ds(0, rows), :], w_s[2]).astype(BF16) * BF16(0.125)).T

        def scores(i, j):
            k = k_s[at, head_cols(i)]
            return (dot(k[:, h // 2 * 128:(h // 2 + 1) * 128], q) + bias[half] for h, q in enumerate(head_queries(qs[head_cols(i), :])))

        attend_all(width // GW, 1, scores, lambda i, j: vt_s[head_cols(i), at], lambda i: None, lambda i: None, scratch)
        return 0

    lax.fori_loop(0, jnp.where(chip1, 2, 1), phase, 0)

    def finish(i, _):
        attend_finish(i, at_s, scratch)
        return 0

    lax.fori_loop(0, width // GW, finish, 0)
    a_s[...] = at_s[...].T
    w_copies[3].wait()

    hid_ref[...] = (own_ref[...].astype(F32) + dot(a_s[...], w_s[3])).astype(BF16)
    a_s[...] = rms(hid_ref[...], gc_ref[layer:layer + 1, :])
    w_copies[4].wait()

    q_ref[...] = (dot(a_s[...], w_s[4]).astype(BF16) * BF16(0.125)).T

    @pl.when(odd == 0)
    def _():
        near.wait_send()

    @pl.when(chip1)
    def _():
        for cp in fwd:
            cp.wait_send()

    if not far_given:
        @pl.when(jnp.logical_not(chip1))
        def _():
            for cp in far:
                cp.wait_send()


def self_attention(layer, own, far, gs, gc, wq, wk, wv, wo, wcq):
    rows, width = own.shape
    far_given = far is not None
    parts = 2 if far_given else 4
    shape = jax.ShapeDtypeStruct((rows, width), BF16)
    flops = 2 * rows * width * width * 11 + 4 * rows * 4 * rows * width
    block = pltpu.VMEM((rows, width), BF16)
    return pl.pallas_call(
        functools.partial(self_kernel, layer, far_given),
        in_specs=[VMEM] * (4 if far_given else 3) + [ANY] * 5,
        out_specs=[VMEM, VMEM],
        out_shape=[shape, jax.ShapeDtypeStruct((width, rows), BF16)],
        scratch_shapes=[
            pltpu.VMEM((5, width, width), BF16),
            pltpu.VMEM((4 * rows, width), BF16),
            pltpu.VMEM((4 * rows, width), BF16),
            pltpu.VMEM((width, 4 * rows), BF16),
            pltpu.VMEM((width, rows), BF16),
            pltpu.VMEM((2, 2 * rows, rows), F32),
            pltpu.VMEM((width, rows), BF16),
            block,
            block,
            block,
            *([] if far_given else [block]),
            *attend_scratch(width // GW, rows),
            pltpu.SemaphoreType.DMA((5,)),
            pltpu.SemaphoreType.DMA((2,)),
            pltpu.SemaphoreType.DMA((2, parts)),
            pltpu.SemaphoreType.DMA((2, parts)),
        ],
        cost_estimate=pl.CostEstimate(flops=flops, bytes_accessed=10 * width * width, transcendentals=0),
        compiler_params=pltpu.CompilerParams(vmem_limit_bytes=VMEM_LIMIT, collective_id=layer, has_side_effects=True),
        name="self_attention",
    )(own, *([far] if far_given else []), gs, gc, wq, wk, wv, wo, wcq)


def cross_kernel(layer, planes, n_kv, lim_ref, q_ref, *refs):
    def take(n):
        nonlocal refs
        head, refs = refs[:n], refs[n:]
        return head

    ks, vts = take(n_kv), take(n_kv)
    hid_ref, gm_ref, wco, wg, wu, wd, out_ref = take(7)
    scratch = take(7)
    kbuf, vbuf, mask, list_s, kv_sems = take(5)
    at_s, a_s, act0, act1, acc_o, wo_s, wg_s, wu_s, wd_s, o_sem, w_sems = take(11)
    ring, ff = wg_s.shape[0], wg_s.shape[2]
    steps = wg.shape[2] // ff
    width, rows = q_ref.shape
    groups = width // GW

    def kv_copies(i, go):
        slot = lax.rem(i, 2)
        cols = pl.ds(pl.multiple_of(i * GW, GW), GW)
        at = 0
        for n in range(n_kv):
            there = pl.ds(at, ks[n].shape[1])
            go(pltpu.make_async_copy(ks[n].at[planes[n], :, cols], kbuf.at[slot, there, :], kv_sems.at[slot, 0, n]))
            go(pltpu.make_async_copy(vts[n].at[planes[n], cols, :], vbuf.at[slot, :, there], kv_sems.at[slot, 1, n]))
            at += ks[n].shape[1]

    def kv_start(i):
        kv_copies(i, lambda cp: cp.start())

    kv_start(0)
    kv_start(1)
    o_copy = pltpu.make_async_copy(wco.at[layer], wo_s, o_sem)

    def w_copies(j):
        cols = pl.ds(pl.multiple_of(j * ff, ff), ff)
        slot = lax.rem(j, ring)
        return (pltpu.make_async_copy(wg.at[layer, :, cols], wg_s.at[slot], w_sems.at[0, slot]),
                pltpu.make_async_copy(wu.at[layer, :, cols], wu_s.at[slot], w_sems.at[1, slot]),
                pltpu.make_async_copy(wd.at[layer, cols, :], wd_s.at[slot], w_sems.at[2, slot]))

    def w_start(j):
        for cp in w_copies(j):
            cp.start()

    attend_reset(scratch)

    n_chunks, last = jnp.int32(0), jnp.int32(0)
    list_s[0] = 0
    for c in range(lim_ref.shape[0]):
        lim = lim_ref[c]

        @pl.when(lim > 0)
        def _(c=c, at=n_chunks):
            list_s[at] = c

        n_chunks = n_chunks + (lim > 0).astype(jnp.int32)
        last = last + jnp.where(lim < CH, lim, 0)
    key = lax.broadcasted_iota(jnp.int32, (CH, 128), 0)
    lane = lax.broadcasted_iota(jnp.int32, (CH, 128), 1)
    mask[0] = jnp.zeros((CH, 128), BF16)
    mask[1] = jnp.where((key >= last) & (lane == 0), NEG_BIG, 0.0).astype(BF16)
    ones = (lax.broadcasted_iota(jnp.int32, (128, rows), 0) == 0).astype(F32).astype(BF16)

    def enter(i):
        kv_copies(i, lambda cp: cp.wait())

        @pl.when(i == 0)
        def _():
            o_copy.start()
            for j in range(ring - groups):
                w_start(j)

        w_start(ring - groups + i)

    def leave(i):
        @pl.when(i + 2 < groups)
        def _():
            kv_start(i + 2)

    def chunk(j):
        return pl.ds(pl.multiple_of(list_s[j] * CH, CH), CH)

    def scores(i, j):
        partial = (lim_ref[list_s[j]] < CH).astype(jnp.int32)
        k = kbuf[lax.rem(i, 2), chunk(j), :]
        ks = [jnp.concatenate([k[:, p * 128:(p + 1) * 128], mask[partial]], axis=1) for p in range(HEADS // 2)]
        queries = head_queries(q_ref[pl.ds(pl.multiple_of(i * GW, GW), GW), :], ones)
        return (dot(ks[h // 2], q) for h, q in enumerate(queries))

    def values(i, j):
        return vbuf[lax.rem(i, 2), :, chunk(j)]

    attend_all(groups, n_chunks, scores, values, enter, leave, scratch)

    def finish(i, _):
        attend_finish(i, at_s, scratch)
        return 0

    lax.fori_loop(0, groups, finish, 0)
    a_s[...] = at_s[...].T
    o_copy.wait()

    out_ref[...] = (hid_ref[...].astype(F32) + dot(a_s[...], wo_s[...])).astype(BF16)
    a_s[...] = rms(out_ref[...], gm_ref[layer:layer + 1, :])
    acc_o[...] = jnp.zeros_like(acc_o)

    def wait_gate_up(j):
        for cp in w_copies(j)[:2]:
            cp.wait()

    def gate_up(j, act_ref):
        x = a_s[...]
        gate = dot(x, wg_s[lax.rem(j, ring)])
        up = dot(x, wu_s[lax.rem(j, ring)])
        act_ref[...] = (gate / (1.0 + jnp.exp(-gate)) * up).astype(BF16)

    wait_gate_up(0)
    gate_up(0, act0)

    def mlp_step(u, _):
        first = 2 * u
        w_copies(first)[2].wait()
        wait_gate_up(first + 1)
        w_copies(first + 1)[2].wait()

        @pl.when(first + 2 < steps)
        def _():
            wait_gate_up(first + 2)

        acc_o[...] += dot(act0[...], wd_s[lax.rem(first, ring)])
        gate_up(first + 1, act1)
        acc_o[...] += dot(act1[...], wd_s[lax.rem(first + 1, ring)])
        gate_up(jnp.minimum(first + 2, steps - 1), act0)

        for j in (first, first + 1):
            @pl.when(j + ring < steps)
            def _(j=j):
                w_start(j + ring)
        return 0

    lax.fori_loop(0, steps // 2, mlp_step, 0)
    out_ref[...] = (out_ref[...].astype(F32) + acc_o[...]).astype(BF16)


def cross_mlp(layer, lims, q, kvs, hid, gm, wco, wg, wu, wd):
    width, rows = q.shape
    groups = width // GW
    planes = tuple(plane for _, _, plane in kvs)
    ks, vts = [k for k, _, _ in kvs], [v for _, v, _ in kvs]
    total = sum(k.shape[1] for k in ks)
    n = len(kvs)
    ff, ring = 512, 6
    return pl.pallas_call(
        functools.partial(cross_kernel, layer, planes, n),
        in_specs=[SMEM, VMEM] + [ANY] * (2 * n) + [VMEM] * 2 + [ANY] * 4,
        out_specs=VMEM,
        out_shape=jax.ShapeDtypeStruct((rows, width), BF16),
        scratch_shapes=attend_scratch(groups, rows) + [
            pltpu.VMEM((2, total, GW), BF16),
            pltpu.VMEM((2, GW, total), BF16),
            pltpu.VMEM((2, CH, 128), BF16),
            pltpu.SMEM((8,), jnp.int32),
            pltpu.SemaphoreType.DMA((2, 2, n)),
            pltpu.VMEM((width, rows), BF16),
            pltpu.VMEM((rows, width), BF16),
            pltpu.VMEM((rows, ff), BF16),
            pltpu.VMEM((rows, ff), BF16),
            pltpu.VMEM((rows, width), F32),
            pltpu.VMEM((width, width), BF16),
            pltpu.VMEM((ring, width, ff), BF16),
            pltpu.VMEM((ring, width, ff), BF16),
            pltpu.VMEM((ring, ff, width), BF16),
            pltpu.SemaphoreType.DMA,
            pltpu.SemaphoreType.DMA((3, ring)),
        ],
        cost_estimate=pl.CostEstimate(
            flops=4 * rows * 3072 * width + 2 * rows * width * (width + 3 * wg.shape[2]),
            bytes_accessed=2 * width * (width + 3 * wg.shape[2]), transcendentals=0),
        compiler_params=pltpu.CompilerParams(vmem_limit_bytes=VMEM_LIMIT),
        name="cross_mlp",
    )(lims, q, *ks, *vts, hid, gm, wco, wg, wu, wd)


NONE = 1 << 20
BASES = (
    (0, 512, 1024, 1536, 2048, NONE, 2560, NONE),
    (1024, 1536, 0, 512, 2560, NONE, 2048, NONE),
    (2048, NONE, 2560, NONE, 0, 512, 1024, 1536),
    (2560, NONE, 2048, NONE, 1024, 1536, 0, 512),
)
FIRST = 768


def solution(mesh):
    row_spec = P(('dp', 'sp'), None)

    def local_step(hidden, memory, mem_len, norm_self, norm_cross, norm_mlp, self_q, self_k, self_v, self_o, cross_q, cross_k, cross_v, cross_o, mlp_gate, mlp_up, mlp_down):
        layers, width = norm_self.shape
        w_so = self_o.reshape(layers, width, width)
        w_co = cross_o.reshape(layers, width, width)
        dev = lax.axis_index('sp')
        dev_arr = dev.astype(jnp.int32).reshape(1)
        bases = jnp.array(BASES, jnp.int32)[dev]
        lims = jnp.clip(mem_len[0] - bases, 0, CH)
        is1, is3 = (dev_arr == 1).astype(jnp.int32), (dev_arr == 3).astype(jnp.int32)

        def swap(x):
            return lax.ppermute(x, 'sp', [(0, 1), (1, 0), (2, 3), (3, 2)])

        def program(hidden):
            far = lax.ppermute(hidden, 'sp', [(0, 2), (1, 3)])
            mem_a, mem_b, mem_c = memory[:FIRST], memory[FIRST:], memory[CH:]
            c2b = lax.ppermute(mem_c, 'sp', [(2, 3)])
            rem_a = lax.ppermute(mem_a, 'sp', [(0, 2), (1, 3), (2, 0)])
            back = lax.ppermute(c2b, 'sp', [(3, 1)])
            rem_b = lax.ppermute(mem_b, 'sp', [(0, 2), (1, 3)])

            both = (0, layers)
            ka, va = kv_project(lims[0:2], is3, [memory, c2b], cross_k, cross_v, 2 * CH, both)
            kas, vas = swap(ka), swap(va)
            kb, vb = kv_project(lims[4:6], is1, [rem_a, back], cross_k, cross_v, FIRST, both)
            kbs, vbs = swap(kb), swap(vb)
            kvs = []
            for layer in range(layers):
                kc, vc = kv_project(lims[5:6], is1, [rem_b], cross_k, cross_v, 2 * CH - FIRST, (layer, 1))
                kcs, vcs = swap(kc), swap(vc)
                kvs.append([(ka, va, layer), (kas, vas, layer), (kb, vb, layer), (kc, vc, 0), (kbs, vbs, layer), (kcs, vcs, 0)])

            for layer in range(layers):
                hidden, q = self_attention(layer, hidden, far, norm_self, norm_cross, self_q, self_k, self_v, w_so, cross_q)
                hidden = cross_mlp(layer, lims, q, kvs[layer], hidden, norm_mlp, w_co, mlp_gate, mlp_up, mlp_down)
                far = None
            return hidden

        return program(hidden)

    return jax.shard_map(local_step, mesh=mesh, in_specs=(row_spec, row_spec, P('dp')) + (P(),) * 14, out_specs=row_spec, check_vma=False)
```

```python
import functools

import jax
import jax.numpy as jnp
from jax import lax
from jax.experimental import pallas as pl
from jax.experimental.pallas import tpu as pltpu
from jax.sharding import PartitionSpec as P


EPS = 1e-6
NEG_BIG = -1e30
F32 = jnp.float32
BF16 = jnp.bfloat16
CH = 512
HEADS = 4
GW = HEADS * 64
VMEM_LIMIT = 62 * 1024 * 1024
ANY = pl.BlockSpec(memory_space=pltpu.HBM)
SMEM = pl.BlockSpec(memory_space=pltpu.SMEM)
VMEM = pl.BlockSpec(memory_space=pltpu.VMEM)


def rms(h, gain):
    h32 = h.astype(F32)
    inv = lax.rsqrt(jnp.mean(h32 * h32, axis=-1, keepdims=True) + EPS)
    return (h32 * inv * gain.astype(F32)).astype(BF16)


def dot(a, b):
    return jnp.dot(a, b, preferred_element_type=F32)


def kv_kernel(layers, n_src, lim_ref, pick_ref, *refs):
    srcs, (wk, wv, k_out, vt_out, mem, w_s, k_s, vt_s, sem, w_sems, o_sems) = refs[:n_src], refs[n_src:]
    rows = mem.shape[0]
    lo, n = layers

    def from_src(go):
        if n_src == 1:
            go(pltpu.make_async_copy(srcs[0], mem, sem))
        else:
            @pl.when(pick_ref[0] == 0)
            def _():
                go(pltpu.make_async_copy(srcs[0], mem, sem))

            @pl.when(pick_ref[0] != 0)
            def _():
                go(pltpu.make_async_copy(srcs[1], mem.at[pl.ds(0, CH)], sem))

    def w_copy(i, v):
        return pltpu.make_async_copy((wk, wv)[v].at[lo + i], w_s.at[2 * i + v], w_sems.at[2 * i + v])

    w_copy(0, 0).start()
    from_src(lambda cp: cp.start())
    from_src(lambda cp: cp.wait())
    w_copy(0, 1).start()

    def out_copy(i, v, c):
        at = pl.ds(pl.multiple_of(c * CH, CH), CH)
        if v == 0:
            return pltpu.make_async_copy(k_s.at[i, at, :], k_out.at[i, at, :], o_sems.at[i, v, c])
        return pltpu.make_async_copy(vt_s.at[i, :, at], vt_out.at[i, :, at], o_sems.at[i, v, c])

    def valid(c, go):
        @pl.when(lim_ref[c] > 0)
        def _():
            go()

    def layer_step(i, _):
        for v in range(2):
            w_copy(i, v).wait()

            @pl.when(i + 1 < n)
            def _(v=v):
                w_copy(i + 1, v).start()

            def chunk_step(c, _):
                def work():
                    def step(r, _):
                        at = pl.ds(pl.multiple_of(c * CH + r * 256, 256), 256)
                        out = dot(mem[at, :], w_s[2 * i + v]).astype(BF16)
                        if v == 0:
                            k_s[i, at, :] = out
                        else:
                            vt_s[i, :, at] = out.T
                        return 0

                    lax.fori_loop(0, CH // 256, step, 0)
                    out_copy(i, v, c).start()

                valid(c, work)
                return 0

            lax.fori_loop(0, rows // CH, chunk_step, 0)
        return 0

    lax.fori_loop(0, n, layer_step, 0)
    for i in range(n):
        for v in range(2):
            for c in range(rows // CH):
                valid(c, lambda i=i, v=v, c=c: out_copy(i, v, c).wait())


def kv_project(lims, pick, srcs, wk, wv, rows, layers):
    width, cols = wk.shape[1], wk.shape[2]
    n = layers[1]
    flops = n * 4 * rows * width * cols
    return pl.pallas_call(
        functools.partial(kv_kernel, layers, len(srcs)),
        in_specs=[SMEM, SMEM] + [ANY] * (len(srcs) + 2),
        out_specs=[ANY, ANY],
        out_shape=[jax.ShapeDtypeStruct((n, rows, cols), BF16), jax.ShapeDtypeStruct((n, cols, rows), BF16)],
        scratch_shapes=[
            pltpu.VMEM((rows, width), BF16),
            pltpu.VMEM((2 * n, width, cols), BF16),
            pltpu.VMEM((n, rows, cols), BF16),
            pltpu.VMEM((n, cols, rows), BF16),
            pltpu.SemaphoreType.DMA,
            pltpu.SemaphoreType.DMA((2 * n,)),
            pltpu.SemaphoreType.DMA((n, 2, rows // CH)),
        ],
        cost_estimate=pl.CostEstimate(flops=flops, bytes_accessed=n * 4 * width * cols, transcendentals=0),
        compiler_params=pltpu.CompilerParams(vmem_limit_bytes=VMEM_LIMIT),
        name="kv_project",
    )(lims, pick, *srcs, wk, wv)


def head_queries(qt, extra=None):
    row = lax.broadcasted_iota(jnp.int32, (128, qt.shape[1]), 0)
    out = []
    for h in range(HEADS):
        pair = qt[h // 2 * 128:(h // 2 + 1) * 128, :]
        q = jnp.where((row < 64) == (h % 2 == 0), pair, jnp.zeros_like(pair))
        out.append(q if extra is None else jnp.concatenate([q, extra], axis=0))
    return out


def attend_all(groups, n_chunks, scores, values, enter, leave, scratch):
    s_refs, mx_refs, (m_ref, l_ref, acc_ref) = scratch[:2], scratch[2:4], scratch[4:]
    total = groups * n_chunks

    def stage1(group, j, buf):
        for h, s in enumerate(scores(group, j)):
            first(h, s, buf)

    def first(h, s, buf):
        s_refs[buf][h] = s
        mx_refs[buf][h:h + 1, :] = jnp.max(s, axis=0, keepdims=True)

    def second(group, h, vt, buf):
        m_old = m_ref[group, h:h + 1, :]
        m_new = jnp.maximum(m_old, mx_refs[buf][h:h + 1, :])
        p = jnp.exp(s_refs[buf][h] - m_new)
        alpha = jnp.exp(m_old - m_new)
        m_ref[group, h:h + 1, :] = m_new
        l_ref[group, h:h + 1, :] = l_ref[group, h:h + 1, :] * alpha + jnp.sum(p, axis=0, keepdims=True)
        acc_ref[group, h] = acc_ref[group, h] * alpha + dot(vt[h * 64:(h + 1) * 64, :], p.astype(BF16))

    def advance(group, j):
        wrap = j + 1 == n_chunks
        return jnp.where(wrap, group + 1, group), jnp.where(wrap, 0, j + 1)

    enter(0)
    stage1(0, 0, 0)

    def item(group, j, buf):
        group_next, j_next = advance(group, j)

        @pl.when((j_next == 0) & (group_next < groups))
        def _():
            enter(group_next)

        made = scores(jnp.minimum(group_next, groups - 1), j_next)
        vt = values(group, j)
        for h in range(HEADS):
            first(h, next(made), 1 - buf)
            second(group, h, vt, buf)

        @pl.when(j_next == 0)
        def _():
            leave(group)

    def step(u, now):
        item(*now, 0)
        now = advance(*now)

        @pl.when(2 * u + 1 < total)
        def _():
            item(*now, 1)

        return advance(*now)

    lax.fori_loop(0, (total + 1) // 2, step, (jnp.int32(0), jnp.int32(0)))


def attend_reset(scratch):
    m_ref, l_ref, acc_ref = scratch[4:]
    m_ref[...] = jnp.full_like(m_ref, -jnp.inf)
    l_ref[...] = jnp.zeros_like(l_ref)
    acc_ref[...] = jnp.zeros_like(acc_ref)


def attend_finish(group, at_ref, scratch):
    l_ref, acc_ref = scratch[5:]
    for h in range(HEADS):
        rows = pl.ds(pl.multiple_of(group * HEADS * 64 + h * 64, 64), 64)
        at_ref[rows, :] = (acc_ref[group, h] / l_ref[group, h:h + 1, :]).astype(BF16)


def attend_scratch(groups, rows):
    return [
        pltpu.VMEM((HEADS, CH, rows), F32),
        pltpu.VMEM((HEADS, CH, rows), F32),
        pltpu.VMEM((HEADS, rows), F32),
        pltpu.VMEM((HEADS, rows), F32),
        pltpu.VMEM((groups, HEADS, rows), F32),
        pltpu.VMEM((groups, HEADS, rows), F32),
        pltpu.VMEM((groups, HEADS, 64, rows), F32),
    ]


def self_kernel(layer, far_given, *refs):
    own_ref, refs = refs[0], refs[1:]
    if far_given:
        s2, refs = refs[0], refs[1:]
    gs_ref, gc_ref, wq, wk, wv, wo, wcq, hid_ref, q_ref, w_s, x_s, k_s, vt_s, qs, bias, at_s, a_s, s1, s3 = refs[:19]
    refs = refs[19:]
    if not far_given:
        s2, refs = refs[0], refs[1:]
    scratch, (sems, near_sems, far_sems, fwd_sems) = refs[:7], refs[7:]
    rows, width = own_ref.shape
    parts = far_sems.shape[1]
    parts_half = parts // 2
    dev = lax.axis_index("sp")
    odd = lax.rem(dev, 2)
    chip1 = dev >= 2
    sibling = dev + 1 - 2 * odd
    across = lax.rem(dev + 2, 4)

    w_copies = [pltpu.make_async_copy(src.at[layer], w_s.at[n], sems.at[n]) for n, src in enumerate((wk, wv, wq, wo, wcq))]
    w_copies[0].start()
    w_copies[1].start()

    barrier = pltpu.get_barrier_semaphore()
    others = (sibling,) if far_given else (sibling, across)
    for other in others:
        pl.semaphore_signal(barrier, inc=1, device_id={"sp": other}, device_id_type=pl.DeviceIdType.MESH)
    pl.semaphore_wait(barrier, len(others))

    def send(src, dst, sem, other):
        return pltpu.make_async_remote_copy(src_ref=src, dst_ref=dst, send_sem=sem.at[0], recv_sem=sem.at[1],
                                            device_id={"sp": other}, device_id_type=pl.DeviceIdType.MESH)

    def part(i):
        return pl.ds(i * (rows // parts), rows // parts)

    near = send(own_ref, s1, near_sems, sibling)
    far = [send(own_ref.at[part(i)], s2.at[part(i)], far_sems.at[:, i], across) for i in range(parts)]
    fwd = [send(s2.at[part(i)], s3.at[part(i)], fwd_sems.at[:, i], sibling) for i in range(parts)]

    if not far_given:
        @pl.when(jnp.logical_not(chip1))
        def _():
            for cp in far:
                cp.start()

    @pl.when(odd == 0)
    def _():
        near.start()

    if far_given:
        @pl.when(chip1)
        def _():
            for cp in fwd:
                cp.start()

    gain = gs_ref[layer:layer + 1, :]
    x_s[pl.ds(0, rows), :] = rms(own_ref[...], gain)
    key = lax.broadcasted_iota(jnp.int32, (rows, rows), 0)
    query = lax.broadcasted_iota(jnp.int32, (rows, rows), 1)
    bias[0, pl.ds(0, rows), :] = jnp.where(key <= query, 0.0, NEG_BIG)
    bias[0, pl.ds(rows, rows), :] = jnp.full((rows, rows), jnp.where(odd == 1, 0.0, NEG_BIG), F32)
    bias[1] = jnp.zeros((2 * rows, rows), F32)
    attend_reset(scratch)

    @pl.when(odd == 1)
    def _():
        near.wait_recv()
        x_s[pl.ds(rows, rows), :] = rms(s1[...], gain)

    @pl.when(odd == 0)
    def _():
        x_s[pl.ds(rows, rows), :] = jnp.zeros((rows, width), BF16)

    def tile(t):
        return pl.ds(pl.multiple_of(t * 256, 256), 256)

    def head_cols(i):
        return pl.ds(pl.multiple_of(i * GW, GW), GW)

    def phase(half, _):
        at = pl.ds(pl.multiple_of(half * CH, CH), CH)

        @pl.when(half == 0)
        def _():
            w_copies[0].wait()
            w_copies[2].start()

        def project_step(r, _):
            rows_at = tile(2 * half + r)
            for first in range(0, parts, parts_half):
                @pl.when((half == 1) & (r == first // parts_half))
                def _(first=first):
                    some = range(first, first + parts_half)
                    if not far_given:
                        for i in some:
                            far[i].wait_recv()
                            fwd[i].start()
                    here = pl.ds(first * (rows // parts), rows // 2)
                    x_s[pl.ds(2 * rows + 2 * first * (rows // parts), rows // 2), :] = rms(s2[here, :], gain)
                    for i in some:
                        fwd[i].wait_recv()
                    x_s[pl.ds(2 * rows + 2 * first * (rows // parts) + rows // 2, rows // 2), :] = rms(s3[here, :], gain)

            k_s[rows_at, :] = dot(x_s[rows_at, :], w_s[0]).astype(BF16)

            @pl.when((half == 0) & (r == 0))
            def _():
                w_copies[1].wait()
                w_copies[3].start()

            vt_s[:, rows_at] = dot(x_s[rows_at, :], w_s[1]).astype(BF16).T
            return 0

        lax.fori_loop(0, 2, project_step, 0)

        @pl.when(half == 0)
        def _():
            w_copies[2].wait()
            w_copies[4].start()

            qs[...] = (dot(x_s[pl.ds(0, rows), :], w_s[2]).astype(BF16) * BF16(0.125)).T

        def scores(i, j):
            k = k_s[at, head_cols(i)]
            return (dot(k[:, h // 2 * 128:(h // 2 + 1) * 128], q) + bias[half] for h, q in enumerate(head_queries(qs[head_cols(i), :])))

        attend_all(width // GW, 1, scores, lambda i, j: vt_s[head_cols(i), at], lambda i: None, lambda i: None, scratch)
        return 0

    lax.fori_loop(0, jnp.where(chip1, 2, 1), phase, 0)

    def finish(i, _):
        attend_finish(i, at_s, scratch)
        return 0

    lax.fori_loop(0, width // GW, finish, 0)
    a_s[...] = at_s[...].T
    w_copies[3].wait()

    hid_ref[...] = (own_ref[...].astype(F32) + dot(a_s[...], w_s[3])).astype(BF16)
    a_s[...] = rms(hid_ref[...], gc_ref[layer:layer + 1, :])
    w_copies[4].wait()

    q_ref[...] = (dot(a_s[...], w_s[4]).astype(BF16) * BF16(0.125)).T

    @pl.when(odd == 0)
    def _():
        near.wait_send()

    @pl.when(chip1)
    def _():
        for cp in fwd:
            cp.wait_send()

    if not far_given:
        @pl.when(jnp.logical_not(chip1))
        def _():
            for cp in far:
                cp.wait_send()


def self_attention(layer, own, far, gs, gc, wq, wk, wv, wo, wcq):
    rows, width = own.shape
    far_given = far is not None
    parts = 2 if far_given else 4
    shape = jax.ShapeDtypeStruct((rows, width), BF16)
    flops = 2 * rows * width * width * 11 + 4 * rows * 4 * rows * width
    block = pltpu.VMEM((rows, width), BF16)
    return pl.pallas_call(
        functools.partial(self_kernel, layer, far_given),
        in_specs=[VMEM] * (4 if far_given else 3) + [ANY] * 5,
        out_specs=[VMEM, VMEM],
        out_shape=[shape, jax.ShapeDtypeStruct((width, rows), BF16)],
        scratch_shapes=[
            pltpu.VMEM((5, width, width), BF16),
            pltpu.VMEM((4 * rows, width), BF16),
            pltpu.VMEM((4 * rows, width), BF16),
            pltpu.VMEM((width, 4 * rows), BF16),
            pltpu.VMEM((width, rows), BF16),
            pltpu.VMEM((2, 2 * rows, rows), F32),
            pltpu.VMEM((width, rows), BF16),
            block,
            block,
            block,
            *([] if far_given else [block]),
            *attend_scratch(width // GW, rows),
            pltpu.SemaphoreType.DMA((5,)),
            pltpu.SemaphoreType.DMA((2,)),
            pltpu.SemaphoreType.DMA((2, parts)),
            pltpu.SemaphoreType.DMA((2, parts)),
        ],
        cost_estimate=pl.CostEstimate(flops=flops, bytes_accessed=10 * width * width, transcendentals=0),
        compiler_params=pltpu.CompilerParams(vmem_limit_bytes=VMEM_LIMIT, collective_id=layer, has_side_effects=True),
        name="self_attention",
    )(own, *([far] if far_given else []), gs, gc, wq, wk, wv, wo, wcq)


def cross_kernel(layer, planes, n_kv, lim_ref, q_ref, *refs):
    def take(n):
        nonlocal refs
        head, refs = refs[:n], refs[n:]
        return head

    ks, vts = take(n_kv), take(n_kv)
    hid_ref, gm_ref, wco, wg, wu, wd, out_ref = take(7)
    scratch = take(7)
    kbuf, vbuf, mask, list_s, kv_sems = take(5)
    at_s, a_s, act0, act1, acc_o, wo_s, wg_s, wu_s, wd_s, o_sem, w_sems = take(11)
    ring, ff = wg_s.shape[0], wg_s.shape[2]
    steps = wg.shape[2] // ff
    width, rows = q_ref.shape
    groups = width // GW

    def kv_copies(i, go):
        slot = lax.rem(i, 2)
        cols = pl.ds(pl.multiple_of(i * GW, GW), GW)
        at = 0
        for n in range(n_kv):
            there = pl.ds(at, ks[n].shape[1])
            go(pltpu.make_async_copy(ks[n].at[planes[n], :, cols], kbuf.at[slot, there, :], kv_sems.at[slot, 0, n]))
            go(pltpu.make_async_copy(vts[n].at[planes[n], cols, :], vbuf.at[slot, :, there], kv_sems.at[slot, 1, n]))
            at += ks[n].shape[1]

    def kv_start(i):
        kv_copies(i, lambda cp: cp.start())

    kv_start(0)
    o_copy = pltpu.make_async_copy(wco.at[layer], wo_s, o_sem)

    def w_copies(j):
        cols = pl.ds(pl.multiple_of(j * ff, ff), ff)
        slot = lax.rem(j, ring)
        return (pltpu.make_async_copy(wg.at[layer, :, cols], wg_s.at[slot], w_sems.at[0, slot]),
                pltpu.make_async_copy(wu.at[layer, :, cols], wu_s.at[slot], w_sems.at[1, slot]),
                pltpu.make_async_copy(wd.at[layer, cols, :], wd_s.at[slot], w_sems.at[2, slot]))

    def w_start(j):
        for cp in w_copies(j):
            cp.start()

    attend_reset(scratch)

    n_chunks, last = jnp.int32(0), jnp.int32(0)
    list_s[0] = 0
    for c in range(lim_ref.shape[0]):
        lim = lim_ref[c]

        @pl.when(lim > 0)
        def _(c=c, at=n_chunks):
            list_s[at] = c

        n_chunks = n_chunks + (lim > 0).astype(jnp.int32)
        last = last + jnp.where(lim < CH, lim, 0)
    key = lax.broadcasted_iota(jnp.int32, (CH, 128), 0)
    lane = lax.broadcasted_iota(jnp.int32, (CH, 128), 1)
    mask[0] = jnp.zeros((CH, 128), BF16)
    mask[1] = jnp.where((key >= last) & (lane == 0), NEG_BIG, 0.0).astype(BF16)
    ones = (lax.broadcasted_iota(jnp.int32, (128, rows), 0) == 0).astype(F32).astype(BF16)

    def enter(i):
        kv_copies(i, lambda cp: cp.wait())

        @pl.when(i == 0)
        def _():
            kv_start(1)
            o_copy.start()
            for j in range(ring - groups):
                w_start(j)

        w_start(ring - groups + i)

    def leave(i):
        @pl.when(i + 2 < groups)
        def _():
            kv_start(i + 2)

    def chunk(j):
        return pl.ds(pl.multiple_of(list_s[j] * CH, CH), CH)

    def scores(i, j):
        partial = (lim_ref[list_s[j]] < CH).astype(jnp.int32)
        k = kbuf[lax.rem(i, 2), chunk(j), :]
        ks = [jnp.concatenate([k[:, p * 128:(p + 1) * 128], mask[partial]], axis=1) for p in range(HEADS // 2)]
        queries = head_queries(q_ref[pl.ds(pl.multiple_of(i * GW, GW), GW), :], ones)
        return (dot(ks[h // 2], q) for h, q in enumerate(queries))

    def values(i, j):
        return vbuf[lax.rem(i, 2), :, chunk(j)]

    attend_all(groups, n_chunks, scores, values, enter, leave, scratch)

    def finish(i, _):
        attend_finish(i, at_s, scratch)
        return 0

    lax.fori_loop(0, groups, finish, 0)
    a_s[...] = at_s[...].T
    o_copy.wait()

    out_ref[...] = (hid_ref[...].astype(F32) + dot(a_s[...], wo_s[...])).astype(BF16)
    a_s[...] = rms(out_ref[...], gm_ref[layer:layer + 1, :])
    acc_o[...] = jnp.zeros_like(acc_o)

    def wait_gate_up(j):
        for cp in w_copies(j)[:2]:
            cp.wait()

    def gate_up(j, act_ref):
        x = a_s[...]
        gate = dot(x, wg_s[lax.rem(j, ring)])
        up = dot(x, wu_s[lax.rem(j, ring)])
        act_ref[...] = (gate / (1.0 + jnp.exp(-gate)) * up).astype(BF16)

    wait_gate_up(0)
    gate_up(0, act0)

    def mlp_step(u, _):
        first = 2 * u
        w_copies(first)[2].wait()
        wait_gate_up(first + 1)
        w_copies(first + 1)[2].wait()

        @pl.when(first + 2 < steps)
        def _():
            wait_gate_up(first + 2)

        acc_o[...] += dot(act0[...], wd_s[lax.rem(first, ring)])
        gate_up(first + 1, act1)
        acc_o[...] += dot(act1[...], wd_s[lax.rem(first + 1, ring)])
        gate_up(jnp.minimum(first + 2, steps - 1), act0)

        for j in (first, first + 1):
            @pl.when(j + ring < steps)
            def _(j=j):
                w_start(j + ring)
        return 0

    lax.fori_loop(0, steps // 2, mlp_step, 0)
    out_ref[...] = (out_ref[...].astype(F32) + acc_o[...]).astype(BF16)


def cross_mlp(layer, lims, q, kvs, hid, gm, wco, wg, wu, wd):
    width, rows = q.shape
    groups = width // GW
    planes = tuple(plane for _, _, plane in kvs)
    ks, vts = [k for k, _, _ in kvs], [v for _, v, _ in kvs]
    total = sum(k.shape[1] for k in ks)
    n = len(kvs)
    ff, ring = 512, 6
    return pl.pallas_call(
        functools.partial(cross_kernel, layer, planes, n),
        in_specs=[SMEM, VMEM] + [ANY] * (2 * n) + [VMEM] * 2 + [ANY] * 4,
        out_specs=VMEM,
        out_shape=jax.ShapeDtypeStruct((rows, width), BF16),
        scratch_shapes=attend_scratch(groups, rows) + [
            pltpu.VMEM((2, total, GW), BF16),
            pltpu.VMEM((2, GW, total), BF16),
            pltpu.VMEM((2, CH, 128), BF16),
            pltpu.SMEM((8,), jnp.int32),
            pltpu.SemaphoreType.DMA((2, 2, n)),
            pltpu.VMEM((width, rows), BF16),
            pltpu.VMEM((rows, width), BF16),
            pltpu.VMEM((rows, ff), BF16),
            pltpu.VMEM((rows, ff), BF16),
            pltpu.VMEM((rows, width), F32),
            pltpu.VMEM((width, width), BF16),
            pltpu.VMEM((ring, width, ff), BF16),
            pltpu.VMEM((ring, width, ff), BF16),
            pltpu.VMEM((ring, ff, width), BF16),
            pltpu.SemaphoreType.DMA,
            pltpu.SemaphoreType.DMA((3, ring)),
        ],
        cost_estimate=pl.CostEstimate(
            flops=4 * rows * 3072 * width + 2 * rows * width * (width + 3 * wg.shape[2]),
            bytes_accessed=2 * width * (width + 3 * wg.shape[2]), transcendentals=0),
        compiler_params=pltpu.CompilerParams(vmem_limit_bytes=VMEM_LIMIT),
        name="cross_mlp",
    )(lims, q, *ks, *vts, hid, gm, wco, wg, wu, wd)


NONE = 1 << 20
BASES = (
    (0, 512, 1024, 1536, 2048, NONE, NONE, 2560),
    (1024, 1536, 0, 512, NONE, 2048, 2560, NONE),
    (2048, NONE, 2560, NONE, 0, 1024, 512, 1536),
    (2560, NONE, 2048, NONE, 1024, 0, 1536, 512),
)


def solution(mesh):
    row_spec = P(('dp', 'sp'), None)

    def local_step(hidden, memory, mem_len, norm_self, norm_cross, norm_mlp, self_q, self_k, self_v, self_o, cross_q, cross_k, cross_v, cross_o, mlp_gate, mlp_up, mlp_down):
        layers, width = norm_self.shape
        w_so = self_o.reshape(layers, width, width)
        w_co = cross_o.reshape(layers, width, width)
        dev = lax.axis_index('sp')
        dev_arr = dev.astype(jnp.int32).reshape(1)
        bases = jnp.array(BASES, jnp.int32)[dev]
        lims = jnp.clip(mem_len[0] - bases, 0, CH)
        is3 = (dev_arr == 3).astype(jnp.int32)

        def swap(x):
            return lax.ppermute(x, 'sp', [(0, 1), (1, 0), (2, 3), (3, 2)])

        def program(hidden):
            far = lax.ppermute(hidden, 'sp', [(0, 2), (1, 3)])
            mem_a, mem_b = memory[:CH], memory[CH:]
            c2b = lax.ppermute(mem_b, 'sp', [(2, 3)])
            rem_a = lax.ppermute(mem_a, 'sp', [(0, 2), (1, 3), (2, 0)])
            rem_b = lax.ppermute(mem_b, 'sp', [(0, 2), (1, 3), (2, 1)])

            both = (0, layers)
            ka, va = kv_project(lims[0:2], is3, [memory, c2b], cross_k, cross_v, 2 * CH, both)
            kas, vas = swap(ka), swap(va)
            kb, vb = kv_project(lims[4:5], is3, [rem_a], cross_k, cross_v, CH, both)
            kbs, vbs = swap(kb), swap(vb)
            kvs = []
            for layer in range(layers):
                kc, vc = kv_project(lims[6:7], is3, [rem_b], cross_k, cross_v, CH, (layer, 1))
                kcs, vcs = swap(kc), swap(vc)
                kvs.append([(ka, va, layer), (kas, vas, layer), (kb, vb, layer), (kbs, vbs, layer), (kc, vc, 0), (kcs, vcs, 0)])

            for layer in range(layers):
                hidden, q = self_attention(layer, hidden, far, norm_self, norm_cross, self_q, self_k, self_v, w_so, cross_q)
                hidden = cross_mlp(layer, lims, q, kvs[layer], hidden, norm_mlp, w_co, mlp_gate, mlp_up, mlp_down)
                far = None
            return hidden

        return program(hidden)

    return jax.shard_map(local_step, mesh=mesh, in_specs=(row_spec, row_spec, P('dp')) + (P(),) * 14, out_specs=row_spec, check_vma=False)
```

```python
import functools

import jax
import jax.numpy as jnp
from jax import lax
from jax.experimental import pallas as pl
from jax.experimental.pallas import tpu as pltpu
from jax.sharding import PartitionSpec as P


EPS = 1e-6
NEG_BIG = -1e30
F32 = jnp.float32
BF16 = jnp.bfloat16
CH = 512
HEADS = 4
GW = HEADS * 64
VMEM_LIMIT = 62 * 1024 * 1024
ANY = pl.BlockSpec(memory_space=pltpu.HBM)
SMEM = pl.BlockSpec(memory_space=pltpu.SMEM)
VMEM = pl.BlockSpec(memory_space=pltpu.VMEM)


def rms(h, gain):
    h32 = h.astype(F32)
    inv = lax.rsqrt(jnp.mean(h32 * h32, axis=-1, keepdims=True) + EPS)
    return (h32 * inv * gain.astype(F32)).astype(BF16)


def dot(a, b):
    return jnp.dot(a, b, preferred_element_type=F32)


def kv_kernel(layers, n_src, lim_ref, pick_ref, *refs):
    srcs, (wk, wv, k_out, vt_out), refs = refs[:n_src], refs[n_src:n_src + 4], refs[n_src + 4:]
    if n_src == 1:
        mem, (w_s, k_s, vt_s, sem, w_sems, o_sems) = srcs[0], refs
    else:
        mem, w_s, k_s, vt_s, sem, w_sems, o_sems = refs
    rows = mem.shape[0]
    lo, n = layers

    def from_src(go):
        if n_src > 1:
            @pl.when(pick_ref[0] == 0)
            def _():
                go(pltpu.make_async_copy(srcs[0], mem, sem))

            @pl.when(pick_ref[0] != 0)
            def _():
                go(pltpu.make_async_copy(srcs[1], mem.at[pl.ds(0, CH)], sem))

    def w_copy(i, v):
        return pltpu.make_async_copy((wk, wv)[v].at[lo + i], w_s.at[2 * i + v], w_sems.at[2 * i + v])

    w_copy(0, 0).start()
    from_src(lambda cp: cp.start())
    from_src(lambda cp: cp.wait())
    w_copy(0, 1).start()

    def out_copy(i, v, c):
        at = pl.ds(pl.multiple_of(c * CH, CH), CH)
        if v == 0:
            return pltpu.make_async_copy(k_s.at[i, at, :], k_out.at[i, at, :], o_sems.at[i, v, c])
        return pltpu.make_async_copy(vt_s.at[i, :, at], vt_out.at[i, :, at], o_sems.at[i, v, c])

    def valid(c, go):
        @pl.when(lim_ref[c] > 0)
        def _():
            go()

    def layer_step(i, _):
        for v in range(2):
            w_copy(i, v).wait()

            @pl.when(i + 1 < n)
            def _(v=v):
                w_copy(i + 1, v).start()

            def chunk_step(c, _):
                def work():
                    def step(r, _):
                        at = pl.ds(pl.multiple_of(c * CH + r * 256, 256), 256)
                        out = dot(mem[at, :], w_s[2 * i + v]).astype(BF16)
                        if v == 0:
                            k_s[i, at, :] = out
                        else:
                            vt_s[i, :, at] = out.T
                        return 0

                    lax.fori_loop(0, CH // 256, step, 0)
                    out_copy(i, v, c).start()

                valid(c, work)
                return 0

            lax.fori_loop(0, rows // CH, chunk_step, 0)
        return 0

    lax.fori_loop(0, n, layer_step, 0)
    for i in range(n):
        for v in range(2):
            for c in range(rows // CH):
                valid(c, lambda i=i, v=v, c=c: out_copy(i, v, c).wait())


def kv_project(lims, pick, srcs, wk, wv, rows, layers):
    width, cols = wk.shape[1], wk.shape[2]
    n = layers[1]
    flops = n * 4 * rows * width * cols
    return pl.pallas_call(
        functools.partial(kv_kernel, layers, len(srcs)),
        in_specs=[SMEM, SMEM] + [VMEM if len(srcs) == 1 else ANY] * len(srcs) + [ANY, ANY],
        out_specs=[ANY, ANY],
        out_shape=[jax.ShapeDtypeStruct((n, rows, cols), BF16), jax.ShapeDtypeStruct((n, cols, rows), BF16)],
        scratch_shapes=[
            *([pltpu.VMEM((rows, width), BF16)] if len(srcs) > 1 else []),
            pltpu.VMEM((2 * n, width, cols), BF16),
            pltpu.VMEM((n, rows, cols), BF16),
            pltpu.VMEM((n, cols, rows), BF16),
            pltpu.SemaphoreType.DMA,
            pltpu.SemaphoreType.DMA((2 * n,)),
            pltpu.SemaphoreType.DMA((n, 2, rows // CH)),
        ],
        cost_estimate=pl.CostEstimate(flops=flops, bytes_accessed=n * 4 * width * cols, transcendentals=0),
        compiler_params=pltpu.CompilerParams(vmem_limit_bytes=VMEM_LIMIT),
        name="kv_project",
    )(lims, pick, *srcs, wk, wv)


def head_queries(qt, extra=None):
    row = lax.broadcasted_iota(jnp.int32, (128, qt.shape[1]), 0)
    out = []
    for h in range(HEADS):
        pair = qt[h // 2 * 128:(h // 2 + 1) * 128, :]
        q = jnp.where((row < 64) == (h % 2 == 0), pair, jnp.zeros_like(pair))
        out.append(q if extra is None else jnp.concatenate([q, extra], axis=0))
    return out


def attend_all(groups, n_chunks, scores, values, enter, leave, scratch):
    s_refs, mx_refs, (m_ref, l_ref, acc_ref) = scratch[:2], scratch[2:4], scratch[4:]
    total = groups * n_chunks

    def stage1(group, j, buf):
        for h, s in enumerate(scores(group, j)):
            first(h, s, buf)

    def first(h, s, buf):
        s_refs[buf][h] = s
        mx_refs[buf][h:h + 1, :] = jnp.max(s, axis=0, keepdims=True)

    def second(group, h, vt, buf):
        m_old = m_ref[group, h:h + 1, :]
        m_new = jnp.maximum(m_old, mx_refs[buf][h:h + 1, :])
        p = jnp.exp(s_refs[buf][h] - m_new)
        alpha = jnp.exp(m_old - m_new)
        m_ref[group, h:h + 1, :] = m_new
        l_ref[group, h:h + 1, :] = l_ref[group, h:h + 1, :] * alpha + jnp.sum(p, axis=0, keepdims=True)
        acc_ref[group, h] = acc_ref[group, h] * alpha + dot(vt[h * 64:(h + 1) * 64, :], p.astype(BF16))

    def advance(group, j):
        wrap = j + 1 == n_chunks
        return jnp.where(wrap, group + 1, group), jnp.where(wrap, 0, j + 1)

    enter(0)
    stage1(0, 0, 0)

    def item(group, j, buf):
        group_next, j_next = advance(group, j)

        @pl.when((j_next == 0) & (group_next < groups))
        def _():
            enter(group_next)

        made = scores(jnp.minimum(group_next, groups - 1), j_next)
        vt = values(group, j)
        for h in range(HEADS):
            first(h, next(made), 1 - buf)
            second(group, h, vt, buf)

        @pl.when(j_next == 0)
        def _():
            leave(group)

    def step(u, now):
        item(*now, 0)
        now = advance(*now)

        @pl.when(2 * u + 1 < total)
        def _():
            item(*now, 1)

        return advance(*now)

    lax.fori_loop(0, (total + 1) // 2, step, (jnp.int32(0), jnp.int32(0)))


def attend_reset(scratch):
    m_ref, l_ref, acc_ref = scratch[4:]
    m_ref[...] = jnp.full_like(m_ref, -jnp.inf)
    l_ref[...] = jnp.zeros_like(l_ref)
    acc_ref[...] = jnp.zeros_like(acc_ref)


def attend_finish(group, at_ref, scratch):
    l_ref, acc_ref = scratch[5:]
    for h in range(HEADS):
        rows = pl.ds(pl.multiple_of(group * HEADS * 64 + h * 64, 64), 64)
        at_ref[rows, :] = (acc_ref[group, h] / l_ref[group, h:h + 1, :]).astype(BF16)


def attend_scratch(groups, rows):
    return [
        pltpu.VMEM((HEADS, CH, rows), F32),
        pltpu.VMEM((HEADS, CH, rows), F32),
        pltpu.VMEM((HEADS, rows), F32),
        pltpu.VMEM((HEADS, rows), F32),
        pltpu.VMEM((groups, HEADS, rows), F32),
        pltpu.VMEM((groups, HEADS, rows), F32),
        pltpu.VMEM((groups, HEADS, 64, rows), F32),
    ]


def self_kernel(layer, far_given, *refs):
    own_ref, refs = refs[0], refs[1:]
    if far_given:
        s2, refs = refs[0], refs[1:]
    gs_ref, gc_ref, wq, wk, wv, wo, wcq, hid_ref, q_ref, w_s, x_s, k_s, vt_s, qs, bias, at_s, a_s, s1, s3 = refs[:19]
    refs = refs[19:]
    if not far_given:
        s2, refs = refs[0], refs[1:]
    scratch, (sems, near_sems, far_sems, fwd_sems) = refs[:7], refs[7:]
    rows, width = own_ref.shape
    parts = far_sems.shape[1]
    parts_half = parts // 2
    dev = lax.axis_index("sp")
    odd = lax.rem(dev, 2)
    chip1 = dev >= 2
    sibling = dev + 1 - 2 * odd
    across = lax.rem(dev + 2, 4)

    w_copies = [pltpu.make_async_copy(src.at[layer], w_s.at[n], sems.at[n]) for n, src in enumerate((wk, wv, wq, wo, wcq))]
    w_copies[0].start()
    w_copies[1].start()

    barrier = pltpu.get_barrier_semaphore()
    others = (sibling,) if far_given else (sibling, across)
    for other in others:
        pl.semaphore_signal(barrier, inc=1, device_id={"sp": other}, device_id_type=pl.DeviceIdType.MESH)
    pl.semaphore_wait(barrier, len(others))

    def send(src, dst, sem, other):
        return pltpu.make_async_remote_copy(src_ref=src, dst_ref=dst, send_sem=sem.at[0], recv_sem=sem.at[1],
                                            device_id={"sp": other}, device_id_type=pl.DeviceIdType.MESH)

    def part(i):
        return pl.ds(i * (rows // parts), rows // parts)

    near = send(own_ref, s1, near_sems, sibling)
    far = [send(own_ref.at[part(i)], s2.at[part(i)], far_sems.at[:, i], across) for i in range(parts)]
    fwd = [send(s2.at[part(i)], s3.at[part(i)], fwd_sems.at[:, i], sibling) for i in range(parts)]

    if not far_given:
        @pl.when(jnp.logical_not(chip1))
        def _():
            for cp in far:
                cp.start()

    @pl.when(odd == 0)
    def _():
        near.start()

    if far_given:
        @pl.when(chip1)
        def _():
            for cp in fwd:
                cp.start()

    gain = gs_ref[layer:layer + 1, :]
    x_s[pl.ds(0, rows), :] = rms(own_ref[...], gain)
    key = lax.broadcasted_iota(jnp.int32, (rows, rows), 0)
    query = lax.broadcasted_iota(jnp.int32, (rows, rows), 1)
    bias[0, pl.ds(0, rows), :] = jnp.where(key <= query, 0.0, NEG_BIG)
    bias[0, pl.ds(rows, rows), :] = jnp.full((rows, rows), jnp.where(odd == 1, 0.0, NEG_BIG), F32)
    bias[1] = jnp.zeros((2 * rows, rows), F32)
    attend_reset(scratch)

    @pl.when(odd == 1)
    def _():
        near.wait_recv()
        x_s[pl.ds(rows, rows), :] = rms(s1[...], gain)

    @pl.when(odd == 0)
    def _():
        x_s[pl.ds(rows, rows), :] = jnp.zeros((rows, width), BF16)

    def tile(t):
        return pl.ds(pl.multiple_of(t * 256, 256), 256)

    def head_cols(i):
        return pl.ds(pl.multiple_of(i * GW, GW), GW)

    def phase(half, _):
        at = pl.ds(pl.multiple_of(half * CH, CH), CH)

        @pl.when(half == 0)
        def _():
            w_copies[0].wait()
            w_copies[2].start()

        def project_step(r, _):
            rows_at = tile(2 * half + r)
            for first in range(0, parts, parts_half):
                @pl.when((half == 1) & (r == first // parts_half))
                def _(first=first):
                    some = range(first, first + parts_half)
                    if not far_given:
                        for i in some:
                            far[i].wait_recv()
                            fwd[i].start()
                    here = pl.ds(first * (rows // parts), rows // 2)
                    x_s[pl.ds(2 * rows + 2 * first * (rows // parts), rows // 2), :] = rms(s2[here, :], gain)
                    for i in some:
                        fwd[i].wait_recv()
                    x_s[pl.ds(2 * rows + 2 * first * (rows // parts) + rows // 2, rows // 2), :] = rms(s3[here, :], gain)

            k_s[rows_at, :] = dot(x_s[rows_at, :], w_s[0]).astype(BF16)

            @pl.when((half == 0) & (r == 0))
            def _():
                w_copies[1].wait()
                w_copies[3].start()

            vt_s[:, rows_at] = dot(x_s[rows_at, :], w_s[1]).astype(BF16).T
            return 0

        lax.fori_loop(0, 2, project_step, 0)

        @pl.when(half == 0)
        def _():
            w_copies[2].wait()
            w_copies[4].start()

            qs[...] = (dot(x_s[pl.ds(0, rows), :], w_s[2]).astype(BF16) * BF16(0.125)).T

        def scores(i, j):
            k = k_s[at, head_cols(i)]
            return (dot(k[:, h // 2 * 128:(h // 2 + 1) * 128], q) + bias[half] for h, q in enumerate(head_queries(qs[head_cols(i), :])))

        attend_all(width // GW, 1, scores, lambda i, j: vt_s[head_cols(i), at], lambda i: None, lambda i: None, scratch)
        return 0

    lax.fori_loop(0, jnp.where(chip1, 2, 1), phase, 0)

    def finish(i, _):
        attend_finish(i, at_s, scratch)
        return 0

    lax.fori_loop(0, width // GW, finish, 0)
    a_s[...] = at_s[...].T
    w_copies[3].wait()

    hid_ref[...] = (own_ref[...].astype(F32) + dot(a_s[...], w_s[3])).astype(BF16)
    a_s[...] = rms(hid_ref[...], gc_ref[layer:layer + 1, :])
    w_copies[4].wait()

    q_ref[...] = (dot(a_s[...], w_s[4]).astype(BF16) * BF16(0.125)).T

    @pl.when(odd == 0)
    def _():
        near.wait_send()

    @pl.when(chip1)
    def _():
        for cp in fwd:
            cp.wait_send()

    if not far_given:
        @pl.when(jnp.logical_not(chip1))
        def _():
            for cp in far:
                cp.wait_send()


def self_attention(layer, own, far, gs, gc, wq, wk, wv, wo, wcq):
    rows, width = own.shape
    far_given = far is not None
    parts = 2 if far_given else 4
    shape = jax.ShapeDtypeStruct((rows, width), BF16)
    flops = 2 * rows * width * width * 11 + 4 * rows * 4 * rows * width
    block = pltpu.VMEM((rows, width), BF16)
    return pl.pallas_call(
        functools.partial(self_kernel, layer, far_given),
        in_specs=[VMEM] * (4 if far_given else 3) + [ANY] * 5,
        out_specs=[VMEM, VMEM],
        out_shape=[shape, jax.ShapeDtypeStruct((width, rows), BF16)],
        scratch_shapes=[
            pltpu.VMEM((5, width, width), BF16),
            pltpu.VMEM((4 * rows, width), BF16),
            pltpu.VMEM((4 * rows, width), BF16),
            pltpu.VMEM((width, 4 * rows), BF16),
            pltpu.VMEM((width, rows), BF16),
            pltpu.VMEM((2, 2 * rows, rows), F32),
            pltpu.VMEM((width, rows), BF16),
            block,
            block,
            block,
            *([] if far_given else [block]),
            *attend_scratch(width // GW, rows),
            pltpu.SemaphoreType.DMA((5,)),
            pltpu.SemaphoreType.DMA((2,)),
            pltpu.SemaphoreType.DMA((2, parts)),
            pltpu.SemaphoreType.DMA((2, parts)),
        ],
        cost_estimate=pl.CostEstimate(flops=flops, bytes_accessed=10 * width * width, transcendentals=0),
        compiler_params=pltpu.CompilerParams(vmem_limit_bytes=VMEM_LIMIT, collective_id=layer, has_side_effects=True),
        name="self_attention",
    )(own, *([far] if far_given else []), gs, gc, wq, wk, wv, wo, wcq)


def cross_kernel(layer, planes, n_kv, lim_ref, q_ref, *refs):
    def take(n):
        nonlocal refs
        head, refs = refs[:n], refs[n:]
        return head

    ks, vts = take(n_kv), take(n_kv)
    hid_ref, gm_ref, wco, wg, wu, wd, out_ref = take(7)
    scratch = take(7)
    kbuf, vbuf, mask, list_s, kv_sems = take(5)
    at_s, a_s, act0, act1, acc_o, wo_s, wg_s, wu_s, wd_s, o_sem, w_sems = take(11)
    ring, ff = wg_s.shape[0], wg_s.shape[2]
    steps = wg.shape[2] // ff
    width, rows = q_ref.shape
    groups = width // GW

    def kv_copies(i, go):
        slot = lax.rem(i, 2)
        cols = pl.ds(pl.multiple_of(i * GW, GW), GW)
        at = 0
        for n in range(n_kv):
            there = pl.ds(at, ks[n].shape[1])
            go(pltpu.make_async_copy(ks[n].at[planes[n], :, cols], kbuf.at[slot, there, :], kv_sems.at[slot, 0, n]))
            go(pltpu.make_async_copy(vts[n].at[planes[n], cols, :], vbuf.at[slot, :, there], kv_sems.at[slot, 1, n]))
            at += ks[n].shape[1]

    def kv_start(i):
        kv_copies(i, lambda cp: cp.start())

    kv_start(0)
    kv_start(1)
    o_copy = pltpu.make_async_copy(wco.at[layer], wo_s, o_sem)

    def w_copies(j):
        cols = pl.ds(pl.multiple_of(j * ff, ff), ff)
        slot = lax.rem(j, ring)
        return (pltpu.make_async_copy(wg.at[layer, :, cols], wg_s.at[slot], w_sems.at[0, slot]),
                pltpu.make_async_copy(wu.at[layer, :, cols], wu_s.at[slot], w_sems.at[1, slot]),
                pltpu.make_async_copy(wd.at[layer, cols, :], wd_s.at[slot], w_sems.at[2, slot]))

    def w_start(j):
        for cp in w_copies(j):
            cp.start()

    attend_reset(scratch)

    n_chunks, last = jnp.int32(0), jnp.int32(0)
    list_s[0] = 0
    for c in range(lim_ref.shape[0]):
        lim = lim_ref[c]

        @pl.when(lim > 0)
        def _(c=c, at=n_chunks):
            list_s[at] = c

        n_chunks = n_chunks + (lim > 0).astype(jnp.int32)
        last = last + jnp.where(lim < CH, lim, 0)
    key = lax.broadcasted_iota(jnp.int32, (CH, 128), 0)
    lane = lax.broadcasted_iota(jnp.int32, (CH, 128), 1)
    mask[0] = jnp.zeros((CH, 128), BF16)
    mask[1] = jnp.where((key >= last) & (lane == 0), NEG_BIG, 0.0).astype(BF16)
    ones = (lax.broadcasted_iota(jnp.int32, (128, rows), 0) == 0).astype(F32).astype(BF16)

    def enter(i):
        kv_copies(i, lambda cp: cp.wait())

        @pl.when(i == 0)
        def _():
            o_copy.start()
            for j in range(ring - groups):
                w_start(j)

        w_start(ring - groups + i)

    def leave(i):
        @pl.when(i + 2 < groups)
        def _():
            kv_start(i + 2)

    def chunk(j):
        return pl.ds(pl.multiple_of(list_s[j] * CH, CH), CH)

    def scores(i, j):
        partial = (lim_ref[list_s[j]] < CH).astype(jnp.int32)
        k = kbuf[lax.rem(i, 2), chunk(j), :]
        ks = [jnp.concatenate([k[:, p * 128:(p + 1) * 128], mask[partial]], axis=1) for p in range(HEADS // 2)]
        queries = head_queries(q_ref[pl.ds(pl.multiple_of(i * GW, GW), GW), :], ones)
        return (dot(ks[h // 2], q) for h, q in enumerate(queries))

    def values(i, j):
        return vbuf[lax.rem(i, 2), :, chunk(j)]

    attend_all(groups, n_chunks, scores, values, enter, leave, scratch)

    def finish(i, _):
        attend_finish(i, at_s, scratch)
        return 0

    lax.fori_loop(0, groups, finish, 0)
    a_s[...] = at_s[...].T
    o_copy.wait()

    out_ref[...] = (hid_ref[...].astype(F32) + dot(a_s[...], wo_s[...])).astype(BF16)
    a_s[...] = rms(out_ref[...], gm_ref[layer:layer + 1, :])
    acc_o[...] = jnp.zeros_like(acc_o)

    def wait_gate_up(j):
        for cp in w_copies(j)[:2]:
            cp.wait()

    def gate_up(j, act_ref):
        x = a_s[...]
        gate = dot(x, wg_s[lax.rem(j, ring)])
        up = dot(x, wu_s[lax.rem(j, ring)])
        act_ref[...] = (gate / (1.0 + jnp.exp(-gate)) * up).astype(BF16)

    wait_gate_up(0)
    gate_up(0, act0)

    def mlp_step(u, _):
        first = 2 * u
        w_copies(first)[2].wait()
        wait_gate_up(first + 1)
        w_copies(first + 1)[2].wait()

        @pl.when(first + 2 < steps)
        def _():
            wait_gate_up(first + 2)

        acc_o[...] += dot(act0[...], wd_s[lax.rem(first, ring)])
        gate_up(first + 1, act1)
        acc_o[...] += dot(act1[...], wd_s[lax.rem(first + 1, ring)])
        gate_up(jnp.minimum(first + 2, steps - 1), act0)

        for j in (first, first + 1):
            @pl.when(j + ring < steps)
            def _(j=j):
                w_start(j + ring)
        return 0

    lax.fori_loop(0, steps // 2, mlp_step, 0)
    out_ref[...] = (out_ref[...].astype(F32) + acc_o[...]).astype(BF16)


def cross_mlp(layer, lims, q, kvs, hid, gm, wco, wg, wu, wd):
    width, rows = q.shape
    groups = width // GW
    planes = tuple(plane for _, _, plane in kvs)
    ks, vts = [k for k, _, _ in kvs], [v for _, v, _ in kvs]
    total = sum(k.shape[1] for k in ks)
    n = len(kvs)
    ff, ring = 512, 6
    return pl.pallas_call(
        functools.partial(cross_kernel, layer, planes, n),
        in_specs=[SMEM, VMEM] + [ANY] * (2 * n) + [VMEM] * 2 + [ANY] * 4,
        out_specs=VMEM,
        out_shape=jax.ShapeDtypeStruct((rows, width), BF16),
        scratch_shapes=attend_scratch(groups, rows) + [
            pltpu.VMEM((2, total, GW), BF16),
            pltpu.VMEM((2, GW, total), BF16),
            pltpu.VMEM((2, CH, 128), BF16),
            pltpu.SMEM((8,), jnp.int32),
            pltpu.SemaphoreType.DMA((2, 2, n)),
            pltpu.VMEM((width, rows), BF16),
            pltpu.VMEM((rows, width), BF16),
            pltpu.VMEM((rows, ff), BF16),
            pltpu.VMEM((rows, ff), BF16),
            pltpu.VMEM((rows, width), F32),
            pltpu.VMEM((width, width), BF16),
            pltpu.VMEM((ring, width, ff), BF16),
            pltpu.VMEM((ring, width, ff), BF16),
            pltpu.VMEM((ring, ff, width), BF16),
            pltpu.SemaphoreType.DMA,
            pltpu.SemaphoreType.DMA((3, ring)),
        ],
        cost_estimate=pl.CostEstimate(
            flops=4 * rows * 3072 * width + 2 * rows * width * (width + 3 * wg.shape[2]),
            bytes_accessed=2 * width * (width + 3 * wg.shape[2]), transcendentals=0),
        compiler_params=pltpu.CompilerParams(vmem_limit_bytes=VMEM_LIMIT),
        name="cross_mlp",
    )(lims, q, *ks, *vts, hid, gm, wco, wg, wu, wd)


NONE = 1 << 20
BASES = (
    (0, 512, 1024, 1536, 2048, NONE, NONE, 2560),
    (1024, 1536, 0, 512, NONE, 2048, 2560, NONE),
    (2048, NONE, 2560, NONE, 0, 1024, 512, 1536),
    (2560, NONE, 2048, NONE, 1024, 0, 1536, 512),
)


def solution(mesh):
    row_spec = P(('dp', 'sp'), None)

    def local_step(hidden, memory, mem_len, norm_self, norm_cross, norm_mlp, self_q, self_k, self_v, self_o, cross_q, cross_k, cross_v, cross_o, mlp_gate, mlp_up, mlp_down):
        layers, width = norm_self.shape
        w_so = self_o.reshape(layers, width, width)
        w_co = cross_o.reshape(layers, width, width)
        dev = lax.axis_index('sp')
        dev_arr = dev.astype(jnp.int32).reshape(1)
        bases = jnp.array(BASES, jnp.int32)[dev]
        lims = jnp.clip(mem_len[0] - bases, 0, CH)
        is3 = (dev_arr == 3).astype(jnp.int32)

        def swap(x):
            return lax.ppermute(x, 'sp', [(0, 1), (1, 0), (2, 3), (3, 2)])

        def program(hidden):
            far = lax.ppermute(hidden, 'sp', [(0, 2), (1, 3)])
            mem_a, mem_b = memory[:CH], memory[CH:]
            c2b = lax.ppermute(mem_b, 'sp', [(2, 3)])
            rem_a = lax.ppermute(mem_a, 'sp', [(0, 2), (1, 3), (2, 0)])
            rem_b = lax.ppermute(mem_b, 'sp', [(0, 2), (1, 3), (2, 1)])

            both = (0, layers)
            ka, va = kv_project(lims[0:2], is3, [memory, c2b], cross_k, cross_v, 2 * CH, both)
            kas, vas = swap(ka), swap(va)
            kb, vb = kv_project(lims[4:5], is3, [rem_a], cross_k, cross_v, CH, both)
            kbs, vbs = swap(kb), swap(vb)
            kvs = []
            for layer in range(layers):
                kc, vc = kv_project(lims[6:7], is3, [rem_b], cross_k, cross_v, CH, (layer, 1))
                kcs, vcs = swap(kc), swap(vc)
                kvs.append([(ka, va, layer), (kas, vas, layer), (kb, vb, layer), (kbs, vbs, layer), (kc, vc, 0), (kcs, vcs, 0)])

            for layer in range(layers):
                hidden, q = self_attention(layer, hidden, far, norm_self, norm_cross, self_q, self_k, self_v, w_so, cross_q)
                hidden = cross_mlp(layer, lims, q, kvs[layer], hidden, norm_mlp, w_co, mlp_gate, mlp_up, mlp_down)
                far = None
            return hidden

        return program(hidden)

    return jax.shard_map(local_step, mesh=mesh, in_specs=(row_spec, row_spec, P('dp')) + (P(),) * 14, out_specs=row_spec, check_vma=False)
```
